32 devices in a mesh: dp: 8 (over z, x), ctx: 4 (over y, core).
Axes of the slice: x: 2, y: 2, z: 4, core: 2. Of those that a mesh axis runs over, the one named last changes fastest.
Arguments:
- tokens: bfloat16 [8192, 1536], P(('dp', 'ctx')), may hold values from -6 to 6
- norm_attn: float32 [1536], P(('dp', 'ctx')), may hold values from 0.5 to 1.5
- w_qkv: bfloat16 [3072, 1536], P(('dp', 'ctx')), may hold values from -1 to 1
- w_out: bfloat16 [1536, 1536], P(('dp', 'ctx')), may hold values from -0.875 to 0.875
- norm_mlp: float32 [1536], P(('dp', 'ctx')), may hold values from 0.5 to 1.5
- w_gate_up: bfloat16 [8192, 1536], P(('dp', 'ctx')), may hold values from -0.15625 to 0.15625
- w_down: bfloat16 [1536, 4096], P(('dp', 'ctx')), may hold values from -0.09375 to 0.09375
- cotangent: bfloat16 [8192, 1536], P(('dp', 'ctx')), may hold values from -6 to 6
- seq_lengths: int32 [8, 2], P('dp'), may hold values from 1 to 768, 1024 in all within a row
- block_slot: int32 [8, 8], P('dp'), may hold values from 0 to 7, each once within a row
Outputs:
- result: bfloat16 [8192, 1536], P(('dp', 'ctx'))
- grad_input: float32 [8192, 1536], P(('dp', 'ctx'))
- grad_norm_attn: float32 [1536], P(('dp', 'ctx'))
- grad_qkv: float32 [3072, 1536], P(('dp', 'ctx'))
- grad_out: float32 [1536, 1536], P(('dp', 'ctx'))
- grad_norm_mlp: float32 [1536], P(('dp', 'ctx'))
- grad_gate_up: float32 [8192, 1536], P(('dp', 'ctx'))
- grad_down: float32 [1536, 4096], P(('dp', 'ctx'))
The draws below stay inside these ranges and needn't reach their ends.
Inputs may be any that keep to these rules, and one draw needn't show every extreme that they name: `seq_lengths`: each row sums to 1024. `block_slot`: each row names every number once; ctx device c of group g holds the blocks of positions c * 2 to (c + 1) * 2 - 1 of that row.
All inputs are finite; a program needn't handle non-finite values.
Results may differ from the reference program's by a relative error of at most 0.025.
Values may be sent and summed in bfloat16 or wider, within the bound.
A program may use at most 320 MiB of HBM per device.

```python
import math
import jax
import jax.numpy as jnp
import numpy as np
from jax import lax

D = 1536
QUERY_HEADS = 16
KEY_VALUE_HEADS = 8
HEAD_SIZE = 96
FF = 4096
BLK = 128
SEQS = 2
TOK_DEV = 256
QUERY_FEATURES = 1536
KEY_FEATURES = 768
GROUP_TOK = 1024
LEN_MAX = 768
BLOCKS = 8
TOKENS = 8192
N_DP = 8
N_CTX = 4


def qkv_normal(key):
    return jax.random.truncated_normal(jax.random.fold_in(key, 7), -3.0, 3.0, (QUERY_FEATURES + 2 * KEY_FEATURES, D), jnp.float32)


def draw_w_qkv(key, part):
    weights_drawn = qkv_normal(key) * (1.0 / D ** 0.5)
    return weights_drawn.astype(jnp.bfloat16)


def draw_tokens(key, part):
    noise_key = jax.random.fold_in(jax.random.fold_in(key, 3), 0)
    noise = jax.random.normal(noise_key, (TOKENS, D), jnp.float32)
    return jnp.clip(noise, -6.0, 6.0).astype(jnp.bfloat16)


def level_of(key, shape, cuts, low, top_value):
    level = 1.0
    for position, parts in cuts:
        heights = jax.random.uniform(jax.random.fold_in(jax.random.fold_in(key, 6), position), (parts,), jnp.float32, low / len(cuts), top_value / len(cuts))
        level = level * jnp.repeat(jnp.exp(heights), shape[position] // parts).reshape((-1,) + (1,) * (len(shape) - 1 - position))
    return level


def profile(count, total, limit, skew):
    portions = [(1 << 20) // math.isqrt(standing ** skew) + 1 for standing in range(2, count + 1)]
    spare, holding = total - limit - (count - 1), [1] * (count - 1)
    while spare > 0:
        candidates = [i for i in range(count - 1) if holding[i] < limit]
        whole, budget = sum([portions[i] for i in candidates]), spare
        for i in candidates:
            extra = min(limit - holding[i], max(1, budget * portions[i] // whole), spare)
            holding[i] = holding[i] + extra
            spare = spare - extra
    return np.array([limit] + holding)


def ragged_sizes(stream_key, number_of, total, limit, lean):
    if number_of == 2:
        one = jax.random.randint(stream_key, (), max(1, total - limit), min(limit, total - 1) + 1)
        return jnp.stack([one, total - one])
    tallies = jnp.asarray(profile(number_of, total, limit, lean), jnp.int32)
    couples = (number_of - 1) // 2
    giver, sink = tallies[1:1 + 2 * couples:2], tallies[2:2 + 2 * couples:2]
    slack = jnp.minimum(giver - 1, limit - sink)
    shifted = jax.random.randint(jax.random.fold_in(stream_key, 1), (couples,), 0, 1 << 20) % (slack + 1)
    tallies = tallies.at[1:1 + 2 * couples:2].set(giver - shifted).at[2:2 + 2 * couples:2].set(sink + shifted)
    return tallies[jax.random.permutation(jax.random.fold_in(stream_key, 2), number_of)]


def centred(key, extent, scale, reach, pieces=(), held_as=jnp.bfloat16):
    entries = scale * jax.random.normal(key, extent, jnp.float32)
    if pieces:
        entries = entries * level_of(key, extent, pieces, -0.22, 0.18)
    return jnp.clip(entries, -reach, reach).astype(held_as)


def setup_inputs(seed: int = 0) -> dict:
    seeds = jax.random.split(jax.random.key(seed), 11)
    tokens = draw_tokens(jax.random.fold_in(seeds[10], 71), 0)
    norm_attn = jnp.clip(1.0 + 0.1 * jax.random.normal(seeds[1], (D,), jnp.float32), 0.5, 1.5)
    w_qkv = draw_w_qkv(jax.random.fold_in(seeds[10], 71), 0)
    w_out = centred(seeds[3], (D, QUERY_FEATURES), (QUERY_FEATURES // 32) ** -0.5, 0.875, ((0, 32),))
    norm_mlp = jnp.clip(1.0 + 0.1 * jax.random.normal(seeds[4], (D,), jnp.float32), 0.5, 1.5)
    w_gate_up = centred(seeds[5], (2 * FF, D), D ** -0.5, 0.15625, ((0, 32),))
    w_down = centred(seeds[6], (D, FF), FF ** -0.5, 0.09375, ((0, 32),))
    cotangent = centred(seeds[7], (TOKENS, D), 1.0, 6.0, ((0, 32),))
    seq_lengths = jax.vmap(lambda own: ragged_sizes(own, SEQS, GROUP_TOK, LEN_MAX, 2))(jax.random.split(seeds[8], N_DP)).reshape((N_DP, SEQS)).astype(jnp.int32)
    block_slot = jax.vmap(lambda own: jax.random.permutation(own, BLOCKS))(jax.random.split(seeds[9], N_DP)).reshape((N_DP, BLOCKS)).astype(jnp.int32)
    return {"tokens": tokens, "norm_attn": norm_attn, "w_qkv": w_qkv, "w_out": w_out, "norm_mlp": norm_mlp, "w_gate_up": w_gate_up, "w_down": w_down, "cotangent": cotangent, "seq_lengths": seq_lengths, "block_slot": block_slot}


EPSILON = 1e-05
THETA = 100000.0
MASK_FILL = -1e+30

def rope_tables(rope_pos):
    half_dim = HEAD_SIZE // 2
    exponent = jnp.arange(half_dim, dtype=jnp.float32) * (2.0 / HEAD_SIZE)
    frequency = jnp.power(jnp.float32(THETA), -exponent)
    angles = rope_pos.astype(jnp.float32)[:, None] * frequency[None, :]
    return (jnp.cos(angles)[:, None, :], jnp.sin(angles)[:, None, :])

def apply_rotation(values, cosine_table, sine_values):
    half_dim = HEAD_SIZE // 2
    first_half = values[..., :half_dim]
    second_half = values[..., half_dim:]
    return jnp.concatenate([first_half * cosine_table - second_half * sine_values, second_half * cosine_table + first_half * sine_values], -1)

def rotate_back(gradient, cosine_table, sine_values):
    half_dim = HEAD_SIZE // 2
    first_half = gradient[..., :half_dim]
    second_half = gradient[..., half_dim:]
    return jnp.concatenate([first_half * cosine_table + second_half * sine_values, second_half * cosine_table - first_half * sine_values], -1)

def positions(lengths, slot_table, first_row, count_of_rows):
    row_index = first_row + jnp.arange(count_of_rows, dtype=jnp.int32)
    block_index = row_index // BLK
    lookup = jnp.arange(slot_table.shape[0], dtype=jnp.int32)
    slot_of = lax.optimization_barrier(jnp.sum(jnp.where(block_index[:, None] == lookup[None, :], slot_table[None, :], 0), 1)).astype(jnp.int32)
    stream = (slot_of * BLK + row_index % BLK).astype(jnp.int32)
    seq_ends = jnp.cumsum(lengths).astype(jnp.int32)
    passed = stream[:, None] >= seq_ends[None, :]
    segment = lax.optimization_barrier(jnp.sum(passed.astype(jnp.int32), 1)).astype(jnp.int32)
    offset = lax.optimization_barrier(jnp.sum(jnp.where(passed, seq_ends[None, :], 0), 1)).astype(jnp.int32)
    return (stream, segment, stream - offset)

def rounded(values):
    return lax.optimization_barrier(values.astype(jnp.bfloat16)).astype(jnp.float32)

def norm_back(grad_normed, gain, source, scale):
    weighted = grad_normed * gain
    return scale * weighted - source * scale ** 3 * lax.optimization_barrier(jnp.mean(weighted * source, -1, keepdims=True))

def masked_scores(query_rows, every_key, query_stream, query_segment, key_stream, key_segment):
    scores = jnp.einsum('rgjd,ngd->gjrn', query_rows.astype(jnp.float32), every_key.astype(jnp.float32)) * (1.0 / math.sqrt(HEAD_SIZE))
    allowed = (query_segment[:, None] == key_segment[None, :]) & (key_stream[None, :] <= query_stream[:, None])
    return (jnp.where(allowed[None, None], scores, MASK_FILL), allowed[None, None])

def reference(tokens, norm_attn, w_qkv, w_out, norm_mlp, w_gate_up, w_down, cotangent, seq_lengths, block_slot):
    grouped_rows = TOK_DEV * N_CTX
    heads_ratio = QUERY_HEADS // KEY_VALUE_HEADS
    score_scale = 1.0 / math.sqrt(HEAD_SIZE)

    def group_pass(totals, inputs):
        group_tokens, upstream, lengths, slot_table = inputs
        stream, segment, rope_pos = positions(lengths, slot_table, 0, grouped_rows)
        cosine_table, sine_values = rope_tables(rope_pos)
        source = group_tokens.astype(jnp.float32)
        scale_one = lax.rsqrt(lax.optimization_barrier(jnp.mean(source * source, -1, keepdims=True)) + EPSILON)
        normed_one = (source * scale_one * norm_attn).astype(jnp.bfloat16)
        projected_output = jnp.dot(normed_one, w_qkv.T, preferred_element_type=jnp.float32)
        query_rows = apply_rotation(projected_output[:, :QUERY_FEATURES].reshape(grouped_rows, QUERY_HEADS, HEAD_SIZE), cosine_table, sine_values).astype(jnp.bfloat16)
        every_key = apply_rotation(projected_output[:, QUERY_FEATURES:QUERY_FEATURES + KEY_FEATURES].reshape(grouped_rows, KEY_VALUE_HEADS, HEAD_SIZE), cosine_table, sine_values).astype(jnp.bfloat16)
        every_value = projected_output[:, QUERY_FEATURES + KEY_FEATURES:].reshape(grouped_rows, KEY_VALUE_HEADS, HEAD_SIZE).astype(jnp.bfloat16)
        grouped_queries = query_rows.reshape(grouped_rows, KEY_VALUE_HEADS, heads_ratio, HEAD_SIZE)
        block_rows = min(512, grouped_rows)
        block_count = grouped_rows // block_rows

        def forward_block(which_block):
            row_begin = which_block * block_rows
            block_queries = lax.dynamic_slice_in_dim(grouped_queries, row_begin, block_rows, 0)
            block_stream = lax.dynamic_slice_in_dim(stream, row_begin, block_rows, 0)
            block_segment = lax.dynamic_slice_in_dim(segment, row_begin, block_rows, 0)
            scores, allowed = masked_scores(block_queries, every_key, block_stream, block_segment, stream, segment)
            highest_score = lax.optimization_barrier(jnp.max(scores, -1, keepdims=True))
            log_total = highest_score + jnp.log(lax.optimization_barrier(jnp.sum(jnp.exp(scores - highest_score), -1, keepdims=True)))
            weights = rounded(jnp.where(allowed, jnp.exp(scores - log_total), 0.0))
            mixture = jnp.einsum('gjrn,ngd->rgjd', weights, every_value.astype(jnp.float32))
            return (mixture.astype(jnp.bfloat16), log_total[..., 0])
        attended, log_totals = lax.map(forward_block, jnp.arange(block_count, dtype=jnp.int32))
        attention_output = attended.reshape(grouped_rows, QUERY_FEATURES)
        residual = source + jnp.dot(attention_output, w_out.T, preferred_element_type=jnp.float32)
        scale_two = lax.rsqrt(lax.optimization_barrier(jnp.mean(residual * residual, -1, keepdims=True)) + EPSILON)
        normed_two = (residual * scale_two * norm_mlp).astype(jnp.bfloat16)
        gate_up = jnp.dot(normed_two, w_gate_up.T, preferred_element_type=jnp.float32)
        gate_part = gate_up[:, :FF]
        up_part = gate_up[:, FF:]
        sigmoid = jax.nn.sigmoid(gate_part)
        hidden = (gate_part * sigmoid * up_part).astype(jnp.bfloat16)
        result = (residual + jnp.dot(hidden, w_down.T, preferred_element_type=jnp.float32)).astype(jnp.bfloat16)
        grad_down = jnp.dot(upstream.T, hidden, preferred_element_type=jnp.float32)
        grad_hidden = jnp.dot(upstream, w_down, preferred_element_type=jnp.float32)
        grad_gate = grad_hidden * up_part * sigmoid * (1.0 + gate_part * (1.0 - sigmoid))
        grad_upper = grad_hidden * gate_part * sigmoid
        grad_gu = jnp.concatenate([grad_gate, grad_upper], 1).astype(jnp.bfloat16)
        grad_w_gate_up = jnp.dot(grad_gu.T, normed_two, preferred_element_type=jnp.float32)
        grad_normed_two = jnp.dot(grad_gu, w_gate_up, preferred_element_type=jnp.float32)
        grad_gain_two = lax.optimization_barrier(jnp.sum(grad_normed_two * residual * scale_two, 0))
        grad_residual = upstream.astype(jnp.float32) + norm_back(grad_normed_two, norm_mlp, residual, scale_two)
        grad_res_bf = grad_residual.astype(jnp.bfloat16)
        grad_w_out = jnp.dot(grad_res_bf.T, attention_output, preferred_element_type=jnp.float32)
        attention_gradient = jnp.dot(grad_res_bf, w_out, preferred_element_type=jnp.float32).astype(jnp.bfloat16)
        grouped_gradient = attention_gradient.reshape(grouped_rows, KEY_VALUE_HEADS, heads_ratio, HEAD_SIZE)
        attention_grouped = attention_output.reshape(grouped_rows, KEY_VALUE_HEADS, heads_ratio, HEAD_SIZE)
        row_delta = jnp.transpose(lax.optimization_barrier(jnp.sum(grouped_gradient.astype(jnp.float32) * attention_grouped.astype(jnp.float32), -1)), (1, 2, 0))

        def backward_block(running, which_block):
            grad_keys, grad_values = running
            row_begin = which_block * block_rows
            block_queries = lax.dynamic_slice_in_dim(grouped_queries, row_begin, block_rows, 0)
            block_grads = lax.dynamic_slice_in_dim(grouped_gradient, row_begin, block_rows, 0).astype(jnp.float32)
            block_stream = lax.dynamic_slice_in_dim(stream, row_begin, block_rows, 0)
            block_segment = lax.dynamic_slice_in_dim(segment, row_begin, block_rows, 0)
            block_delta = lax.dynamic_slice_in_dim(row_delta, row_begin, block_rows, 2)
            block_log = log_totals[which_block]
            scores, allowed = masked_scores(block_queries, every_key, block_stream, block_segment, stream, segment)
            weights = jnp.where(allowed, jnp.exp(scores - block_log[..., None]), 0.0)
            grad_values = grad_values + jnp.einsum('gjrn,rgjd->ngd', rounded(weights), block_grads)
            grad_weights = jnp.einsum('rgjd,ngd->gjrn', block_grads, every_value.astype(jnp.float32))
            grad_scores = rounded(weights * (grad_weights - block_delta[..., None]))
            grad_queries = jnp.einsum('gjrn,ngd->rgjd', grad_scores, every_key.astype(jnp.float32)) * score_scale
            grad_keys = grad_keys + jnp.einsum('gjrn,rgjd->ngd', grad_scores, block_queries.astype(jnp.float32)) * score_scale
            return ((grad_keys, grad_values), grad_queries)
        key_value_zeros = jnp.zeros((grouped_rows, KEY_VALUE_HEADS, HEAD_SIZE), jnp.float32)
        (grad_keys, grad_values), grad_queries = lax.scan(backward_block, (key_value_zeros, key_value_zeros), jnp.arange(block_count, dtype=jnp.int32))
        grad_queries = rotate_back(grad_queries.reshape(grouped_rows, QUERY_HEADS, HEAD_SIZE), cosine_table, sine_values).reshape(grouped_rows, QUERY_FEATURES)
        grad_keys = rotate_back(grad_keys, cosine_table, sine_values).reshape(grouped_rows, KEY_FEATURES)
        grad_projected = jnp.concatenate([grad_queries, grad_keys, grad_values.reshape(grouped_rows, KEY_FEATURES)], 1).astype(jnp.bfloat16)
        grad_w_qkv = jnp.dot(grad_projected.T, normed_one, preferred_element_type=jnp.float32)
        grad_normed_one = jnp.dot(grad_projected, w_qkv, preferred_element_type=jnp.float32)
        grad_gain_one = lax.optimization_barrier(jnp.sum(grad_normed_one * source * scale_one, 0))
        grad_tokens = grad_residual + norm_back(grad_normed_one, norm_attn, source, scale_one)
        updates = (grad_gain_one, grad_w_qkv, grad_w_out, grad_gain_two, grad_w_gate_up, grad_down)
        new_totals = tuple((total_item + update_item for total_item, update_item in zip(totals, updates)))
        return (new_totals, (result, grad_tokens))
    start_totals = (jnp.zeros((D,), jnp.float32), jnp.zeros((QUERY_FEATURES + 2 * KEY_FEATURES, D), jnp.float32), jnp.zeros((D, QUERY_FEATURES), jnp.float32), jnp.zeros((D,), jnp.float32), jnp.zeros((2 * FF, D), jnp.float32), jnp.zeros((D, FF), jnp.float32))
    inputs = (tokens.reshape(N_DP, grouped_rows, D), cotangent.reshape(N_DP, grouped_rows, D), seq_lengths, block_slot)
    totals, (results, grad_tokens) = lax.scan(group_pass, start_totals, inputs)
    return (results.reshape(TOKENS, D), grad_tokens.reshape(TOKENS, D), totals[0], totals[1], totals[2], totals[3], totals[4], totals[5])
```

```python
import functools
import math

import jax
import jax.numpy as jnp
from jax import lax
from jax.experimental import pallas as pl
from jax.experimental.pallas import tpu as pltpu
from jax.sharding import Mesh
from jax.sharding import PartitionSpec as P

QUERY_HEADS = 16
KEY_VALUE_HEADS = 8
HEAD_SIZE = 96
FF = 4096
BLK = 128
QUERY_FEATURES = 1536
KEY_FEATURES = 768

EPSILON = 1e-05
THETA = 100000.0
MASK_FILL = -1e30
BF = jnp.bfloat16
F32 = jnp.float32
PLANE = ("i", "ctx")
ALL = ("o", "i", "ctx")


def rope_tables(rope_pos):
    half_dim = HEAD_SIZE // 2
    exponent = jnp.arange(half_dim, dtype=F32) * (2.0 / HEAD_SIZE)
    frequency = jnp.power(F32(THETA), -exponent)
    angles = rope_pos.astype(F32)[..., None] * frequency
    return (jnp.cos(angles), jnp.sin(angles))


def rotate(values, cosine, sine):
    half_dim = HEAD_SIZE // 2
    first, second = values[..., :half_dim], values[..., half_dim:]
    return jnp.concatenate([first * cosine - second * sine, second * cosine + first * sine], -1)


def rotate_back(values, cosine, sine):
    return rotate(values, cosine, -sine)


def positions(lengths, slot_table, count_of_rows):
    row_index = jnp.arange(count_of_rows, dtype=jnp.int32)
    slot_of = jnp.repeat(slot_table, BLK)
    stream = slot_of * BLK + row_index % BLK
    seq_ends = jnp.cumsum(lengths)
    passed = stream[:, None] >= seq_ends[None, :]
    segment = jnp.sum(passed.astype(jnp.int32), 1)
    offset = jnp.max(jnp.where(passed, seq_ends[None, :], 0), 1)
    return (stream, segment, stream - offset)


def norm_back(grad_normed, gain, source, scale):
    weighted = grad_normed * gain
    return scale * weighted - source * scale**3 * jnp.mean(weighted * source, -1, keepdims=True)


def nt(a, b):
    return lax.dot_general(a, b, (((1,), (1,)), ((), ())), preferred_element_type=F32)


def nn(a, b):
    return lax.dot_general(a, b, (((1,), (0,)), ((), ())), preferred_element_type=F32)


def tn(a, b):
    return lax.dot_general(a, b, (((0,), (0,)), ((), ())), preferred_element_type=F32)


MESH = pl.DeviceIdType.MESH


def places(n_ctx):
    o, i, c = lax.axis_index("o"), lax.axis_index("i"), lax.axis_index("ctx")
    return o, i, c, c + 1 - 2 * (c % 2), (c + n_ctx // 2) % n_ctx


def greet(devices):
    barrier = pltpu.get_barrier_semaphore()
    for device in devices:
        pl.semaphore_signal(barrier, inc=1, device_id=device, device_id_type=MESH)
    pl.semaphore_wait(barrier, len(devices))


def send(src, dst, send_sem, recv_sem, device):
    copy = pltpu.make_async_remote_copy(
        src_ref=src, dst_ref=dst, send_sem=send_sem, recv_sem=recv_sem, device_id=device, device_id_type=MESH
    )
    copy.start()
    return copy


def gather_kernel(n_ctx, n_arrays, *refs):
    sources, outs = refs[:n_arrays], refs[n_arrays : 2 * n_arrays]
    send_sem, recv_sem, local_sem = refs[2 * n_arrays :]
    o, i, c, mate, far = places(n_ctx)
    j, core = 1 - i, c % 2
    d_mate, d_x, d_y = (o, i, mate), (o, j, c), (o, i, far)
    me, s_x, s_y, s_d = i * n_ctx + c, j * n_ctx + c, i * n_ctx + far, j * n_ctx + far
    greet([d_mate, d_x, d_y])
    relay = (o, j * core + i * (1 - core), c * core + far * (1 - core))
    relayed = s_y * core + s_x * (1 - core)
    copies = []

    def start(a, kind, src, slot, device):
        copy = send(src, outs[a].at[slot], send_sem.at[a, kind], recv_sem.at[a, kind], device)
        copies.append(copy)
        return copy

    first, later = [], []
    for a in range(n_arrays):
        own = pltpu.make_async_copy(sources[a], outs[a].at[me], local_sem.at[a])
        own.start()
        along_x = start(a, 1, sources[a], me, d_x)
        along_y = start(a, 2, sources[a], me, d_y)
        late = [start(a, 0, sources[a], me, d_mate)]
        along_x.wait_recv()
        late.append(start(a, 3, outs[a].at[s_x], s_x, d_mate))
        along_y.wait_recv()
        diagonal = start(a, 5, outs[a].at[relayed], relayed, relay)
        late.append(start(a, 4, outs[a].at[s_y], s_y, d_mate))
        first.append((own, diagonal))
        later += late
    for a, (own, diagonal) in enumerate(first):
        own.wait()
        diagonal.wait_recv()
        later.append(start(a, 6, outs[a].at[s_d], s_d, d_mate))
    for copy in later:
        copy.wait_recv()
    for copy in copies:
        copy.wait_send()


def plane_gather(arrays, n_ctx, number):
    n = len(arrays)
    outs = pl.pallas_call(
        functools.partial(gather_kernel, n_ctx, n),
        out_shape=[jax.ShapeDtypeStruct((2 * n_ctx,) + a.shape, a.dtype) for a in arrays],
        in_specs=[pl.BlockSpec(memory_space=pltpu.VMEM)] * n,
        out_specs=[pl.BlockSpec(memory_space=pl.ANY)] * n,
        scratch_shapes=[
            pltpu.SemaphoreType.DMA((n, 7)),
            pltpu.SemaphoreType.DMA((n, 7)),
            pltpu.SemaphoreType.DMA((n,)),
        ],
        compiler_params=pltpu.CompilerParams(collective_id=number, has_side_effects=True),
        name=f"plane_gather_{number}",
    )(*arrays)
    return [x.reshape(-1, x.shape[-1]) for x in outs]


def scatter_kernel(n_ctx, x_ref, out_ref, from_mate, got, going, send_sem, recv_sem):
    o, i, c, mate, far = places(n_ctx)
    j, core = 1 - i, c % 2
    rows = x_ref.shape[1]
    d_mate, d_x, d_y = (o, i, mate), (o, j, c), (o, i, far)
    greet([d_mate, d_x, d_y])
    far_mate = (mate + n_ctx // 2) % n_ctx
    mine = [j * n_ctx + far, j * n_ctx + c, i * n_ctx + far, i * n_ctx + c]
    theirs = [j * n_ctx + far_mate, j * n_ctx + mate, i * n_ctx + far_mate, i * n_ctx + mate]
    combined = (o, j * (1 - core) + i * core, c * (1 - core) + far * core)
    direct = (o, j * core + i * (1 - core), c * core + far * (1 - core))

    def start(kind, src, dst, device):
        return send(src, dst, send_sem.at[kind], recv_sem.at[kind], device)

    def each(body):
        @pl.loop(0, rows, step=32)
        def _(r):
            body(pl.ds(pl.multiple_of(r, 32), 32))

    mates = [start(n, x_ref.at[theirs[n]], from_mate.at[n], d_mate) for n in range(4)]
    mates[0].wait_recv()

    @each
    def _(r):
        going[0, r] = (x_ref[mine[0], r].astype(F32) + from_mate[0, r].astype(F32)).astype(BF)

    diagonal = start(4, going.at[0], got.at[0], direct)
    mates[1].wait_recv()
    mates[2].wait_recv()
    s_direct = mine[2] * (1 - core) + mine[1] * core
    s_combined = mine[1] * (1 - core) + mine[2] * core

    @each
    def _(r):
        going[1, r] = (x_ref[s_direct, r].astype(F32) + from_mate[2 - core, r].astype(F32)).astype(BF)

    straight = start(5, going.at[1], got.at[1], direct)
    diagonal.wait_recv()

    @each
    def _(r):
        pair = x_ref[s_combined, r].astype(F32) + from_mate[1 + core, r].astype(F32)
        going[2, r] = (pair + got[0, r].astype(F32)).astype(BF)

    joined = start(6, going.at[2], got.at[2], combined)
    mates[3].wait_recv()
    straight.wait_recv()
    joined.wait_recv()

    @each
    def _(r):
        pair = x_ref[mine[3], r].astype(F32) + from_mate[3, r].astype(F32)
        out_ref[r] = pair + got[1, r].astype(F32) + got[2, r].astype(F32)

    for copy in mates + [diagonal, straight, joined]:
        copy.wait_send()


def plane_scatter(x, n_ctx, number):
    n = 2 * n_ctx
    rows, width = x.shape[0] // n, x.shape[1]
    return pl.pallas_call(
        functools.partial(scatter_kernel, n_ctx),
        out_shape=jax.ShapeDtypeStruct((rows, width), F32),
        in_specs=[pl.BlockSpec(memory_space=pltpu.VMEM)],
        out_specs=pl.BlockSpec(memory_space=pltpu.VMEM),
        scratch_shapes=[
            pltpu.VMEM((4, rows, width), BF),
            pltpu.VMEM((3, rows, width), BF),
            pltpu.VMEM((3, rows, width), BF),
            pltpu.SemaphoreType.DMA((7,)),
            pltpu.SemaphoreType.DMA((7,)),
        ],
        compiler_params=pltpu.CompilerParams(collective_id=number, has_side_effects=True),
        name=f"plane_scatter_{number}",
    )(x.reshape(n, rows, width))


def swap_kernel(n_ctx, n_arrays, *refs):
    sources, outs = refs[:n_arrays], refs[n_arrays : 2 * n_arrays]
    send_sem, recv_sem, local_sem = refs[2 * n_arrays :]
    o, i, c, _, _ = places(n_ctx)
    n = 2 * n_ctx
    me = i * n_ctx + c
    others = [(me + k) % n for k in range(1, n)]
    greet([(o, d // n_ctx, d % n_ctx) for d in others])
    copies = []
    for a in range(n_arrays):
        for k, d in enumerate(others):
            copies.append(
                send(
                    sources[a].at[d],
                    outs[a].at[me],
                    send_sem.at[a, k],
                    recv_sem.at[a, k],
                    (o, d // n_ctx, d % n_ctx),
                )
            )
    own = [pltpu.make_async_copy(sources[a].at[me], outs[a].at[me], local_sem.at[a]) for a in range(n_arrays)]
    for copy in own:
        copy.start()
    for copy in copies:
        copy.wait_recv()
        copy.wait_send()
    for copy in own:
        copy.wait()


def plane_swap(arrays, n_ctx, number):
    n = len(arrays)
    return pl.pallas_call(
        functools.partial(swap_kernel, n_ctx, n),
        out_shape=[jax.ShapeDtypeStruct(a.shape, a.dtype) for a in arrays],
        in_specs=[pl.BlockSpec(memory_space=pltpu.VMEM)] * n,
        out_specs=[pl.BlockSpec(memory_space=pltpu.VMEM)] * n,
        scratch_shapes=[
            pltpu.SemaphoreType.DMA((n, 2 * n_ctx - 1)),
            pltpu.SemaphoreType.DMA((n, 2 * n_ctx - 1)),
            pltpu.SemaphoreType.DMA((n,)),
        ],
        compiler_params=pltpu.CompilerParams(collective_id=number, has_side_effects=True),
        name=f"plane_swap_{number}",
    )(*arrays)


def z_ag(x):
    return lax.all_gather(x, "o", axis=0, tiled=True)


def z_rs(x):
    return lax.psum_scatter(x, "o", scatter_dimension=0, tiled=True)


def inv_rms(x):
    return lax.rsqrt(jnp.mean(x * x, -1, keepdims=True) + EPSILON)


def feature_moves(n_outer, n_plane):
    moves = []
    half, quarter = n_outer // 2, n_outer // 4
    for block in range(n_outer * n_plane):
        if block < 4 * n_outer:
            place, step = block // half, block % half
        elif block < 6 * n_outer:
            place, step = divmod(block - 4 * n_outer, quarter)
            step += half
        else:
            place, step = divmod(block - 6 * n_outer, quarter)
            step += half + quarter
        moves.append((block, step * n_plane + place))
    return moves


def make_shards(n_outer, n_inner, n_ctx):
    n_plane = n_inner * n_ctx
    moves = feature_moves(n_outer, n_plane)
    back = [(b, a) for a, b in moves]
    heads = QUERY_HEADS // n_plane
    score_scale = 1.0 / math.sqrt(HEAD_SIZE)

    def shards(tokens, norm_attn, w_qkv, w_out, norm_mlp, w_gate_up, w_down, cotangent, seq_lengths, block_slot):
        rows, width = tokens.shape
        gain_rows = norm_attn.shape[0]
        feature_rows = w_qkv.shape[0]
        out_rows = w_out.shape[0]
        unit_rows = w_gate_up.shape[0]
        n_seqs = seq_lengths.shape[1]
        group_rows = n_ctx * rows
        out_parts = w_out.reshape(out_rows, n_plane, -1).transpose(1, 0, 2)
        down_parts = (
            w_down.reshape(out_rows, n_outer // 2, n_plane, unit_rows).transpose(2, 0, 1, 3).reshape(n_plane, out_rows, -1)
        )
        gain_part = jnp.pad(jnp.stack([norm_attn, norm_mlp]), ((0, 6), (0, 128 - gain_rows)))
        meta = jnp.concatenate([seq_lengths[0], block_slot[0]])
        meta = jnp.pad(meta[None], ((0, 7), (0, 128 - meta.shape[0])))
        out_parts, down_parts, gain_parts, metas = plane_swap(
            [out_parts, down_parts] + [jnp.broadcast_to(part, (n_plane, 8, 128)) for part in (gain_part, meta)], n_ctx, 0
        )
        stream, segment, rope_pos = jax.vmap(
            lambda m: positions(m[:n_seqs], m[n_seqs : n_seqs + block_slot.shape[1]], group_rows)
        )(metas[::n_ctx, 0])
        cosine, sine = rope_tables(rope_pos)
        gain_parts = gain_parts[:, :2, :gain_rows]
        gain_high = lax.reduce_precision(gain_parts, 8, 7)
        gain_row = jnp.stack([gain_high, gain_parts - gain_high]).astype(BF).reshape(1, -1)
        gain_row = jnp.pad(gain_row, ((0, 15), (0, width - gain_row.shape[1])))
        sent = jnp.concatenate(
            [lax.ppermute(w_qkv, ALL, moves), out_parts.reshape(out_rows, -1), gain_row], 0
        )
        got = z_ag(sent).reshape(n_outer, -1, width)
        qkv = got[:, :feature_rows].reshape(-1, width)
        out_w = got[:, feature_rows : feature_rows + out_rows].reshape(n_outer * n_plane * out_rows, -1)
        gains = got[:, feature_rows + out_rows, : 4 * n_plane * gain_rows].astype(F32)
        gains = gains.reshape(n_outer, 2, n_plane, 2, gain_rows).sum(1).transpose(2, 0, 1, 3).reshape(2, width)
        gain_one, gain_two = gains[0], gains[1]
        sent = jnp.concatenate([w_gate_up, down_parts.reshape(-1, width)], 0)
        got = z_ag(sent).reshape(n_outer, -1, width)
        gate_up = got[:, :unit_rows].reshape(-1, width)
        down_w = got[:, unit_rows:].reshape(width, -1)
        units = down_w.shape[1]
        source = tokens.astype(F32)
        scale_one = inv_rms(source)
        x_all, dy_all = plane_gather([tokens, cotangent], n_ctx, 1)
        x_all_f = x_all.astype(F32)
        xn1 = (x_all_f * inv_rms(x_all_f) * gain_one).astype(BF)
        proj = nt(xn1, qkv).reshape(n_inner, group_rows, -1)
        qf = heads * HEAD_SIZE
        c4, s4 = cosine[:, :, None], sine[:, :, None]
        q = rotate(proj[..., :qf].reshape(n_inner, group_rows, heads, HEAD_SIZE), c4, s4).astype(BF)
        k = rotate(proj[..., qf : qf + HEAD_SIZE], cosine, sine).astype(BF)
        v = proj[..., qf + HEAD_SIZE :].astype(BF)
        allowed = ((segment[:, :, None] == segment[:, None, :]) & (stream[:, None, :] <= stream[:, :, None]))[:, None]

        def score_of():
            s = jnp.einsum("gqhd,gkd->ghqk", q, k, preferred_element_type=F32) * score_scale
            return jnp.where(allowed, s, MASK_FILL)

        s = score_of()
        high = jnp.max(s, -1, keepdims=True)
        e = jnp.where(allowed, jnp.exp(s - high), 0.0)
        total = jnp.sum(e, -1, keepdims=True)
        lse = high + jnp.log(total)
        p = (e / total).astype(BF)
        attn = jnp.einsum("ghqk,gkd->gqhd", p, v, preferred_element_type=F32).astype(BF)
        attn_flat = attn.reshape(n_inner * group_rows, qf)
        out_term = plane_scatter(nt(attn_flat, out_w).astype(BF), n_ctx, 2)
        residual = source + out_term
        scale_two = inv_rms(residual)
        xn2 = plane_gather([(residual * scale_two * gain_two).astype(BF)], n_ctx, 3)[0]
        gu = nt(xn2, gate_up)
        gate, up = gu[:, :units], gu[:, units:]
        sg = jax.nn.sigmoid(gate)
        hidden = (gate * sg * up).astype(BF)
        result = (residual + plane_scatter(nt(hidden, down_w).astype(BF), n_ctx, 6)).astype(BF)
        dhid = nn(dy_all, down_w)
        dgu = jnp.concatenate([dhid * up * sg * (1.0 + gate * (1.0 - sg)), dhid * gate * sg], 1).astype(BF)
        g_down = z_rs(tn(dy_all, hidden).astype(BF))
        grad_gate_up = z_rs(tn(dgu, xn2).astype(BF)).astype(F32)
        dxn2 = plane_scatter(nn(dgu, gate_up).astype(BF), n_ctx, 4)
        grad_gain_two = jnp.sum(dxn2 * residual * scale_two, 0)
        dh1 = cotangent.astype(F32) + norm_back(dxn2, gain_two, residual, scale_two)
        dh1_all = plane_gather([dh1.astype(BF)], n_ctx, 5)[0]
        dattn = nn(dh1_all, out_w).astype(BF)
        g_out = z_rs(tn(dh1_all, attn_flat).astype(BF))
        da = dattn.reshape(n_inner, group_rows, heads, HEAD_SIZE)
        delta = jnp.sum(da.astype(F32) * attn.astype(F32), -1).transpose(0, 2, 1)[..., None]
        pf = jnp.where(allowed, jnp.exp(score_of() - lse), 0.0)
        dv = jnp.einsum("ghqk,gqhd->gkd", pf.astype(BF), da, preferred_element_type=F32)
        dpf = jnp.einsum("gqhd,gkd->ghqk", da, v, preferred_element_type=F32)
        ds = (pf * (dpf - delta)).astype(BF)
        dq = jnp.einsum("ghqk,gkd->gqhd", ds, k, preferred_element_type=F32) * score_scale
        dk = jnp.einsum("ghqk,gqhd->gkd", ds, q, preferred_element_type=F32) * score_scale
        dq = rotate_back(dq, c4, s4).reshape(n_inner, group_rows, qf)
        dk = rotate_back(dk, cosine, sine)
        dproj = jnp.concatenate([dq, dk, dv], -1).astype(BF).reshape(n_inner * group_rows, -1)
        g_qkv = z_rs(tn(dproj, xn1).astype(BF))
        grad_qkv = lax.ppermute(g_qkv, ALL, back).astype(F32)
        dxn1 = plane_scatter(nn(dproj, qkv).astype(BF), n_ctx, 7)
        grad_gain_one = jnp.sum(dxn1 * source * scale_one, 0)
        grad_input = dh1 + norm_back(dxn1, gain_one, source, scale_one)
        g_gain = jnp.stack([grad_gain_one, grad_gain_two]).reshape(2, n_outer, n_plane, gain_rows)
        g_gain = g_gain.transpose(2, 1, 0, 3).reshape(n_plane, 2 * n_outer, gain_rows)
        g_gain = jnp.pad(g_gain, ((0, 0), (0, 0), (0, 128 - gain_rows)))
        g_out, g_down, g_gain = plane_swap(
            [g_out.reshape(n_plane, out_rows, -1), g_down.reshape(n_plane, out_rows, -1), g_gain], n_ctx, 8
        )
        grad_out = g_out.transpose(1, 0, 2).reshape(out_rows, -1).astype(F32)
        grad_down = g_down.reshape(n_plane, out_rows, n_outer // 2, unit_rows).transpose(1, 2, 0, 3)
        grad_down = grad_down.reshape(out_rows, -1).astype(F32)
        g = lax.psum_scatter(jnp.sum(g_gain, 0).reshape(n_outer, 2, 128), "o", scatter_dimension=0, tiled=True)
        g = g[0, :, :gain_rows]
        return (result, grad_input, g[0], grad_qkv, grad_out, g[1], grad_gate_up, grad_down)

    return shards


def solution(mesh):
    n_inner = 2
    n_ctx = mesh.shape["ctx"]
    n_outer = mesh.shape["dp"] // n_inner
    split = Mesh(mesh.devices.reshape(n_outer, n_inner, n_ctx), ALL)
    rows, vec, grp = P(ALL, None), P(ALL), P(("o", "i"), None)
    return jax.shard_map(
        make_shards(n_outer, n_inner, n_ctx),
        mesh=split,
        in_specs=(rows, vec, rows, rows, vec, rows, rows, rows, grp, grp),
        out_specs=(rows, rows, vec, rows, rows, vec, rows, rows),
        check_vma=False,
    )
```

```python
import functools
import math

import jax
import jax.numpy as jnp
import numpy as np
from jax import lax
from jax.experimental import pallas as pl
from jax.experimental.pallas import tpu as pltpu
from jax.sharding import Mesh
from jax.sharding import PartitionSpec as P

QUERY_HEADS = 16
KEY_VALUE_HEADS = 8
HEAD_SIZE = 96
FF = 4096
BLK = 128
LANES = 128
QUERY_BLOCK = 512
CHUNKS = 4

EPSILON = 1e-05
THETA = 100000.0
MASK_FILL = -1e30
BF = jnp.bfloat16
F32 = jnp.float32
ALL = ("o", "i", "ctx")
MESH = pl.DeviceIdType.MESH
SCALE = 1.0 / math.sqrt(HEAD_SIZE)


def nt(a, b):
    return lax.dot_general(a, b, (((1,), (1,)), ((), ())), preferred_element_type=F32)


def nn(a, b):
    return lax.dot_general(a, b, (((1,), (0,)), ((), ())), preferred_element_type=F32)


def tn(a, b):
    return lax.dot_general(a, b, (((0,), (0,)), ((), ())), preferred_element_type=F32)


def z_ag(x):
    return lax.all_gather(x, "o", axis=0, tiled=True)


def z_rs(x):
    return lax.psum_scatter(x, "o", scatter_dimension=0, tiled=True)


def inv_rms(x):
    return lax.rsqrt(jnp.mean(x * x, -1, keepdims=True) + EPSILON)


def norm_back(grad_normed, gain, source, scale):
    weighted = grad_normed * gain
    return scale * weighted - source * scale**3 * jnp.mean(weighted * source, -1, keepdims=True)


def feature_moves(n_outer, n_plane):
    moves = []
    half, quarter = n_outer // 2, n_outer // 4
    for block in range(n_outer * n_plane):
        if block < 4 * n_outer:
            place, step = block // half, block % half
        elif block < 6 * n_outer:
            place, step = divmod(block - 4 * n_outer, quarter)
            step += half
        else:
            place, step = divmod(block - 6 * n_outer, quarter)
            step += half + quarter
        moves.append((block, step * n_plane + place))
    return moves


def pad_heads(x, axis):
    half = HEAD_SIZE // 2
    shape = x.shape
    x = x.reshape(shape[:axis] + (-1, half) + shape[axis + 1 :])
    pads = [(0, 0)] * x.ndim
    pads[axis + 1] = (0, LANES // 2 - half)
    return jnp.pad(x, pads).reshape(shape[:axis] + (-1,) + shape[axis + 1 :])


def cut_heads(x, axis):
    half = HEAD_SIZE // 2
    shape = x.shape
    x = x.reshape(shape[:axis] + (-1, LANES // 2) + shape[axis + 1 :])
    x = lax.slice_in_dim(x, 0, half, axis=axis + 1)
    return x.reshape(shape[:axis] + (-1,) + shape[axis + 1 :])


def pack_down(w, chunks):
    width, units = w.shape
    span = width // units
    w = w.reshape(chunks, span, width // (chunks * span), units)
    return w.transpose(0, 2, 1, 3).reshape(chunks, -1, width)


def in_chunks(weights, unit_rows, units):
    n_outer, _, width = weights.shape
    if n_outer == CHUNKS:
        return weights
    gate_up = weights[:, :unit_rows].reshape(CHUNKS, -1, width)
    down = weights[:, unit_rows:].reshape(n_outer, -1, width // units, units).transpose(0, 2, 1, 3)
    return jnp.concatenate([gate_up, pack_down(down.reshape(width, units), CHUNKS)], 1)


def places(n_ctx):
    o, i, c = lax.axis_index("o"), lax.axis_index("i"), lax.axis_index("ctx")
    return o, i, c, c + 1 - 2 * (c % 2), (c + n_ctx // 2) % n_ctx


def greet(devices):
    barrier = pltpu.get_barrier_semaphore()
    for device in devices:
        pl.semaphore_signal(barrier, inc=1, device_id=device, device_id_type=MESH)
    pl.semaphore_wait(barrier, len(devices))


def greet_neighbours(n_ctx):
    o, i, c, mate, far = places(n_ctx)
    greet([(o, i, mate), (o, 1 - i, c), (o, i, far)])


def send(src, dst, send_sem, recv_sem, device):
    copy = pltpu.make_async_remote_copy(
        src_ref=src, dst_ref=dst, send_sem=send_sem, recv_sem=recv_sem, device_id=device, device_id_type=MESH
    )
    copy.start()
    return copy


class Gather:
    def __init__(self, n_ctx, src, out, send_sem, recv_sem, local_sem):
        self.src, self.out, self.sems = src, out, (send_sem, recv_sem, local_sem)
        o, i, c, mate, far = places(n_ctx)
        j, core = 1 - i, c % 2
        self.mate, self.x, self.y = (o, i, mate), (o, j, c), (o, i, far)
        self.me, self.s_x = i * n_ctx + c, j * n_ctx + c
        self.s_y, self.s_d = i * n_ctx + far, j * n_ctx + far
        self.relay = (o, j * core + i * (1 - core), c * core + far * (1 - core))
        self.relayed = self.s_y * core + self.s_x * (1 - core)
        mate_far = (mate + n_ctx // 2) % n_ctx
        self.mates_slots = [i * n_ctx + mate, j * n_ctx + mate, i * n_ctx + mate_far, j * n_ctx + mate_far]
        self.copies = {}

    def go(self, kind, src, slot, device):
        copy = send(src, self.out.at[slot], self.sems[0].at[kind], self.sems[1].at[kind], device)
        self.copies[kind] = copy

    def begin(self):
        self.go(1, self.src, self.me, self.x)
        self.go(2, self.src, self.me, self.y)
        self.go(0, self.src, self.me, self.mate)
        self.own = pltpu.make_async_copy(self.src, self.out.at[self.me], self.sems[2])
        self.own.start()

    def middle(self):
        self.copies[1].wait_recv()
        self.copies[2].wait_recv()
        self.go(5, self.out.at[self.relayed], self.relayed, self.relay)
        self.go(3, self.out.at[self.s_x], self.s_x, self.mate)
        self.go(4, self.out.at[self.s_y], self.s_y, self.mate)

    def corner(self):
        self.copies[5].wait_recv()
        self.go(6, self.out.at[self.s_d], self.s_d, self.mate)

    def arrived(self, kind):
        self.copies[kind].wait_recv()

    def sent(self):
        self.own.wait()
        for copy in self.copies.values():
            copy.wait_send()

    def end(self):
        self.corner()
        for kind in (0, 3, 4, 6):
            self.arrived(kind)
        self.sent()


GATHER_SEMS = [pltpu.SemaphoreType.DMA((7,)), pltpu.SemaphoreType.DMA((7,)), pltpu.SemaphoreType.DMA]


class Scatter:
    def __init__(self, n_ctx, partial, tile, ready, from_mate, going, got, send_sem, recv_sem, total):
        self.partial, self.tile = partial, tile
        self.ready, self.from_mate, self.going, self.got = ready, from_mate, going, got
        self.sems, self.total = (send_sem, recv_sem), total
        o, i, c, mate, far = places(n_ctx)
        j, core = 1 - i, c % 2
        self.core = core
        far_mate = (mate + n_ctx // 2) % n_ctx
        self.mine = [j * n_ctx + far, j * n_ctx + c, i * n_ctx + far, i * n_ctx + c]
        self.theirs = [j * n_ctx + far_mate, j * n_ctx + mate, i * n_ctx + far_mate, i * n_ctx + mate]
        self.mate = (o, i, mate)
        self.combined = (o, j * (1 - core) + i * core, c * (1 - core) + far * core)
        self.direct = (o, j * core + i * (1 - core), c * core + far * (1 - core))
        self.s_direct = self.mine[2] * (1 - core) + self.mine[1] * core
        self.s_combined = self.mine[1] * (1 - core) + self.mine[2] * core
        self.copies = []

    def go(self, kind, part, src, dst, device):
        copy = send(src.at[part], dst.at[part], self.sems[0].at[kind, part], self.sems[1].at[kind, part], device)
        self.copies.append(copy)
        return copy

    def each(self, part, body):
        tiles = self.ready.shape[-1] // self.tile

        @pl.loop(0, tiles)
        def _(t):
            at = pl.multiple_of(t * self.tile, self.tile)
            body(part * tiles + t, pl.ds(at, self.tile), pl.ds(part * tiles * self.tile + at, self.tile))

    def fill(self, n, part):
        def body(t, lanes, _):
            self.ready[n, part, :, lanes] = self.partial(self.theirs[n], t).astype(BF)

        self.each(part, body)

    def give(self, n, part):
        self.mates[n, part] = self.go(n, part, self.ready.at[n], self.from_mate.at[n], self.mate)

    def pair(self, slot, n, part, place):
        def body(t, lanes, _):
            pair = self.partial(slot, t) + self.from_mate[n, part, :, lanes].astype(F32)
            self.going[place, part, :, lanes] = pair.astype(BF)

        self.each(part, body)

    def to_mate(self):
        self.mates, self.straights, self.diagonals, self.joins = {}, [], [], []
        order = [(0, 0), (0, 1), (1, 0), (2, 0), (1, 1), (2, 1), (3, 0), (3, 1)]
        self.fill(*order[0])
        for k, at in enumerate(order[1:]):
            self.fill(*at)
            self.give(*order[k])
            if k == 2:
                self.mates[0, 0].wait_recv()
                self.pair(self.mine[0], 0, 0, 0)
            if k == 3:
                self.diagonals.append(self.go(4, 0, self.going.at[0], self.got.at[0], self.direct))
                self.mates[0, 1].wait_recv()
                self.pair(self.mine[0], 0, 1, 0)
            if k == 4:
                self.diagonals.append(self.go(4, 1, self.going.at[0], self.got.at[0], self.direct))
        self.last = order[-1]

    def pairs(self):
        for part in range(PARTS):
            self.mates[1, part].wait_recv()
            self.mates[2, part].wait_recv()
            self.pair(self.s_direct, 2 - self.core, part, 1)
            if part == 0:
                self.give(*self.last)
            else:
                self.straights.append(self.go(5, part - 1, self.going.at[1], self.got.at[1], self.direct))

    def join(self):
        for part in range(PARTS):
            self.diagonals[part].wait_recv()

            def combined(t, lanes, _):
                pair = self.partial(self.s_combined, t) + self.from_mate[1 + self.core, part, :, lanes].astype(F32)
                self.going[2, part, :, lanes] = (pair + self.got[0, part, :, lanes].astype(F32)).astype(BF)

            self.each(part, combined)
            if part == 0:
                self.straights.append(self.go(5, PARTS - 1, self.going.at[1], self.got.at[1], self.direct))
            else:
                self.joins.append(self.go(6, part - 1, self.going.at[2], self.got.at[2], self.combined))
        self.own(0)
        self.joins.append(self.go(6, PARTS - 1, self.going.at[2], self.got.at[2], self.combined))

    def own(self, part):
        self.mates[3, part].wait_recv()

        def body(t, lanes, out):
            self.total[:, out] = self.partial(self.mine[3], t) + self.from_mate[3, part, :, lanes].astype(F32)

        self.each(part, body)

    def end(self):
        total = self.total
        for part in range(1, PARTS):
            self.own(part)
        for part in range(PARTS):
            self.straights[part].wait_recv()
            self.joins[part].wait_recv()

            def rest(t, lanes, out):
                other = self.got[1, part, :, lanes].astype(F32) + self.got[2, part, :, lanes].astype(F32)
                total[:, out] = total[:, out] + other

            self.each(part, rest)
        for copy in self.copies:
            copy.wait_send()


PARTS = 2


def scatter_scratch(rows, width):
    return [
        pltpu.VMEM((4, PARTS, rows, width // PARTS), BF),
        pltpu.VMEM((4, PARTS, rows, width // PARTS), BF),
        pltpu.VMEM((3, PARTS, rows, width // PARTS), BF),
        pltpu.VMEM((3, PARTS, rows, width // PARTS), BF),
        pltpu.SemaphoreType.DMA((7, PARTS)),
        pltpu.SemaphoreType.DMA((7, PARTS)),
        pltpu.VMEM((rows, width), F32),
    ]


def row_chunks(rows, step, body):
    @pl.loop(0, rows // step)
    def _(r):
        body(pl.ds(pl.multiple_of(r * step, step), step))


class Load:
    def __init__(self, parts, sem):
        self.copies = [pltpu.make_async_copy(src, dst, sem.at[n]) for n, (src, dst) in enumerate(parts)]

    def begin(self):
        for copy in self.copies:
            copy.start()
        return self

    def wait(self):
        for copy in self.copies:
            copy.wait()


IN_VMEM = pl.BlockSpec(memory_space=pltpu.VMEM)
ANYWHERE = pl.BlockSpec(memory_space=pl.ANY)


def remote_call(kernel, name, number, ins, outs, scratch, any_outs=(), any_ins=()):
    return pl.pallas_call(
        kernel,
        out_shape=outs,
        in_specs=[ANYWHERE if n in any_ins else IN_VMEM for n in range(len(ins))],
        out_specs=[ANYWHERE if n in any_outs else IN_VMEM for n in range(len(outs))],
        scratch_shapes=scratch,
        compiler_params=pltpu.CompilerParams(collective_id=number, has_side_effects=True, vmem_limit_bytes=60 << 20),
        name=name,
    )(*ins)


def shape(dims, dtype):
    return jax.ShapeDtypeStruct(tuple(dims), dtype)


class Swap:
    def __init__(self, n_ctx, pairs, send_sem, recv_sem, local_sem):
        self.pairs, self.sems = pairs, (send_sem, recv_sem, local_sem)
        self.o, i, c, _, _ = places(n_ctx)
        self.n, self.n_ctx = 2 * n_ctx, n_ctx
        self.me = i * n_ctx + c
        self.others = [(self.me + k) % self.n for k in range(1, self.n)]
        self.devices = [(self.o, d // n_ctx, d % n_ctx) for d in self.others]

    def begin(self):
        self.copies, self.own = [], []
        for a, (src, dst) in enumerate(self.pairs):
            for k, (d, device) in enumerate(zip(self.others, self.devices)):
                self.copies.append(
                    send(src.at[d], dst.at[self.me], self.sems[0].at[a, k], self.sems[1].at[a, k], device)
                )
            own = pltpu.make_async_copy(src.at[self.me], dst.at[self.me], self.sems[2].at[a])
            own.start()
            self.own.append(own)

    def end(self):
        for copy in self.copies:
            copy.wait_recv()
            copy.wait_send()
        for copy in self.own:
            copy.wait()


def swap_sems(n_arrays, n_ctx):
    return [
        pltpu.SemaphoreType.DMA((n_arrays, 2 * n_ctx - 1)),
        pltpu.SemaphoreType.DMA((n_arrays, 2 * n_ctx - 1)),
        pltpu.SemaphoreType.DMA((n_arrays,)),
    ]


def outer_peers(n_outer):
    o, i, c = lax.axis_index("o"), lax.axis_index("i"), lax.axis_index("ctx")
    return [(lax.rem(o + k, n_outer), i, c) for k in range(1, n_outer)]


def rotary_constants():
    frequency = THETA ** -(np.arange(HEAD_SIZE // 2) * (2.0 / HEAD_SIZE))
    rates = np.zeros((8, LANES), np.float32)
    for half, sign in ((0, -1.0), (LANES // 2, 1.0)):
        rates[0, half : half + HEAD_SIZE // 2] = frequency
        rates[1, half : half + HEAD_SIZE // 2] = sign
    angles = np.arange(BLK)[:, None] * rates[0].astype(np.float64)
    return rates, np.stack([np.cos(angles), np.sin(angles)]).astype(np.float32)


def exchange(meta, gains, n_outer, n_ctx, number):
    n = 2 * n_ctx

    def kernel(meta_ref, gains_ref, metas_out, gains_out, send_sem, recv_sem, local_sem):
        o, i, c, _, _ = places(n_ctx)
        me = i * n_ctx + c
        plane = [lax.rem(me + k, n) for k in range(1, n)]
        plane = [(o, d // n_ctx, d % n_ctx) for d in plane]
        peers = outer_peers(n_outer)
        greet(plane + peers)
        first, second, later = [], [], []
        for k, device in enumerate(plane):
            first.append(send(gains_ref, gains_out.at[o, me], send_sem.at[0, k], recv_sem.at[0, k], device))
        own = [
            pltpu.make_async_copy(gains_ref, gains_out.at[o, me], local_sem.at[0]),
            pltpu.make_async_copy(meta_ref, metas_out.at[me], local_sem.at[1]),
        ]
        for copy in own:
            copy.start()
        for k, device in enumerate(plane):
            later.append(send(meta_ref, metas_out.at[me], send_sem.at[1, k], recv_sem.at[1, k], device))
        for copy in own:
            copy.wait()
        for copy in first:
            copy.wait_recv()
        for k, device in enumerate(peers):
            second.append(send(gains_out.at[o], gains_out.at[o], send_sem.at[2, k], recv_sem.at[2, k], device))
        for copy in second + later:
            copy.wait_recv()
        for copy in first + second + later:
            copy.wait_send()

    outs = [shape((n,) + meta.shape, meta.dtype), shape((n_outer, n) + gains.shape, F32)]
    most = max(n, n_outer) - 1
    sems = [pltpu.SemaphoreType.DMA((3, most)), pltpu.SemaphoreType.DMA((3, most)), pltpu.SemaphoreType.DMA((2,))]
    return remote_call(kernel, "exchange", number, [meta, gains], outs, sems)


def prologue(xn, outs_parts, down_parts, metas, n_seqs, n_ctx, number):
    rows, width = xn.shape
    n = 2 * n_ctx
    blocks = n_ctx * rows // BLK

    def kernel(
        x_ref,
        out_src,
        down_src,
        metas_ref,
        rates_ref,
        angles_ref,
        xn_all,
        out_dst,
        down_dst,
        cos_ref,
        sin_ref,
        rows_ref,
        columns_ref,
        *sems,
    ):
        out_swap = Swap(n_ctx, [(out_src, out_dst), (down_src, down_dst)], *sems[:3])
        gather = Gather(n_ctx, x_ref, xn_all, *sems[3:6])
        greet(out_swap.devices)
        gather.begin()
        lane = lax.broadcasted_iota(jnp.int32, (BLK, LANES), 1)
        row = lax.broadcasted_iota(jnp.int32, (BLK, LANES), 0)
        rows_ref[...] = jnp.zeros_like(rows_ref)
        pieces = 2 * blocks * n_seqs
        piece = lax.broadcasted_iota(jnp.int32, (pieces, LANES), 0)
        bases = jnp.zeros((pieces, LANES), jnp.int32)
        places_of = []
        for g in range(2):
            starts, end = [], jnp.zeros((1, 1), jnp.int32)
            for q in range(n_seqs):
                starts.append(end)
                end = end + metas_ref[g * n_ctx, 0:1, q : q + 1]
            for b in range(blocks):
                first = metas_ref[g * n_ctx, 0:1, n_seqs + b : n_seqs + b + 1] * BLK
                for q in range(n_seqs):
                    index = (g * blocks + b) * n_seqs + q
                    bases = jnp.where(piece == index, first - starts[q], bases)
                places_of.append((first, starts))
        angle = bases.astype(F32) * rates_ref[0:1]
        base_cos, base_sin = jnp.cos(angle), jnp.sin(angle)
        for n_block, (first, starts) in enumerate(places_of):
            at = slice(n_block * BLK, (n_block + 1) * BLK)
            stream, lanes_stream = first + row, first + lane[0:1]
            start, lanes_start = jnp.zeros_like(stream), jnp.zeros_like(lanes_stream)
            cos, sin = angles_ref[0], angles_ref[1]
            for q in range(n_seqs):
                index = n_block * n_seqs + q
                cos_0, sin_0 = base_cos[index : index + 1], base_sin[index : index + 1]
                cos_q = cos_0 * angles_ref[0] - sin_0 * angles_ref[1]
                sin_q = sin_0 * angles_ref[0] + cos_0 * angles_ref[1]
                inside = stream >= starts[q]
                start = jnp.where(inside, starts[q], start)
                lanes_start = jnp.where(lanes_stream >= starts[q], starts[q], lanes_start)
                cos, sin = jnp.where(inside, cos_q, cos), jnp.where(inside, sin_q, sin)
            cos_ref[at] = cos
            sin_ref[at] = sin * rates_ref[1:2]
            columns_ref[at] = jnp.where(lane == 0, stream, start)
            rows_ref[0:1, at] = lanes_stream
            rows_ref[1:2, at] = lanes_start
        gather.middle()
        out_swap.begin()
        gather.end()
        out_swap.end()

    outs = [
        shape((n, rows, width), BF),
        shape(outs_parts.shape, BF),
        shape(down_parts.shape, BF),
        shape((n * rows, LANES), F32),
        shape((n * rows, LANES), F32),
        shape((8, n * rows), jnp.int32),
        shape((n * rows, LANES), jnp.int32),
    ]
    rates, angles = rotary_constants()
    ins = [xn, outs_parts, down_parts, metas, jnp.asarray(rates), jnp.asarray(angles)]
    return remote_call(kernel, "prologue", number, ins, outs, swap_sems(2, n_ctx) + GATHER_SEMS, any_outs=(0,))


def plane_gather(x, n_ctx, number):
    def kernel(src, out, *sems):
        gather = Gather(n_ctx, src, out, *sems)
        greet_neighbours(n_ctx)
        gather.begin()
        gather.middle()
        gather.end()

    outs = [shape((2 * n_ctx,) + x.shape, x.dtype)]
    got = remote_call(kernel, f"gather_{number}", number, [x], outs, GATHER_SEMS, any_outs=(0,))
    return got[0].reshape(-1, x.shape[-1])


def rotate(x, cosine, sine):
    return x * cosine + pltpu.roll(x, LANES // 2, 1) * sine


def padded_loads(w_ref, w_pad):
    half = HEAD_SIZE // 2
    rows = w_ref.shape[1]
    pairs, at = [], 0
    for row in range(half, w_pad.shape[0], LANES // 2):
        w_pad[row : row + LANES // 2 - half] = jnp.zeros((LANES // 2 - half, w_pad.shape[1]), BF)
    for n in range(w_ref.shape[0]):
        for b in range(rows // half):
            src = w_ref.at[n, pl.ds(b * half, half)]
            pairs.append((src, w_pad.at[pl.ds(at * LANES // 2, half)]))
            at += 1
    return pairs


def attention_forward(xn, w, cosine, sine, pos_rows, pos_columns, dy, n_ctx, number):
    rows, width = xn.shape
    group = rows // 2
    heads = QUERY_HEADS // (2 * n_ctx)
    features = (heads + 2) * LANES
    k_at, v_at = heads * LANES, (heads + 1) * LANES
    block = min(QUERY_BLOCK, group)
    n_loads = w.shape[0] * w.shape[1] // (HEAD_SIZE // 2)

    def kernel(
        xn_ref, w_hbm, cos_ref, sin_ref, rows_ref, columns_ref, dy_ref, qkv_ref, attn_ref, lse_ref, dy_all, w_ref, load_sem, *sems
    ):
        gather = Gather(n_ctx, dy_ref, dy_all, *sems)
        load = Load(padded_loads(w_hbm, w_ref), load_sem).begin()
        greet_neighbours(n_ctx)
        gather.begin()
        load.wait()

        def project(r):
            cos, sin = cos_ref[r], sin_ref[r]
            for h in range(heads + 2):
                lanes = slice(h * LANES, (h + 1) * LANES)
                part = nt(xn_ref[r], w_ref[lanes])
                qkv_ref[r, lanes] = (rotate(part, cos, sin) if h <= heads else part).astype(BF)

        def attend(g):
            keys_at = pl.ds(g * group, group)

            @pl.loop(0, group // block)
            def _(b):
                r = pl.ds(pl.multiple_of(g * group + b * block, block), block)
                key_pos = rows_ref[0:1, keys_at]
                ok = (key_pos >= columns_ref[r, 1:2]) & (key_pos <= columns_ref[r, 0:1])
                for h in range(heads):
                    lanes = slice(h * LANES, (h + 1) * LANES)
                    s = nt(qkv_ref[r, lanes], qkv_ref[keys_at, k_at : k_at + LANES])
                    s = jnp.where(ok, s, MASK_FILL)
                    high = jnp.max(s, -1, keepdims=True)
                    e = jnp.exp((s - high) * SCALE)
                    total = jnp.sum(e, -1, keepdims=True)
                    mixed = nn(e.astype(BF), qkv_ref[keys_at, v_at : v_at + LANES])
                    attn_ref[r, lanes] = (mixed / total).astype(BF)
                    lse = jnp.broadcast_to(high * SCALE + jnp.log(total), (block, LANES))
                    lse_ref[h : h + 1, r] = jnp.transpose(lse)[0:1]

        row_chunks(rows, block, project)
        attend(0)
        gather.middle()
        attend(1)
        gather.end()

    outs = [
        shape((rows, features), BF),
        shape((rows, heads * LANES), BF),
        shape((8, rows), F32),
        shape((2 * n_ctx,) + dy.shape, BF),
    ]
    ins = [xn, w, cosine, sine, pos_rows, pos_columns, dy]
    scratch = [pltpu.VMEM((features, width), BF), pltpu.SemaphoreType.DMA((n_loads,))] + GATHER_SEMS
    got = remote_call(kernel, "attention_forward", number, ins, outs, scratch, any_outs=(3,), any_ins=(1,))
    return got[0], got[1], got[2], got[3].reshape(rows, width)


def out_loads(w_ref, w_pad):
    features = w_pad.shape[1]
    chunks, _, width = w_ref.shape
    rows = features // chunks
    span = width // features
    pairs = []
    for n in range(chunks):
        for b in range(span):
            dst = w_pad.at[pl.ds((n * span + b) * rows, rows)]
            pairs.append((w_ref.at[n, pl.ds(0, rows), pl.ds(b * features, features)], dst))
    return pairs


def output_projection(attn, out_w, tokens, gain, n_ctx, number):
    rows, width = tokens.shape
    tile = 256

    features = attn.shape[1]

    def kernel(attn_ref, w_hbm, x_ref, gain_ref, h_ref, xn_ref, w_ref, load_sem, *scratch):
        total = scratch[-1]
        load = Load(out_loads(w_hbm, w_ref), load_sem).begin()

        def partial(slot, t):
            a = attn_ref[pl.ds(pl.multiple_of(slot * rows, rows), rows)]
            return nt(a, w_ref[pl.ds(pl.multiple_of(t * tile, tile), tile)])

        scatter = Scatter(n_ctx, partial, tile, *scratch)
        greet_neighbours(n_ctx)
        load.wait()
        scatter.to_mate()
        scatter.pairs()
        scatter.join()
        scatter.end()

        def finish(r):
            h = x_ref[r].astype(F32) + total[r]
            h_ref[r] = h
            xn_ref[r] = (h * inv_rms(h) * gain_ref[1:2]).astype(BF)

        row_chunks(rows, 32, finish)

    outs = [shape((rows, width), F32), shape((rows, width), BF)]
    n_loads = out_w.shape[0] * width // features
    scratch = [pltpu.VMEM((width, features), BF), pltpu.SemaphoreType.DMA((n_loads,))] + scatter_scratch(rows, width)
    return remote_call(kernel, "output_projection", number, [attn, out_w, tokens, gain], outs, scratch, any_ins=(1,))


def feed_forward(xn, dy, weights, unit_rows, number_of_units):
    rows, width = xn.shape
    n_outer = weights.shape[0]
    block = 256
    pack = weights.shape[1] - unit_rows
    span = width // number_of_units

    def kernel(x_ref, dy_ref, w_ref, hidden_ref, dgu_ref):
        x, dy = x_ref[...], dy_ref[...]
        half = n_outer // 2
        for n in range(half):
            lanes = slice(n * unit_rows, (n + 1) * unit_rows)
            gate = nt(x, w_ref[n, :unit_rows])
            up = nt(x, w_ref[half + n, :unit_rows])
            dhid = jnp.zeros_like(gate)
            for m in range(n_outer):
                for b in range(span):
                    at = (m * span + b) * pack
                    u = b * number_of_units + n * unit_rows
                    dhid = dhid + nn(dy[:, at : at + pack], w_ref[m, unit_rows:, u : u + unit_rows])
            sg = 1.0 / (1.0 + jnp.exp(-gate))
            act = gate * sg
            hidden_ref[:, lanes] = (act * up).astype(BF)
            dgu_ref[:, lanes] = (dhid * up * sg * (1.0 + gate * (1.0 - sg))).astype(BF)
            second = slice(number_of_units + n * unit_rows, number_of_units + (n + 1) * unit_rows)
            dgu_ref[:, second] = (dhid * act).astype(BF)

    return pl.pallas_call(
        kernel,
        grid=(rows // block,),
        out_shape=[shape((rows, number_of_units), BF), shape((rows, 2 * number_of_units), BF)],
        in_specs=[
            pl.BlockSpec((block, width), lambda b: (b, 0)),
            pl.BlockSpec((block, width), lambda b: (b, 0)),
            IN_VMEM,
        ],
        out_specs=[
            pl.BlockSpec((block, number_of_units), lambda b: (b, 0)),
            pl.BlockSpec((block, 2 * number_of_units), lambda b: (b, 0)),
        ],
        compiler_params=pltpu.CompilerParams(vmem_limit_bytes=60 << 20),
        cost_estimate=pl.CostEstimate(
            flops=6 * rows * width * number_of_units, bytes_accessed=4 * rows * width, transcendentals=rows * number_of_units
        ),
        name="feed_forward",
    )(xn, dy, weights)


def feed_forward_input(dgu, weights, unit_rows, h1, cotangent, gain, n_ctx, number):
    rows, width = h1.shape
    n_outer = weights.shape[0]
    tile = 256

    def kernel(dgu_ref, w_ref, h_ref, dy_ref, gain_ref, dh_ref, dhb_ref, dgain_ref, *scratch):
        total = scratch[-1]

        def partial(slot, t):
            r = pl.ds(pl.multiple_of(slot * rows, rows), rows)
            lanes = pl.ds(pl.multiple_of(t * tile, tile), tile)
            acc = nn(dgu_ref[r, :unit_rows], w_ref[0, :unit_rows, lanes])
            for n in range(1, n_outer):
                acc = acc + nn(dgu_ref[r, n * unit_rows : (n + 1) * unit_rows], w_ref[n, :unit_rows, lanes])
            return acc

        scatter = Scatter(n_ctx, partial, tile, *scratch)
        greet_neighbours(n_ctx)
        scatter.to_mate()
        scatter.pairs()
        scatter.join()
        scatter.end()
        dgain_ref[...] = jnp.zeros_like(dgain_ref)

        def finish(r):
            h, d = h_ref[r], total[r]
            scale = inv_rms(h)
            dgain_ref[0:1] += jnp.sum(d * h * scale, 0, keepdims=True)
            dh = dy_ref[r].astype(F32) + norm_back(d, gain_ref[1:2], h, scale)
            dh_ref[r] = dh
            dhb_ref[r] = dh.astype(BF)

        row_chunks(rows, 32, finish)

    outs = [shape((rows, width), F32), shape((rows, width), BF), shape((8, width), F32)]
    return remote_call(
        kernel,
        "feed_forward_input",
        number,
        [dgu, weights, h1, cotangent, gain],
        outs,
        scatter_scratch(rows, width),
    )


def attention_backward(
    dh_all, out_w, qkv, attn, lse, cosine, sine, pos_rows, pos_columns, hidden, weights, unit_rows, h1, swapped, g_out, n_outer, n_ctx, number
):
    rows = dh_all.shape[0]
    own_rows, width = h1.shape
    group = rows // 2
    heads = attn.shape[1] // LANES
    k_at, v_at = heads * LANES, (heads + 1) * LANES
    block = min(QUERY_BLOCK, group)
    pack = weights.shape[1] - unit_rows
    units = hidden.shape[1]
    span = width // units

    def kernel(
        dh_hbm,
        ow_hbm,
        qkv_ref,
        attn_ref,
        lse_ref,
        cos_ref,
        sin_ref,
        rows_ref,
        columns_ref,
        hidden_ref,
        w_hbm,
        h_ref,
        swap_src,
        g_ref,
        dproj_ref,
        result_ref,
        swap_dst,
        g_dst,
        g_arrived,
        g_sum,
        g_send,
        g_recv,
        dk_ref,
        dv_ref,
        w_ref,
        out_w_ref,
        dh_ref,
        load_sem,
        out_load_sem,
        dh_sem,
        *scratch,
    ):
        swap_sem, g_swap_sem, scratch = scratch[:3], scratch[3:6], scratch[6:]
        total = scratch[-1]
        o = lax.axis_index("o")
        peers = outer_peers(n_outer)
        load = Load([(w_hbm.at[:, pl.ds(unit_rows, pack)], w_ref)], load_sem).begin()
        out_load = Load(out_loads(ow_hbm, out_w_ref), out_load_sem).begin()
        dh_load = Load([(dh_hbm, dh_ref)], dh_sem).begin()
        swap = Swap(n_ctx, [(swap_src, swap_dst)], *swap_sem)
        g_swap = Swap(n_ctx, [(g_sum, g_dst)], *g_swap_sem)

        def partial(slot, t):
            a = hidden_ref[pl.ds(pl.multiple_of(slot * own_rows, own_rows), own_rows)]
            lanes = pl.ds(pl.multiple_of((t % span) * units, units), units)
            return nt(a, w_ref[t // span, :, lanes])

        scatter = Scatter(n_ctx, partial, pack, *scratch)
        greet(swap.devices + peers)
        g_copies = [
            send(g_ref.at[device[0]], g_arrived.at[k], g_send.at[k], g_recv.at[k], device) for k, device in enumerate(peers)
        ]

        def back(g):
            keys_at = pl.ds(g * group, group)
            dk_ref[...] = jnp.zeros_like(dk_ref)
            dv_ref[...] = jnp.zeros_like(dv_ref)

            @pl.loop(0, group // block)
            def _(b):
                r = pl.ds(pl.multiple_of(g * group + b * block, block), block)
                key_pos = columns_ref[keys_at, 0:1]
                ok = (key_pos >= rows_ref[1:2, r]) & (key_pos <= rows_ref[0:1, r])
                da_all = nn(dh_ref[r], out_w_ref[...]).astype(BF)
                for h in range(heads):
                    lanes = slice(h * LANES, (h + 1) * LANES)
                    da, q = da_all[:, lanes], qkv_ref[r, lanes]
                    keys = qkv_ref[keys_at, k_at : k_at + LANES]
                    s = nt(keys, q) * SCALE - lse_ref[h : h + 1, r]
                    p = jnp.exp(jnp.where(ok, s, MASK_FILL))
                    dv_ref[...] += nn(p.astype(BF), da)
                    delta = jnp.transpose(da.astype(F32) * attn_ref[r, lanes].astype(F32))
                    delta = jnp.sum(delta, 0, keepdims=True)
                    dp = nt(qkv_ref[keys_at, v_at : v_at + LANES], da)
                    ds = (p * (dp - delta)).astype(BF)
                    dk_ref[...] += nn(ds, q)
                    dq = tn(ds, keys) * SCALE
                    dproj_ref[r, lanes] = rotate(dq, cos_ref[r], -sin_ref[r]).astype(BF)

            dk = rotate(dk_ref[...] * SCALE, cos_ref[keys_at], -sin_ref[keys_at])
            dproj_ref[keys_at, k_at : k_at + LANES] = dk.astype(BF)
            dproj_ref[keys_at, v_at : v_at + LANES] = dv_ref[...].astype(BF)

        load.wait()
        scatter.to_mate()
        scatter.pairs()
        swap.begin()
        out_load.wait()
        dh_load.wait()
        back(0)
        scatter.join()
        for copy in g_copies:
            copy.wait_recv()
        for d in range(2 * n_ctx):
            g_part = g_ref[o, d].astype(F32)
            for k in range(n_outer - 1):
                g_part = g_part + g_arrived[k, d].astype(F32)
            g_sum[d] = g_part.astype(BF)
        back(1)
        g_swap.begin()
        scatter.end()
        swap.end()

        def finish(r):
            result_ref[r] = (h_ref[r] + total[r]).astype(BF)

        row_chunks(own_rows, 32, finish)
        g_swap.end()
        for copy in g_copies:
            copy.wait_send()

    outs = [shape(qkv.shape, BF), shape((own_rows, width), BF), shape(swapped.shape, BF), shape(g_out.shape[1:], BF)]
    ins = [dh_all, out_w, qkv, attn, lse, cosine, sine, pos_rows, pos_columns, hidden, weights, h1, swapped, g_out]
    features = attn.shape[1]
    n_loads = out_w.shape[0] * width // features
    scratch = [
        pltpu.VMEM((n_outer - 1,) + g_out.shape[1:], BF),
        pltpu.VMEM(g_out.shape[1:], BF),
        pltpu.SemaphoreType.DMA((n_outer - 1,)),
        pltpu.SemaphoreType.DMA((n_outer - 1,)),
        pltpu.VMEM((group, LANES), F32),
        pltpu.VMEM((group, LANES), F32),
        pltpu.VMEM((weights.shape[0], pack, width), BF),
        pltpu.VMEM((width, features), BF),
        pltpu.VMEM(dh_all.shape, BF),
        pltpu.SemaphoreType.DMA((1,)),
        pltpu.SemaphoreType.DMA((n_loads,)),
        pltpu.SemaphoreType.DMA((1,)),
    ]
    scratch += swap_sems(1, n_ctx) + swap_sems(1, n_ctx) + scatter_scratch(own_rows, width)
    return remote_call(kernel, "attention_backward", number, ins, outs, scratch, any_ins=(0, 1, 10))


def attention_input(dproj, w, tokens, dh1, gain, gain_terms, n_outer, n_ctx, number):
    rows, width = tokens.shape
    tile = 256
    features = dproj.shape[1]
    n = 2 * n_ctx

    def kernel(
        d_ref, w_hbm, x_ref, dh_ref, gain_ref, terms_ref, out_ref, sum_ref, w_ref, load_sem, *scratch
    ):
        swap_sem, scratch = scratch[:3], scratch[3:]
        terms, summed, arrived, send_sem, recv_sem, local_sem = scratch[:6]
        scratch = scratch[6:]
        total = scratch[-1]
        load = Load(padded_loads(w_hbm, w_ref), load_sem).begin()
        o = lax.axis_index("o")

        def partial(slot, t):
            a = d_ref[pl.ds(pl.multiple_of(slot * rows, rows), rows)]
            return nn(a, w_ref[:, pl.ds(pl.multiple_of(t * tile, tile), tile)])

        scatter = Scatter(n_ctx, partial, tile, *scratch)
        swap = Swap(n_ctx, [(terms_ref, terms)], *swap_sem)
        peers = outer_peers(n_outer)
        greet(swap.devices + peers)
        swap.begin()
        load.wait()
        scatter.to_mate()
        scatter.pairs()
        swap.end()
        summed[...] = jnp.sum(terms[...], 0)
        scatter.join()
        copies = []
        for k, device in enumerate(peers):
            copies.append(send(summed.at[device[0]], arrived.at[o], send_sem.at[k], recv_sem.at[k], device))
        own = pltpu.make_async_copy(summed.at[o], arrived.at[o], local_sem)
        own.start()
        scatter.end()

        def finish(r):
            x, d = x_ref[r].astype(F32), total[r]
            out_ref[r] = dh_ref[r] + norm_back(d, gain_ref[0:1], x, inv_rms(x))

        row_chunks(rows, 32, finish)
        for copy in copies:
            copy.wait_recv()
        own.wait()
        sum_ref[...] = jnp.sum(arrived[...], 0)
        for copy in copies:
            copy.wait_send()

    outs = [shape((rows, width), F32), shape((8, LANES), F32)]
    ins = [dproj, w, tokens, dh1, gain, gain_terms]
    n_loads = w.shape[0] * w.shape[1] // (HEAD_SIZE // 2)
    scratch = [pltpu.VMEM((features, width), BF), pltpu.SemaphoreType.DMA((n_loads,))]
    scratch += swap_sems(1, n_ctx)
    scratch += [
        pltpu.VMEM((n, n_outer, 8, LANES), F32),
        pltpu.VMEM((n_outer, 8, LANES), F32),
        pltpu.VMEM((n_outer, 8, LANES), F32),
        pltpu.SemaphoreType.DMA((n_outer - 1,)),
        pltpu.SemaphoreType.DMA((n_outer - 1,)),
        pltpu.SemaphoreType.DMA,
    ]
    scratch += scatter_scratch(rows, width)
    return remote_call(kernel, "attention_input", number, ins, outs, scratch, any_ins=(1,))


def make_shards(n_outer, n_inner, n_ctx):
    n_plane = n_inner * n_ctx
    moves = feature_moves(n_outer, n_plane)
    back = [(b, a) for a, b in moves]

    def shards(tokens, norm_attn, w_qkv, w_out, norm_mlp, w_gate_up, w_down, cotangent, seq_lengths, block_slot):
        rows, width = tokens.shape
        gain_rows = norm_attn.shape[0]
        feature_rows = w_qkv.shape[0]
        out_rows = w_out.shape[0]
        unit_rows = w_gate_up.shape[0]
        n_seqs, n_slots = seq_lengths.shape[1], block_slot.shape[1]
        units = FF // n_plane
        gain_part = jnp.pad(jnp.stack([norm_attn, norm_mlp]), ((0, 6), (0, LANES - gain_rows)))
        meta = jnp.concatenate([seq_lengths[0], block_slot[0]])
        meta = jnp.pad(meta[None], ((0, 7), (0, LANES - n_seqs - n_slots)))
        moved_qkv = lax.ppermute(w_qkv, ALL, moves)
        metas, gains = exchange(meta, gain_part, n_outer, n_ctx, 0)
        gains = gains[:, :, :2, :gain_rows].transpose(2, 0, 1, 3).reshape(2, width)
        moved_qkv, metas = lax.optimization_barrier((moved_qkv, metas))
        qkv_w = z_ag(moved_qkv).reshape(CHUNKS, -1, width)
        source = tokens.astype(F32)
        xn1 = (source * inv_rms(source) * gains[0:1]).astype(BF)
        out_parts = pad_heads(w_out, 1).reshape(out_rows, n_plane, -1).transpose(1, 0, 2)
        down_parts = w_down.reshape(out_rows, n_outer // 2, n_plane, unit_rows).transpose(2, 0, 1, 3)
        down_parts = down_parts.reshape(n_plane, out_rows, units)
        xn1, out_parts, down_parts, cosine, sine, pos_rows, pos_columns = prologue(
            xn1, out_parts, down_parts, metas, n_seqs, n_ctx, 1
        )
        xn1 = xn1.reshape(-1, width)
        features = out_parts.shape[-1]
        out_pack = out_parts.reshape(width // features, -1, features).transpose(1, 0, 2).reshape(-1, width)
        short = -(-(1 << 20) // (2 * width * n_outer * 16)) * 16 - out_pack.shape[0]
        out_w = z_ag(jnp.pad(out_pack, ((0, max(short, 0)), (0, 0)))).reshape(n_outer, -1, width)
        if n_outer != CHUNKS:
            out_w = out_w[:, : out_pack.shape[0]].reshape(n_outer, -1, width // features, features).transpose(0, 2, 1, 3)
            out_w = pack_down(out_w.reshape(width, features), CHUNKS)
        down_pack = down_parts.reshape(width // units, -1, units).transpose(1, 0, 2).reshape(-1, width)
        mlp_w = z_ag(jnp.concatenate([w_gate_up, down_pack], 0)).reshape(n_outer, -1, width)
        mlp_w = in_chunks(mlp_w, unit_rows, units)
        qkv, attn, lse, dy_all = attention_forward(xn1, qkv_w, cosine, sine, pos_rows, pos_columns, cotangent, n_ctx, 2)
        h1, xn2 = output_projection(attn, out_w, tokens, gains, n_ctx, 3)
        xn2_all = plane_gather(xn2, n_ctx, 4)
        chunk_rows = 2 * units // CHUNKS
        hidden, dgu = feed_forward(xn2_all, dy_all, mlp_w, chunk_rows, units)
        g_down = tn(dy_all, hidden).astype(BF)
        dgu, g_down = lax.optimization_barrier((dgu, g_down))
        g_gate_up = tn(dgu, xn2_all).astype(BF)
        dgu, g_gate_up = lax.optimization_barrier((dgu, g_gate_up))
        g_down, g_gate_up = z_rs(g_down), z_rs(g_gate_up)
        dh1, dh1_bf, dgain_two = feed_forward_input(dgu, mlp_w, chunk_rows, h1, cotangent, gains, n_ctx, 5)
        dh1_all = plane_gather(dh1_bf, n_ctx, 6)
        dh1_all, g_gate_up, g_down = lax.optimization_barrier((dh1_all, g_gate_up, g_down))
        g_down = g_down.reshape(n_plane, out_rows, units)
        g_out = tn(dh1_all, attn).astype(BF).reshape(n_outer, n_plane, out_rows, -1)
        dproj, result, g_down, g_out = attention_backward(
            dh1_all, out_w, qkv, attn, lse, cosine, sine, pos_rows, pos_columns, hidden, mlp_w, chunk_rows, h1, g_down, g_out, n_outer, n_ctx, 7
        )
        g_qkv = cut_heads(tn(dproj, xn1).astype(BF), 0)
        terms = jnp.sum(qkv_w.reshape(-1, width).astype(F32) * g_qkv.astype(F32), 0) / gains[0]
        terms = jnp.stack([terms, dgain_two[0]]).reshape(2, n_outer, n_plane, gain_rows).transpose(2, 1, 0, 3)
        terms = jnp.pad(terms, ((0, 0), (0, 0), (0, 6), (0, LANES - gain_rows)))
        dproj, g_qkv = lax.optimization_barrier((dproj, g_qkv))
        g_qkv = z_rs(g_qkv)
        grad_input, g = attention_input(dproj, qkv_w, tokens, dh1, gains, terms, n_outer, n_ctx, 8)
        grad_input, g_qkv = lax.optimization_barrier((grad_input, g_qkv))
        grad_qkv = lax.ppermute(g_qkv, ALL, back).astype(F32)
        grad_out = cut_heads(g_out.transpose(1, 0, 2).reshape(out_rows, -1), 1).astype(F32)
        grad_down = g_down.reshape(n_plane, out_rows, n_outer // 2, unit_rows).transpose(1, 2, 0, 3)
        grad_down = grad_down.reshape(out_rows, -1).astype(F32)
        g = g[:, :gain_rows]
        return (result, grad_input, g[0], grad_qkv, grad_out, g[1], g_gate_up.astype(F32), grad_down)

    return shards


def solution(mesh):
    n_inner = 2
    n_ctx = mesh.shape["ctx"]
    n_outer = mesh.shape["dp"] // n_inner
    split = Mesh(mesh.devices.reshape(n_outer, n_inner, n_ctx), ALL)
    rows, vec, grp = P(ALL, None), P(ALL), P(("o", "i"), None)
    return jax.shard_map(
        make_shards(n_outer, n_inner, n_ctx),
        mesh=split,
        in_specs=(rows, vec, rows, rows, vec, rows, rows, rows, grp, grp),
        out_specs=(rows, rows, vec, rows, rows, vec, rows, rows),
        check_vma=False,
    )
```

```python
import math

import jax
import jax.numpy as jnp
import numpy as np
from jax import lax
from jax.experimental import pallas as pl
from jax.experimental.pallas import tpu as pltpu
from jax.sharding import Mesh
from jax.sharding import PartitionSpec as P


QUERY_HEADS = 16
HEAD_SIZE = 96
FF = 4096
BLK = 128
LANES = 128
QUERY_BLOCK = 512
CHUNKS = 4

EPSILON = 1e-05
THETA = 100000.0
MASK_FILL = -1e30
BF = jnp.bfloat16
F32 = jnp.float32
ALL = ("o", "i", "ctx")
MESH = pl.DeviceIdType.MESH
SCALE = 1.0 / math.sqrt(HEAD_SIZE)


def nt(a, b):
    return lax.dot_general(a, b, (((1,), (1,)), ((), ())), preferred_element_type=F32)


def nn(a, b):
    return lax.dot_general(a, b, (((1,), (0,)), ((), ())), preferred_element_type=F32)


def tn(a, b):
    return lax.dot_general(a, b, (((0,), (0,)), ((), ())), preferred_element_type=F32)


def z_ag(x):
    return lax.all_gather(x, "o", axis=0, tiled=True)


def z_rs(x):
    return lax.psum_scatter(x, "o", scatter_dimension=0, tiled=True)


def inv_rms(x):
    return lax.rsqrt(jnp.mean(x * x, -1, keepdims=True) + EPSILON)


def norm_back(grad_normed, gain, source, scale):
    weighted = grad_normed * gain
    return scale * weighted - source * scale**3 * jnp.mean(weighted * source, -1, keepdims=True)


def feature_moves(n_outer, n_plane):
    moves = []
    half, quarter = n_outer // 2, n_outer // 4
    for block in range(n_outer * n_plane):
        if block < 4 * n_outer:
            head, step = block // half, block % half
        elif block < 6 * n_outer:
            head, step = divmod(block - 4 * n_outer, quarter)
            step += half
        else:
            head, step = divmod(block - 6 * n_outer, quarter)
            step += half + quarter
        place = 2 * (head % (n_plane // 2)) + head // (n_plane // 2)
        moves.append((block, step * n_plane + place))
    return moves


def pad_heads(x, axis):
    half = HEAD_SIZE // 2
    shape = x.shape
    x = x.reshape(shape[:axis] + (-1, half) + shape[axis + 1 :])
    pads = [(0, 0)] * x.ndim
    pads[axis + 1] = (0, LANES // 2 - half)
    return jnp.pad(x, pads).reshape(shape[:axis] + (-1,) + shape[axis + 1 :])


def cut_heads(x, axis):
    half = HEAD_SIZE // 2
    shape = x.shape
    x = x.reshape(shape[:axis] + (-1, LANES // 2) + shape[axis + 1 :])
    x = lax.slice_in_dim(x, 0, half, axis=axis + 1)
    return x.reshape(shape[:axis] + (-1,) + shape[axis + 1 :])


def places(n_ctx):
    o, i, c = lax.axis_index("o"), lax.axis_index("i"), lax.axis_index("ctx")
    return o, i, c, c + 1 - 2 * (c % 2), (c + n_ctx // 2) % n_ctx


def greet(devices):
    barrier = pltpu.get_barrier_semaphore()
    for device in devices:
        pl.semaphore_signal(barrier, inc=1, device_id=device, device_id_type=MESH)
    pl.semaphore_wait(barrier, len(devices))


def greet_neighbours(n_ctx):
    o, i, c, mate, far = places(n_ctx)
    greet([(o, i, mate), (o, 1 - i, c), (o, i, far)])


def send(src, dst, send_sem, recv_sem, device):
    copy = pltpu.make_async_remote_copy(
        src_ref=src, dst_ref=dst, send_sem=send_sem, recv_sem=recv_sem, device_id=device, device_id_type=MESH
    )
    copy.start()
    return copy


class Gather:
    def __init__(self, n_ctx, src, out, send_sem, recv_sem, local_sem):
        self.src, self.out, self.sems = src, out, (send_sem, recv_sem, local_sem)
        o, i, c, mate, far = places(n_ctx)
        j, core = 1 - i, c % 2
        self.mate, self.x, self.y = (o, i, mate), (o, j, c), (o, i, far)
        self.me, self.s_x = i * n_ctx + c, j * n_ctx + c
        self.s_y, self.s_d = i * n_ctx + far, j * n_ctx + far
        self.relay = (o, j * core + i * (1 - core), c * core + far * (1 - core))
        self.relayed = self.s_y * core + self.s_x * (1 - core)
        mate_far = (mate + n_ctx // 2) % n_ctx
        self.mates_slots = [i * n_ctx + mate, j * n_ctx + mate, i * n_ctx + mate_far, j * n_ctx + mate_far]
        self.copies = {}

    def go(self, kind, src, slot, device):
        copy = send(src, self.out.at[slot], self.sems[0].at[kind], self.sems[1].at[kind], device)
        self.copies[kind] = copy

    def begin(self):
        self.go(1, self.src, self.me, self.x)
        self.go(2, self.src, self.me, self.y)
        self.go(0, self.src, self.me, self.mate)
        self.own = pltpu.make_async_copy(self.src, self.out.at[self.me], self.sems[2])
        self.own.start()

    def middle(self):
        self.copies[1].wait_recv()
        self.copies[2].wait_recv()
        self.go(5, self.out.at[self.relayed], self.relayed, self.relay)
        self.go(3, self.out.at[self.s_x], self.s_x, self.mate)
        self.go(4, self.out.at[self.s_y], self.s_y, self.mate)

    def corner(self):
        self.copies[5].wait_recv()
        self.go(6, self.out.at[self.s_d], self.s_d, self.mate)

    def arrived(self, kind):
        self.copies[kind].wait_recv()

    def sent(self):
        self.own.wait()
        for copy in self.copies.values():
            copy.wait_send()

    def end(self):
        self.corner()
        for kind in (0, 3, 4, 6):
            self.arrived(kind)
        self.sent()


GATHER_SEMS = [pltpu.SemaphoreType.DMA((7,)), pltpu.SemaphoreType.DMA((7,)), pltpu.SemaphoreType.DMA]


class Scatter:
    def __init__(self, n_ctx, partial, tile, ready, from_mate, going, got, send_sem, recv_sem, total):
        self.partial, self.tile = partial, tile
        self.ready, self.from_mate, self.going, self.got = ready, from_mate, going, got
        self.sems, self.total = (send_sem, recv_sem), total
        o, i, c, mate, far = places(n_ctx)
        j, core = 1 - i, c % 2
        self.core = core
        far_mate = (mate + n_ctx // 2) % n_ctx
        self.mine = [j * n_ctx + far, j * n_ctx + c, i * n_ctx + far, i * n_ctx + c]
        self.theirs = [j * n_ctx + far_mate, j * n_ctx + mate, i * n_ctx + far_mate, i * n_ctx + mate]
        self.mate = (o, i, mate)
        self.combined = (o, j * (1 - core) + i * core, c * (1 - core) + far * core)
        self.direct = (o, j * core + i * (1 - core), c * core + far * (1 - core))
        self.s_direct = self.mine[2] * (1 - core) + self.mine[1] * core
        self.s_combined = self.mine[1] * (1 - core) + self.mine[2] * core
        self.copies = []

    def go(self, kind, part, src, dst, device):
        copy = send(src.at[part], dst.at[part], self.sems[0].at[kind, part], self.sems[1].at[kind, part], device)
        self.copies.append(copy)
        return copy

    def each(self, part, body):
        tiles = self.ready.shape[-1] // self.tile

        @pl.loop(0, tiles)
        def _(t):
            at = pl.multiple_of(t * self.tile, self.tile)
            body(part * tiles + t, pl.ds(at, self.tile), pl.ds(part * tiles * self.tile + at, self.tile))

    def fill(self, n, part):
        def body(t, lanes, _):
            self.ready[n, part, :, lanes] = self.partial(self.theirs[n], t).astype(BF)

        self.each(part, body)

    def give(self, n, part):
        self.mates[n, part] = self.go(n, part, self.ready.at[n], self.from_mate.at[n], self.mate)

    def pair(self, slot, n, part, place):
        def body(t, lanes, _):
            pair = self.partial(slot, t) + self.from_mate[n, part, :, lanes].astype(F32)
            self.going[place, part, :, lanes] = pair.astype(BF)

        self.each(part, body)

    def to_mate(self):
        self.mates, self.straights, self.diagonals, self.joins = {}, [], [], []
        order = [(0, 0), (0, 1), (1, 0), (2, 0), (1, 1), (2, 1), (3, 0), (3, 1)]
        self.fill(*order[0])
        for k, at in enumerate(order[1:]):
            self.fill(*at)
            self.give(*order[k])
            if k == 2:
                self.mates[0, 0].wait_recv()
                self.pair(self.mine[0], 0, 0, 0)
            if k == 3:
                self.diagonals.append(self.go(4, 0, self.going.at[0], self.got.at[0], self.direct))
                self.mates[0, 1].wait_recv()
                self.pair(self.mine[0], 0, 1, 0)
            if k == 4:
                self.diagonals.append(self.go(4, 1, self.going.at[0], self.got.at[0], self.direct))
        self.last = order[-1]

    def pairs(self):
        for part in range(PARTS):
            self.mates[1, part].wait_recv()
            self.mates[2, part].wait_recv()
            self.pair(self.s_direct, 2 - self.core, part, 1)
            if part == 0:
                self.give(*self.last)
            else:
                self.straights.append(self.go(5, part - 1, self.going.at[1], self.got.at[1], self.direct))

    def join(self):
        for part in range(PARTS):
            self.diagonals[part].wait_recv()
            if part == 0:
                self.straights.append(self.go(5, PARTS - 1, self.going.at[1], self.got.at[1], self.direct))

            def combined(t, lanes, _):
                pair = self.partial(self.s_combined, t) + self.from_mate[1 + self.core, part, :, lanes].astype(F32)
                self.going[2, part, :, lanes] = (pair + self.got[0, part, :, lanes].astype(F32)).astype(BF)

            self.each(part, combined)
            if part:
                self.joins.append(self.go(6, part - 1, self.going.at[2], self.got.at[2], self.combined))
        self.own(0)
        self.joins.append(self.go(6, PARTS - 1, self.going.at[2], self.got.at[2], self.combined))

    def own(self, part):
        self.mates[3, part].wait_recv()

        def body(t, lanes, out):
            self.total[:, out] = self.partial(self.mine[3], t) + self.from_mate[3, part, :, lanes].astype(F32)

        self.each(part, body)

    def end(self):
        total = self.total
        for part in range(1, PARTS):
            self.own(part)
        for part in range(PARTS):
            self.straights[part].wait_recv()
            self.joins[part].wait_recv()

            def rest(t, lanes, out):
                other = self.got[1, part, :, lanes].astype(F32) + self.got[2, part, :, lanes].astype(F32)
                total[:, out] = total[:, out] + other

            self.each(part, rest)
        for copy in self.copies:
            copy.wait_send()


PARTS = 2


def scatter_scratch(rows, width):
    return [
        pltpu.VMEM((4, PARTS, rows, width // PARTS), BF),
        pltpu.VMEM((4, PARTS, rows, width // PARTS), BF),
        pltpu.VMEM((3, PARTS, rows, width // PARTS), BF),
        pltpu.VMEM((3, PARTS, rows, width // PARTS), BF),
        pltpu.SemaphoreType.DMA((7, PARTS)),
        pltpu.SemaphoreType.DMA((7, PARTS)),
        pltpu.VMEM((rows, width), F32),
    ]


def row_chunks(rows, step, body):
    @pl.loop(0, rows // step)
    def _(r):
        body(pl.ds(pl.multiple_of(r * step, step), step))


class Load:
    def __init__(self, parts, sem):
        self.copies = [pltpu.make_async_copy(src, dst, sem.at[n]) for n, (src, dst) in enumerate(parts)]

    def begin(self):
        for copy in self.copies:
            copy.start()
        return self

    def wait(self):
        for copy in self.copies:
            copy.wait()


IN_VMEM = pl.BlockSpec(memory_space=pltpu.VMEM)
ANYWHERE = pl.BlockSpec(memory_space=pl.ANY)


def remote_call(kernel, number, ins, outs, scratch, any_outs=(), any_ins=()):
    return pl.pallas_call(
        kernel,
        out_shape=outs,
        in_specs=[ANYWHERE if n in any_ins else IN_VMEM for n in range(len(ins))],
        out_specs=[ANYWHERE if n in any_outs else IN_VMEM for n in range(len(outs))],
        scratch_shapes=scratch,
        compiler_params=pltpu.CompilerParams(collective_id=number, has_side_effects=True, vmem_limit_bytes=60 << 20),
    )(*ins)


def shape(dims, dtype):
    return jax.ShapeDtypeStruct(tuple(dims), dtype)


class Swap:
    def __init__(self, n_ctx, pairs, send_sem, recv_sem, local_sem):
        self.pairs, self.sems = pairs, (send_sem, recv_sem, local_sem)
        self.o, i, c, _, _ = places(n_ctx)
        self.n, self.n_ctx = 2 * n_ctx, n_ctx
        self.me = i * n_ctx + c
        self.others = [(self.me + k) % self.n for k in range(1, self.n)]
        self.devices = [(self.o, d // n_ctx, d % n_ctx) for d in self.others]

    def begin(self):
        self.copies, self.own = [], []
        for a, (src, dst) in enumerate(self.pairs):
            for k, (d, device) in enumerate(zip(self.others, self.devices)):
                self.copies.append(
                    send(src.at[d], dst.at[self.me], self.sems[0].at[a, k], self.sems[1].at[a, k], device)
                )
            own = pltpu.make_async_copy(src.at[self.me], dst.at[self.me], self.sems[2].at[a])
            own.start()
            self.own.append(own)

    def end(self):
        for copy in self.copies:
            copy.wait_recv()
            copy.wait_send()
        for copy in self.own:
            copy.wait()


def swap_sems(n_arrays, n_ctx):
    return [
        pltpu.SemaphoreType.DMA((n_arrays, 2 * n_ctx - 1)),
        pltpu.SemaphoreType.DMA((n_arrays, 2 * n_ctx - 1)),
        pltpu.SemaphoreType.DMA((n_arrays,)),
    ]


def outer_peers(n_outer):
    o, i, c = lax.axis_index("o"), lax.axis_index("i"), lax.axis_index("ctx")
    return [(lax.rem(o + k, n_outer), i, c) for k in range(1, n_outer)]


def rotary_constants():
    frequency = THETA ** -(np.arange(HEAD_SIZE // 2) * (2.0 / HEAD_SIZE))
    rates = np.zeros((8, LANES), np.float32)
    for half, sign in ((0, -1.0), (LANES // 2, 1.0)):
        rates[0, half : half + HEAD_SIZE // 2] = frequency
        rates[1, half : half + HEAD_SIZE // 2] = sign
    angles = np.arange(BLK)[:, None] * rates[0].astype(np.float64)
    return rates, np.stack([np.cos(angles), np.sin(angles)]).astype(np.float32)


def prologue(tokens, out_parts, down_parts, gains, meta, n_seqs, n_outer, n_ctx, number):
    rows, width = tokens.shape
    n = 2 * n_ctx
    blocks = n_ctx * rows // BLK

    def kernel(
        x_ref,
        out_src,
        down_src,
        gains_ref,
        meta_ref,
        rates_ref,
        angles_ref,
        x_all,
        out_dst,
        down_dst,
        gains_out,
        cos_ref,
        sin_ref,
        rows_ref,
        columns_ref,
        *sems,
    ):
        o = lax.axis_index("o")
        metas_ref, send_sem, recv_sem, local_sem = sems[:4]
        out_swap = Swap(n_ctx, [(out_src, out_dst)], *sems[4:7])
        down_swap = Swap(n_ctx, [(down_src, down_dst)], *sems[7:10])
        gather = Gather(n_ctx, x_ref, x_all, *sems[10:])
        peers = outer_peers(n_outer)
        me = out_swap.me
        greet(out_swap.devices + peers)
        gather.begin()
        own = [
            pltpu.make_async_copy(meta_ref, metas_ref.at[me], local_sem.at[0]),
            pltpu.make_async_copy(gains_ref, gains_out.at[o, me], local_sem.at[1]),
        ]
        meta_copies, gain_copies, z_copies = [], [], []
        for copy in own:
            copy.start()
        for k, device in enumerate(out_swap.devices):
            meta_copies.append(send(meta_ref, metas_ref.at[me], send_sem.at[0, k], recv_sem.at[0, k], device))
            gain_copies.append(send(gains_ref, gains_out.at[o, me], send_sem.at[1, k], recv_sem.at[1, k], device))
        out_swap.begin()
        for copy in own:
            copy.wait()
        for copy in meta_copies:
            copy.wait_recv()
        lane = lax.broadcasted_iota(jnp.int32, (BLK, LANES), 1)
        row = lax.broadcasted_iota(jnp.int32, (BLK, LANES), 0)
        rows_ref[...] = jnp.zeros_like(rows_ref)
        pieces = 2 * blocks * n_seqs
        piece = lax.broadcasted_iota(jnp.int32, (pieces, LANES), 0)
        bases = jnp.zeros((pieces, LANES), jnp.int32)
        places_of = []
        for g in range(2):
            starts, end = [], jnp.zeros((1, 1), jnp.int32)
            for q in range(n_seqs):
                starts.append(end)
                end = end + metas_ref[g * n_ctx, 0:1, q : q + 1]
            for b in range(blocks):
                first = metas_ref[g * n_ctx, 0:1, n_seqs + b : n_seqs + b + 1] * BLK
                for q in range(n_seqs):
                    index = (g * blocks + b) * n_seqs + q
                    bases = jnp.where(piece == index, first - starts[q], bases)
                places_of.append((first, starts))
        angle = bases.astype(F32) * rates_ref[0:1]
        base_cos, base_sin = jnp.cos(angle), jnp.sin(angle)
        for n_block, (first, starts) in enumerate(places_of):
            at = slice(n_block * BLK, (n_block + 1) * BLK)
            stream, lanes_stream = first + row, first + lane[0:1]
            start, lanes_start = jnp.zeros_like(stream), jnp.zeros_like(lanes_stream)
            cos, sin = angles_ref[0], angles_ref[1]
            for q in range(n_seqs):
                index = n_block * n_seqs + q
                cos_0, sin_0 = base_cos[index : index + 1], base_sin[index : index + 1]
                cos_q = cos_0 * angles_ref[0] - sin_0 * angles_ref[1]
                sin_q = sin_0 * angles_ref[0] + cos_0 * angles_ref[1]
                inside = stream >= starts[q]
                start = jnp.where(inside, starts[q], start)
                lanes_start = jnp.where(lanes_stream >= starts[q], starts[q], lanes_start)
                cos, sin = jnp.where(inside, cos_q, cos), jnp.where(inside, sin_q, sin)
            cos_ref[at] = cos
            sin_ref[at] = sin * rates_ref[1:2]
            columns_ref[at] = jnp.where(lane == 0, stream, start)
            rows_ref[0:1, at] = lanes_stream
            rows_ref[1:2, at] = lanes_start
        for copy in gain_copies:
            copy.wait_recv()
        for k, device in enumerate(peers):
            z_copies.append(send(gains_out.at[o], gains_out.at[o], send_sem.at[2, k], recv_sem.at[2, k], device))
        gather.middle()
        down_swap.begin()
        gather.end()
        out_swap.end()
        down_swap.end()
        for copy in z_copies:
            copy.wait_recv()
        for copy in meta_copies + gain_copies + z_copies:
            copy.wait_send()

    outs = [
        shape((n, rows, width), BF),
        shape(out_parts.shape, BF),
        shape(down_parts.shape, BF),
        shape((n_outer, n) + gains.shape, F32),
        shape((n * rows, LANES), F32),
        shape((n * rows, LANES), F32),
        shape((8, n * rows), jnp.int32),
        shape((n * rows, LANES), jnp.int32),
    ]
    rates, angles = rotary_constants()
    ins = [tokens, out_parts, down_parts, gains, meta, jnp.asarray(rates), jnp.asarray(angles)]
    most = max(n, n_outer) - 1
    scratch = [
        pltpu.VMEM((n,) + meta.shape, jnp.int32),
        pltpu.SemaphoreType.DMA((3, most)),
        pltpu.SemaphoreType.DMA((3, most)),
        pltpu.SemaphoreType.DMA((2,)),
    ]
    scratch += swap_sems(1, n_ctx) + swap_sems(1, n_ctx) + GATHER_SEMS
    return remote_call(kernel, number, ins, outs, scratch, any_outs=(0,))


def plane_gather(x, n_ctx, number):
    def kernel(src, out, *sems):
        gather = Gather(n_ctx, src, out, *sems)
        greet_neighbours(n_ctx)
        gather.begin()
        gather.middle()
        gather.end()

    outs = [shape((2 * n_ctx,) + x.shape, x.dtype)]
    got = remote_call(kernel, number, [x], outs, GATHER_SEMS, any_outs=(0,))
    return got[0].reshape(-1, x.shape[-1])


def rotate(x, cosine, sine):
    return x * cosine + pltpu.roll(x, LANES // 2, 1) * sine


def qkv_rows(features):
    return features // LANES * HEAD_SIZE // CHUNKS


def padded_loads(w_ref, w_pad):
    half = HEAD_SIZE // 2
    rows = qkv_rows(w_pad.shape[0])
    pairs, at = [], 0
    for row in range(half, w_pad.shape[0], LANES // 2):
        w_pad[row : row + LANES // 2 - half] = jnp.zeros((LANES // 2 - half, w_pad.shape[1]), BF)
    for n in range(w_ref.shape[0]):
        for b in range(rows // half):
            src = w_ref.at[n, pl.ds(b * half, half)]
            pairs.append((src, w_pad.at[pl.ds(at * LANES // 2, half)]))
            at += 1
    return pairs


def attention_forward(x_all, gains, w, cosine, sine, pos_rows, pos_columns, dy, out_part, n_outer, n_ctx, number):
    rows, width = x_all.shape
    group = rows // 2
    heads = QUERY_HEADS // (2 * n_ctx)
    features = (heads + 2) * LANES
    k_at, v_at = heads * LANES, (heads + 1) * LANES
    block = min(QUERY_BLOCK, group)
    n_loads = features // (LANES // 2)

    def kernel(
        x_hbm,
        gain_ref,
        w_hbm,
        cos_ref,
        sin_ref,
        rows_ref,
        columns_ref,
        dy_ref,
        part_ref,
        qkv_ref,
        attn_ref,
        lse_ref,
        dy_all,
        xn_out,
        out_w,
        w_ref,
        xn_ref,
        load_sem,
        xn_sem,
        store_sem,
        z_send,
        z_recv,
        z_local,
        *sems,
    ):
        gather = Gather(n_ctx, dy_ref, dy_all, *sems)
        load = Load(padded_loads(w_hbm, w_ref), load_sem).begin()
        xn_load = Load([(x_hbm, xn_ref)], xn_sem).begin()
        o = lax.axis_index("o")
        peers = outer_peers(n_outer)
        greet([gather.mate, gather.x, gather.y] + peers)
        gather.begin()
        z_copies = [send(part_ref, out_w.at[o], z_send.at[k], z_recv.at[k], device) for k, device in enumerate(peers)]
        own_part = pltpu.make_async_copy(part_ref, out_w.at[o], z_local)
        own_part.start()
        load.wait()
        xn_load.wait()

        def normalise(r):
            x = xn_ref[r].astype(F32)
            xn_ref[r] = (x * inv_rms(x) * gain_ref[0:1]).astype(BF)

        def project(r):
            cos, sin = cos_ref[r], sin_ref[r]
            for h in range(heads + 2):
                lanes = slice(h * LANES, (h + 1) * LANES)
                part = nt(xn_ref[r], w_ref[lanes])
                qkv_ref[r, lanes] = (rotate(part, cos, sin) if h <= heads else part).astype(BF)

        def attend(g):
            keys_at = pl.ds(g * group, group)

            @pl.loop(0, group // block)
            def _(b):
                r = pl.ds(pl.multiple_of(g * group + b * block, block), block)
                key_pos = rows_ref[0:1, keys_at]
                ok = (key_pos >= columns_ref[r, 1:2]) & (key_pos <= columns_ref[r, 0:1])
                for h in range(heads):
                    lanes = slice(h * LANES, (h + 1) * LANES)
                    s = nt(qkv_ref[r, lanes], qkv_ref[keys_at, k_at : k_at + LANES])
                    s = jnp.where(ok, s, MASK_FILL)
                    high = jnp.max(s, -1, keepdims=True)
                    e = jnp.exp((s - high) * SCALE)
                    total = jnp.sum(e, -1, keepdims=True)
                    mixed = nn(e.astype(BF), qkv_ref[keys_at, v_at : v_at + LANES])
                    attn_ref[r, lanes] = (mixed / total).astype(BF)
                    lse = jnp.broadcast_to(high * SCALE + jnp.log(total), (block, LANES))
                    lse_ref[h : h + 1, r] = jnp.transpose(lse)[0:1]

        row_chunks(rows, 64, normalise)
        row_chunks(rows, block, project)
        gather.middle()
        store = Load([(xn_ref, xn_out)], store_sem).begin()
        attend(0)
        attend(1)
        gather.end()
        store.wait()
        own_part.wait()
        for copy in z_copies:
            copy.wait_recv()
            copy.wait_send()

    outs = [
        shape((rows, features), BF),
        shape((rows, heads * LANES), BF),
        shape((8, rows), F32),
        shape((2 * n_ctx,) + dy.shape, BF),
        shape(x_all.shape, BF),
        shape((n_outer,) + out_part.shape, BF),
    ]
    ins = [x_all, gains, w, cosine, sine, pos_rows, pos_columns, dy, out_part]
    scratch = [
        pltpu.VMEM((features, width), BF),
        pltpu.VMEM(x_all.shape, BF),
        pltpu.SemaphoreType.DMA((n_loads,)),
        pltpu.SemaphoreType.DMA((1,)),
        pltpu.SemaphoreType.DMA((1,)),
        pltpu.SemaphoreType.DMA((n_outer - 1,)),
        pltpu.SemaphoreType.DMA((n_outer - 1,)),
        pltpu.SemaphoreType.DMA,
    ]
    scratch += GATHER_SEMS
    got = remote_call(kernel, number, ins, outs, scratch, any_outs=(3, 4), any_ins=(0, 2))
    return got[0], got[1], got[2], got[3].reshape(rows, width), got[4], got[5]


def output_projection(attn, out_w, tokens, gain, n_ctx, number):
    rows, width = tokens.shape
    tile = 256


    def kernel(attn_ref, w_ref, x_ref, gain_ref, h_ref, xn_ref, *scratch):
        total = scratch[-1]

        def partial(slot, t):
            a = attn_ref[pl.ds(pl.multiple_of(slot * rows, rows), rows)]
            return nt(a, w_ref[pl.ds(pl.multiple_of(t * tile, tile), tile)])

        scatter = Scatter(n_ctx, partial, tile, *scratch)
        greet_neighbours(n_ctx)
        scatter.to_mate()
        scatter.pairs()
        scatter.join()
        scatter.end()

        def finish(r):
            h = x_ref[r].astype(F32) + total[r]
            h_ref[r] = h
            xn_ref[r] = (h * inv_rms(h) * gain_ref[1:2]).astype(BF)

        row_chunks(rows, 32, finish)

    outs = [shape((rows, width), F32), shape((rows, width), BF)]
    return remote_call(kernel, number, [attn, out_w, tokens, gain], outs, scatter_scratch(rows, width))


def feed_forward(xn, dy, gate_up, down, n_ctx, number):
    rows, width = xn.shape
    n = 2 * n_ctx
    chunks, unit_rows, _ = gate_up.shape
    units = down.shape[1]
    tile = 256

    def kernel(
        x_ref,
        dy_hbm,
        up_hbm,
        down_hbm,
        xn_all,
        hidden_ref,
        dgu_ref,
        dgu_t,
        g_down_ref,
        raw,
        dy_ref,
        up_ref,
        down_ref,
        hidden_t,
        g_acc,
        load_sem,
        store_sem,
        *sems,
    ):
        gather = Gather(n_ctx, x_ref, raw, *sems)
        pairs = [(up_hbm, up_ref), (down_hbm, down_ref), (dy_hbm, dy_ref)]
        load = Load(pairs, load_sem).begin()
        greet_neighbours(n_ctx)
        gather.begin()
        half = chunks // 2
        core = gather.me % 2

        def chip(slot):
            both = pl.ds(pl.multiple_of((slot - core) * rows, 2 * rows), 2 * rows)
            x = raw[pl.ds(slot - core, 2)].reshape(2 * rows, width)
            for m in range(half):
                lanes = slice(m * unit_rows, (m + 1) * unit_rows)
                second = slice(units + m * unit_rows, units + (m + 1) * unit_rows)
                gate = nt(x, up_ref[m])
                up = nt(x, up_ref[half + m])
                dhid = nn(dy_ref[both], down_ref[:, lanes])
                sg = 1.0 / (1.0 + jnp.exp(-gate))
                act = gate * sg
                hidden = act * up
                dgate = dhid * up * sg * (1.0 + gate * (1.0 - sg))
                dup = dhid * act
                hidden_ref[both, lanes] = hidden.astype(BF)
                dgu_ref[both, lanes] = dgate.astype(BF)
                dgu_ref[both, second] = dup.astype(BF)
                hidden_t[lanes] = jnp.transpose(hidden).astype(BF)
                dgu_t[lanes, both] = jnp.transpose(dgate).astype(BF)
                dgu_t[second, both] = jnp.transpose(dup).astype(BF)

            @pl.loop(0, width // tile)
            def _(t):
                lanes = pl.ds(pl.multiple_of(t * tile, tile), tile)
                g = nn(hidden_t[...], dy_ref[both, lanes])
                g_acc[:, lanes] = g if slot is gather.me else g_acc[:, lanes] + g

        stores = []

        def store(slot):
            copy = pltpu.make_async_copy(raw.at[slot], xn_all.at[slot], store_sem.at[len(stores)])
            copy.start()
            stores.append(copy)

        load.wait()
        gather.arrived(0)
        gather.own.wait()
        store(gather.me)
        store(gather.mates_slots[0])
        chip(gather.me)
        gather.middle()
        gather.arrived(3)
        store(gather.s_x)
        store(gather.mates_slots[1])
        chip(gather.s_x)
        gather.arrived(4)
        store(gather.s_y)
        store(gather.mates_slots[2])
        chip(gather.s_y)
        gather.corner()
        gather.arrived(6)
        store(gather.s_d)
        store(gather.mates_slots[3])
        chip(gather.s_d)

        @pl.loop(0, width // tile)
        def _(t):
            lanes = pl.ds(pl.multiple_of(t * tile, tile), tile)
            g_down_ref[lanes] = jnp.transpose(g_acc[:, lanes]).astype(BF)

        for copy in gather.copies.values():
            copy.wait_send()
        for copy in stores:
            copy.wait()

    outs = [
        shape((n, rows, width), BF),
        shape((n * rows, units), BF),
        shape((n * rows, 2 * units), BF),
        shape((2 * units, n * rows), BF),
        shape((width, units), BF),
    ]
    scratch = [
        pltpu.VMEM((n, rows, width), BF),
        pltpu.VMEM(dy.shape, BF),
        pltpu.VMEM(gate_up.shape, BF),
        pltpu.VMEM(down.shape, BF),
        pltpu.VMEM((units, 2 * rows), BF),
        pltpu.VMEM((units, width), F32),
        pltpu.SemaphoreType.DMA((3,)),
        pltpu.SemaphoreType.DMA((n,)),
    ]
    ins = [xn, dy, gate_up, down]
    return remote_call(kernel, number, ins, outs, scratch + GATHER_SEMS, any_outs=(0,), any_ins=(1, 2, 3))


def feed_forward_input(dgu, gate_up, h1, cotangent, gain, xn_all, dgu_t, n_ctx, number):
    rows, width = h1.shape
    chunks, unit_rows, _ = gate_up.shape
    units = chunks * unit_rows // 2
    tile, part = 256, 256

    def kernel(
        dgu_ref,
        w_hbm,
        h_ref,
        dy_ref,
        gain_ref,
        xn_hbm,
        dgu_t_hbm,
        dh_ref,
        dhb_ref,
        dgain_ref,
        g_up_ref,
        w_ref,
        xn_ref,
        dgu_t_ref,
        w_sem,
        load_sem,
        *scratch,
    ):
        total = scratch[-1]
        w_load = Load([(w_hbm, w_ref)], w_sem).begin()
        load = Load([(dgu_t_hbm, dgu_t_ref), (xn_hbm, xn_ref)], load_sem).begin()

        def partial(slot, t):
            r = pl.ds(pl.multiple_of(slot * rows, rows), rows)
            lanes = pl.ds(pl.multiple_of(t * tile, tile), tile)
            acc = nn(dgu_ref[r, :unit_rows], w_ref[0, :, lanes])
            for n in range(1, chunks):
                acc = acc + nn(dgu_ref[r, n * unit_rows : (n + 1) * unit_rows], w_ref[n, :, lanes])
            return acc

        def up_gradient(first, last):
            @pl.loop(first, last)
            def _(k):
                r = pl.ds(pl.multiple_of(k * part, part), part)

                @pl.loop(0, width // tile)
                def _(t):
                    lanes = pl.ds(pl.multiple_of(t * tile, tile), tile)
                    g_up_ref[r, lanes] = nn(dgu_t_ref[r], xn_ref[:, lanes]).astype(BF)

        scatter = Scatter(n_ctx, partial, tile, *scratch)
        greet_neighbours(n_ctx)
        w_load.wait()
        scatter.to_mate()
        scatter.pairs()
        load.wait()
        up_gradient(0, units // part)
        scatter.join()
        up_gradient(units // part, 2 * units // part)
        scatter.end()
        dgain_ref[...] = jnp.zeros_like(dgain_ref)

        def finish(r):
            h, d = h_ref[r], total[r]
            scale = inv_rms(h)
            dgain_ref[0:1] += jnp.sum(d * h * scale, 0, keepdims=True)
            dh = dy_ref[r].astype(F32) + norm_back(d, gain_ref[1:2], h, scale)
            dh_ref[r] = dh
            dhb_ref[r] = dh.astype(BF)

        row_chunks(rows, 32, finish)

    outs = [
        shape((rows, width), F32),
        shape((rows, width), BF),
        shape((8, width), F32),
        shape((2 * units, width), BF),
    ]
    scratch = [
        pltpu.VMEM((chunks, unit_rows, width), BF),
        pltpu.VMEM(xn_all.shape, BF),
        pltpu.VMEM(dgu_t.shape, BF),
        pltpu.SemaphoreType.DMA((1,)),
        pltpu.SemaphoreType.DMA((2,)),
    ]
    return remote_call(
        kernel,
        number,
        [dgu, gate_up, h1, cotangent, gain, xn_all, dgu_t],
        outs,
        scratch + scatter_scratch(rows, width),
        any_ins=(1, 5, 6),
    )


def attention_backward(
    dh_all, xn, qkv, attn, lse, cosine, sine, pos_rows, pos_columns, hidden, out_w, down_w, h1, swapped, n_outer, n_ctx, number
):
    rows = dh_all.shape[0]
    own_rows, width = h1.shape
    group = rows // 2
    heads = attn.shape[1] // LANES
    k_at, v_at = heads * LANES, (heads + 1) * LANES
    block = min(QUERY_BLOCK, group)
    features = attn.shape[1]
    tile = 256
    place_rows = width // n_outer // (2 * n_ctx)

    def kernel(
        dh_hbm,
        xn_hbm,
        qkv_hbm,
        attn_hbm,
        lse_ref,
        cos_hbm,
        sin_hbm,
        rows_ref,
        columns_hbm,
        hidden_ref,
        out_w_hbm,
        w_hbm,
        h_ref,
        swap_src,
        dproj_ref,
        result_ref,
        swap_dst,
        g_dst,
        g_qkv_ref,
        xn_ref,
        qkv_ref,
        attn_ref,
        cos_ref,
        sin_ref,
        columns_ref,
        g_ref,
        g_arrived,
        g_sum,
        g_send,
        g_recv,
        dk_ref,
        dv_ref,
        w_ref,
        out_w_ref,
        dh_ref,
        load_sem,
        dh_sem,
        *scratch,
    ):
        swap_sem, g_swap_sem, scratch = scratch[:3], scratch[3:6], scratch[6:]
        total = scratch[-1]
        o = lax.axis_index("o")
        peers = outer_peers(n_outer)
        load = Load([(w_hbm, w_ref)], load_sem).begin()
        pairs = [(out_w_hbm, out_w_ref), (dh_hbm, dh_ref), (attn_hbm, attn_ref), (qkv_hbm, qkv_ref), (cos_hbm, cos_ref), (sin_hbm, sin_ref)]
        dh_load = Load(pairs + [(columns_hbm, columns_ref), (xn_hbm, xn_ref)], dh_sem).begin()
        swap = Swap(n_ctx, [(swap_src, swap_dst)], *swap_sem)
        g_swap = Swap(n_ctx, [(g_sum, g_dst)], *g_swap_sem)

        def partial(slot, t):
            a = hidden_ref[pl.ds(pl.multiple_of(slot * own_rows, own_rows), own_rows)]
            return nt(a, w_ref[pl.ds(pl.multiple_of(t * tile, tile), tile)])

        scatter = Scatter(n_ctx, partial, tile, *scratch)
        greet(swap.devices + peers)

        def back(g, b):
            keys_at = pl.ds(g * group, group)
            r = pl.ds(g * group + b * block, block)
            if b == 0:
                dk_ref[...] = jnp.zeros_like(dk_ref)
                dv_ref[...] = jnp.zeros_like(dv_ref)
            key_pos = columns_ref[keys_at, 0:1]
            ok = (key_pos >= rows_ref[1:2, r]) & (key_pos <= rows_ref[0:1, r])
            da_all = nn(dh_ref[r], out_w_ref[...]).astype(BF)

            for h in range(heads):
                lanes = slice(h * LANES, (h + 1) * LANES)
                da, q = da_all[:, lanes], qkv_ref[r, lanes]
                keys = qkv_ref[keys_at, k_at : k_at + LANES]
                s = nt(keys, q) * SCALE - lse_ref[h : h + 1, r]
                p = jnp.exp(jnp.where(ok, s, MASK_FILL))
                dv_ref[...] += nn(p.astype(BF), da)
                delta = jnp.transpose(da.astype(F32) * attn_ref[r, lanes].astype(F32))
                delta = jnp.sum(delta, 0, keepdims=True)
                dp = nt(qkv_ref[keys_at, v_at : v_at + LANES], da)
                ds = (p * (dp - delta)).astype(BF)
                dk_ref[...] += nn(ds, q)
                dq = tn(ds, keys) * SCALE
                dproj_ref[r, lanes] = rotate(dq, cos_ref[r], -sin_ref[r]).astype(BF)

            if b == group // block - 1:
                dk = rotate(dk_ref[...] * SCALE, cos_ref[keys_at], -sin_ref[keys_at])
                dproj_ref[keys_at, k_at : k_at + LANES] = dk.astype(BF)
                dproj_ref[keys_at, v_at : v_at + LANES] = dv_ref[...].astype(BF)

        def out_gradient():
            @pl.loop(0, width // 384)
            def _(k):
                d = pl.ds(pl.multiple_of(k * 384, 384), 384)
                g_ref[d] = jnp.transpose(tn(attn_ref[...], dh_ref[:, d])).astype(BF)

        def own_place(outer):
            return pl.ds(pl.multiple_of(outer * (width // n_outer), 16), width // n_outer)

        def qkv_gradient():
            half = HEAD_SIZE // 2

            @pl.loop(0, width // 256)
            def _(t):
                lanes = pl.ds(pl.multiple_of(t * 256, 256), 256)
                for h in range(heads + 2):
                    g = tn(dproj_ref[:, h * LANES : (h + 1) * LANES], xn_ref[:, lanes]).astype(BF)
                    for k in range(2):
                        at = h * HEAD_SIZE + k * half
                        g_qkv_ref[at : at + half, lanes] = g[k * LANES // 2 : k * LANES // 2 + half]

        load.wait()
        units = [(g, b) for g in range(2) for b in range(group // block)]
        scatter.to_mate()
        dh_load.wait()
        back(*units[0])
        scatter.pairs()
        swap.begin()
        out_gradient()
        back(*units[1])
        scatter.join()
        g_copies = [
            send(g_ref.at[own_place(device[0])], g_arrived.at[k], g_send.at[k], g_recv.at[k], device)
            for k, device in enumerate(peers)
        ]
        for unit in units[2:]:
            back(*unit)
        for copy in g_copies:
            copy.wait_recv()
        g_total = g_ref[own_place(o)].astype(F32)
        for k in range(n_outer - 1):
            g_total = g_total + g_arrived[k].astype(F32)
        for d in range(2 * n_ctx):
            g_sum[d] = g_total[d * place_rows : (d + 1) * place_rows].astype(BF)
        qkv_gradient()
        g_swap.begin()
        scatter.end()
        swap.end()

        def finish(r):
            result_ref[r] = (h_ref[r] + total[r]).astype(BF)

        row_chunks(own_rows, 32, finish)
        g_swap.end()
        for copy in g_copies:
            copy.wait_send()

    outs = [
        shape(qkv.shape, BF),
        shape((own_rows, width), BF),
        shape(swapped.shape, BF),
        shape((2 * n_ctx, place_rows, features), BF),
        shape((qkv.shape[1] // LANES * HEAD_SIZE, width), BF),
    ]
    ins = [dh_all, xn, qkv, attn, lse, cosine, sine, pos_rows, pos_columns, hidden, out_w, down_w, h1, swapped]
    scratch = [
        pltpu.VMEM(xn.shape, BF),
        pltpu.VMEM(qkv.shape, BF),
        pltpu.VMEM(attn.shape, BF),
        pltpu.VMEM(cosine.shape, F32),
        pltpu.VMEM(sine.shape, F32),
        pltpu.VMEM(pos_columns.shape, jnp.int32),
        pltpu.VMEM((width, features), BF),
        pltpu.VMEM((n_outer - 1, width // n_outer, features), BF),
        pltpu.VMEM((2 * n_ctx, place_rows, features), BF),
        pltpu.SemaphoreType.DMA((n_outer - 1,)),
        pltpu.SemaphoreType.DMA((n_outer - 1,)),
        pltpu.VMEM((group, LANES), F32),
        pltpu.VMEM((group, LANES), F32),
        pltpu.VMEM(down_w.shape, BF),
        pltpu.VMEM(out_w.shape, BF),
        pltpu.VMEM(dh_all.shape, BF),
        pltpu.SemaphoreType.DMA((1,)),
        pltpu.SemaphoreType.DMA((8,)),
    ]
    scratch += swap_sems(1, n_ctx) + swap_sems(1, n_ctx) + scatter_scratch(own_rows, width)
    return remote_call(kernel, number, ins, outs, scratch, any_ins=(0, 1, 2, 3, 5, 6, 8, 10, 11))


def attention_input(dproj, w, tokens, dh1, gain, gain_terms, n_outer, n_ctx, number):
    rows, width = tokens.shape
    tile = 256
    features = dproj.shape[1]
    n = 2 * n_ctx

    def kernel(
        d_ref, w_hbm, x_ref, dh_ref, gain_ref, terms_ref, out_ref, sum_ref, w_ref, load_sem, *scratch
    ):
        swap_sem, scratch = scratch[:3], scratch[3:]
        terms, summed, arrived, send_sem, recv_sem, local_sem = scratch[:6]
        scratch = scratch[6:]
        total = scratch[-1]
        load = Load(padded_loads(w_hbm, w_ref), load_sem).begin()
        o = lax.axis_index("o")

        def partial(slot, t):
            a = d_ref[pl.ds(pl.multiple_of(slot * rows, rows), rows)]
            return nn(a, w_ref[:, pl.ds(pl.multiple_of(t * tile, tile), tile)])

        scatter = Scatter(n_ctx, partial, tile, *scratch)
        swap = Swap(n_ctx, [(terms_ref, terms)], *swap_sem)
        peers = outer_peers(n_outer)
        greet(swap.devices + peers)
        swap.begin()
        load.wait()
        scatter.to_mate()
        scatter.pairs()
        swap.end()
        summed[...] = jnp.sum(terms[...], 0)
        scatter.join()
        copies = []
        for k, device in enumerate(peers):
            copies.append(send(summed.at[device[0]], arrived.at[o], send_sem.at[k], recv_sem.at[k], device))
        own = pltpu.make_async_copy(summed.at[o], arrived.at[o], local_sem)
        own.start()
        scatter.end()

        def finish(r):
            x, d = x_ref[r].astype(F32), total[r]
            out_ref[r] = dh_ref[r] + norm_back(d, gain_ref[0:1], x, inv_rms(x))

        row_chunks(rows, 32, finish)
        for copy in copies:
            copy.wait_recv()
        own.wait()
        sum_ref[...] = jnp.sum(arrived[...], 0)
        for copy in copies:
            copy.wait_send()

    outs = [shape((rows, width), F32), shape((8, LANES), F32)]
    ins = [dproj, w, tokens, dh1, gain, gain_terms]
    n_loads = features // (LANES // 2)
    scratch = [pltpu.VMEM((features, width), BF), pltpu.SemaphoreType.DMA((n_loads,))]
    scratch += swap_sems(1, n_ctx)
    scratch += [
        pltpu.VMEM((n, n_outer, 8, LANES), F32),
        pltpu.VMEM((n_outer, 8, LANES), F32),
        pltpu.VMEM((n_outer, 8, LANES), F32),
        pltpu.SemaphoreType.DMA((n_outer - 1,)),
        pltpu.SemaphoreType.DMA((n_outer - 1,)),
        pltpu.SemaphoreType.DMA,
    ]
    scratch += scatter_scratch(rows, width)
    return remote_call(kernel, number, ins, outs, scratch, any_ins=(1,))


def make_shards(n_outer, n_inner, n_ctx):
    n_plane = n_inner * n_ctx
    moves = feature_moves(n_outer, n_plane)
    back = [(b, a) for a, b in moves]

    def layer(tokens, norm_attn, w_qkv, w_out, norm_mlp, w_gate_up, w_down, cotangent, seq_lengths, block_slot):
        _, width = tokens.shape
        gain_rows = norm_attn.shape[0]
        out_rows = w_out.shape[0]
        unit_rows = w_gate_up.shape[0]
        n_seqs, n_slots = seq_lengths.shape[1], block_slot.shape[1]
        units = FF // n_plane
        qkv_w = z_ag(lax.ppermute(w_qkv, ALL, moves)).reshape(CHUNKS, -1, width)
        gain_part = jnp.pad(jnp.stack([norm_attn, norm_mlp]), ((0, 6), (0, LANES - gain_rows)))
        meta = jnp.concatenate([seq_lengths[0], block_slot[0]])
        meta = jnp.pad(meta[None], ((0, 7), (0, LANES - n_seqs - n_slots)))
        out_parts = pad_heads(w_out, 1).reshape(out_rows, 2, n_plane // 2, -1).transpose(2, 1, 0, 3)
        out_parts = out_parts.reshape(n_plane, out_rows, -1)
        down_parts = w_down.reshape(out_rows, n_outer // 2, n_plane, unit_rows).transpose(2, 0, 1, 3)
        down_parts = down_parts.reshape(n_plane, out_rows, units)
        w_gate_up, out_parts, down_parts = lax.optimization_barrier((w_gate_up, out_parts, down_parts))
        gate_up = z_ag(w_gate_up)
        gate_up = gate_up.reshape(CHUNKS, -1, width)
        x_all, out_parts, down_w, gains, cosine, sine, pos_rows, pos_columns = prologue(
            tokens, out_parts, down_parts, gain_part, meta, n_seqs, n_outer, n_ctx, 1
        )
        x_all = x_all.reshape(-1, width)
        gains = gains[:, :, :2, :gain_rows].transpose(2, 0, 1, 3).reshape(2, width)
        down_w = z_ag(down_w.reshape(-1, units))
        qkv, attn, lse, dy_all, xn1, out_w = attention_forward(
            x_all, gains, qkv_w, cosine, sine, pos_rows, pos_columns, cotangent, out_parts, n_outer, n_ctx, 2
        )
        out_w = out_w.reshape(width, -1)
        h1, xn2 = output_projection(attn, out_w, tokens, gains, n_ctx, 3)
        xn2_all, hidden, dgu, dgu_t, g_down = feed_forward(xn2, dy_all, gate_up, down_w, n_ctx, 4)
        dgu, g_down = lax.optimization_barrier((dgu, g_down))
        g_down = z_rs(g_down)
        dh1, dh1_bf, dgain_two, g_gate_up = feed_forward_input(
            dgu, gate_up, h1, cotangent, gains, xn2_all.reshape(-1, width), dgu_t, n_ctx, 5
        )
        g_gate_up = z_rs(g_gate_up)
        dh1_all = plane_gather(dh1_bf, n_ctx, 6)
        dh1_all, g_down = lax.optimization_barrier((dh1_all, g_down))
        g_down = g_down.reshape(n_plane, out_rows, units)
        dproj, result, g_down, g_out, g_qkv = attention_backward(
            dh1_all, xn1, qkv, attn, lse, cosine, sine, pos_rows, pos_columns, hidden, out_w, down_w, h1, g_down, n_outer, n_ctx, 7
        )
        terms = jnp.sum(qkv_w.reshape(-1, width).astype(F32) * g_qkv.astype(F32), 0) / gains[0]
        terms = jnp.stack([terms, dgain_two[0]]).reshape(2, n_outer, n_plane, gain_rows).transpose(2, 1, 0, 3)
        terms = jnp.pad(terms, ((0, 0), (0, 0), (0, 6), (0, LANES - gain_rows)))
        dproj, g_qkv, g_gate_up = lax.optimization_barrier((dproj, g_qkv, g_gate_up))
        g_qkv = z_rs(g_qkv)
        grad_input, g = attention_input(dproj, qkv_w, tokens, dh1, gains, terms, n_outer, n_ctx, 8)
        grad_input, g_qkv = lax.optimization_barrier((grad_input, g_qkv))
        grad_qkv = lax.ppermute(g_qkv, ALL, back).astype(F32)
        g_out = g_out.reshape(n_plane // 2, 2, out_rows, -1).transpose(2, 1, 0, 3)
        grad_out = cut_heads(g_out.reshape(out_rows, -1), 1).astype(F32)
        grad_down = g_down.reshape(n_plane, out_rows, n_outer // 2, unit_rows).transpose(1, 2, 0, 3)
        grad_down = grad_down.reshape(out_rows, -1).astype(F32)
        g = g[:, :gain_rows]
        return (result, grad_input, g[0], grad_qkv, grad_out, g[1], g_gate_up.astype(F32), grad_down)

    return layer


def solution(mesh):
    n_inner = 2
    n_ctx = mesh.shape["ctx"]
    n_outer = mesh.shape["dp"] // n_inner
    split = Mesh(mesh.devices.reshape(n_outer, n_inner, n_ctx), ALL)
    rows, vec, grp = P(ALL, None), P(ALL), P(("o", "i"), None)
    return jax.shard_map(
        make_shards(n_outer, n_inner, n_ctx),
        mesh=split,
        in_specs=(rows, vec, rows, rows, vec, rows, rows, rows, grp, grp),
        out_specs=(rows, rows, vec, rows, rows, vec, rows, rows),
        check_vma=False,
    )
```

```python
import math

import jax
import jax.numpy as jnp
import numpy as np
from jax import lax
from jax.experimental import pallas as pl
from jax.experimental.pallas import tpu as pltpu
from jax.sharding import Mesh
from jax.sharding import PartitionSpec as P


QUERY_HEADS = 16
HEAD_SIZE = 96
FF = 4096
BLK = 128
LANES = 128
QUERY_BLOCK = 512
CHUNKS = 4

EPSILON = 1e-05
THETA = 100000.0
MASK_FILL = -1e30
BF = jnp.bfloat16
F32 = jnp.float32
ALL = ("o", "i", "ctx")
MESH = pl.DeviceIdType.MESH
SCALE = 1.0 / math.sqrt(HEAD_SIZE)


def nt(a, b):
    return lax.dot_general(a, b, (((1,), (1,)), ((), ())), preferred_element_type=F32)


def nn(a, b):
    return lax.dot_general(a, b, (((1,), (0,)), ((), ())), preferred_element_type=F32)


def tn(a, b):
    return lax.dot_general(a, b, (((0,), (0,)), ((), ())), preferred_element_type=F32)


def z_ag(x):
    return lax.all_gather(x, "o", axis=0, tiled=True)


def z_rs(x):
    return lax.psum_scatter(x, "o", scatter_dimension=0, tiled=True)


def inv_rms(x):
    return lax.rsqrt(jnp.mean(x * x, -1, keepdims=True) + EPSILON)


def norm_back(grad_normed, gain, source, scale):
    weighted = grad_normed * gain
    return scale * weighted - source * scale**3 * jnp.mean(weighted * source, -1, keepdims=True)


def feature_moves(n_outer, n_plane):
    moves = []
    half, quarter = n_outer // 2, n_outer // 4
    for block in range(n_outer * n_plane):
        if block < 4 * n_outer:
            head, step = block // half, block % half
        elif block < 6 * n_outer:
            head, step = divmod(block - 4 * n_outer, quarter)
            step += half
        else:
            head, step = divmod(block - 6 * n_outer, quarter)
            step += half + quarter
        place = 2 * (head % (n_plane // 2)) + head // (n_plane // 2)
        moves.append((block, step * n_plane + place))
    return moves


def pad_heads(x, axis):
    half = HEAD_SIZE // 2
    shape = x.shape
    x = x.reshape(shape[:axis] + (-1, half) + shape[axis + 1 :])
    pads = [(0, 0)] * x.ndim
    pads[axis + 1] = (0, LANES // 2 - half)
    return jnp.pad(x, pads).reshape(shape[:axis] + (-1,) + shape[axis + 1 :])


def cut_heads(x, axis):
    half = HEAD_SIZE // 2
    shape = x.shape
    x = x.reshape(shape[:axis] + (-1, LANES // 2) + shape[axis + 1 :])
    x = lax.slice_in_dim(x, 0, half, axis=axis + 1)
    return x.reshape(shape[:axis] + (-1,) + shape[axis + 1 :])


def places(n_ctx):
    o, i, c = lax.axis_index("o"), lax.axis_index("i"), lax.axis_index("ctx")
    return o, i, c, c + 1 - 2 * (c % 2), (c + n_ctx // 2) % n_ctx


def greet(devices):
    barrier = pltpu.get_barrier_semaphore()
    for device in devices:
        pl.semaphore_signal(barrier, inc=1, device_id=device, device_id_type=MESH)
    pl.semaphore_wait(barrier, len(devices))


def greet_neighbours(n_ctx):
    o, i, c, mate, far = places(n_ctx)
    greet([(o, i, mate), (o, 1 - i, c), (o, i, far)])


def send(src, dst, send_sem, recv_sem, device):
    copy = pltpu.make_async_remote_copy(
        src_ref=src, dst_ref=dst, send_sem=send_sem, recv_sem=recv_sem, device_id=device, device_id_type=MESH
    )
    copy.start()
    return copy


class Gather:
    def __init__(self, n_ctx, src, out, send_sem, recv_sem, local_sem):
        self.src, self.out, self.sems = src, out, (send_sem, recv_sem, local_sem)
        o, i, c, mate, far = places(n_ctx)
        j, core = 1 - i, c % 2
        self.mate, self.x, self.y = (o, i, mate), (o, j, c), (o, i, far)
        self.me, self.s_x = i * n_ctx + c, j * n_ctx + c
        self.s_y, self.s_d = i * n_ctx + far, j * n_ctx + far
        self.relay = (o, j * core + i * (1 - core), c * core + far * (1 - core))
        self.relayed = self.s_y * core + self.s_x * (1 - core)
        mate_far = (mate + n_ctx // 2) % n_ctx
        self.mates_slots = [i * n_ctx + mate, j * n_ctx + mate, i * n_ctx + mate_far, j * n_ctx + mate_far]
        self.copies = {}

    def go(self, kind, src, slot, device):
        copy = send(src, self.out.at[slot], self.sems[0].at[kind], self.sems[1].at[kind], device)
        self.copies[kind] = copy

    def begin(self):
        self.go(1, self.src, self.me, self.x)
        self.go(2, self.src, self.me, self.y)
        self.go(0, self.src, self.me, self.mate)
        self.own = pltpu.make_async_copy(self.src, self.out.at[self.me], self.sems[2])
        self.own.start()

    def middle(self):
        self.copies[1].wait_recv()
        self.copies[2].wait_recv()
        self.go(5, self.out.at[self.relayed], self.relayed, self.relay)
        self.go(3, self.out.at[self.s_x], self.s_x, self.mate)
        self.go(4, self.out.at[self.s_y], self.s_y, self.mate)

    def corner(self):
        self.copies[5].wait_recv()
        self.go(6, self.out.at[self.s_d], self.s_d, self.mate)

    def arrived(self, kind):
        self.copies[kind].wait_recv()

    def sent(self):
        self.own.wait()
        for copy in self.copies.values():
            copy.wait_send()

    def end(self):
        self.corner()
        for kind in (0, 3, 4, 6):
            self.arrived(kind)
        self.sent()


GATHER_SEMS = [pltpu.SemaphoreType.DMA((7,)), pltpu.SemaphoreType.DMA((7,)), pltpu.SemaphoreType.DMA]


class Scatter:
    def __init__(self, n_ctx, partial, tile, ready, from_mate, going, got, send_sem, recv_sem, total):
        self.partial, self.tile = partial, tile
        self.ready, self.from_mate, self.going, self.got = ready, from_mate, going, got
        self.sems, self.total = (send_sem, recv_sem), total
        o, i, c, mate, far = places(n_ctx)
        j, core = 1 - i, c % 2
        self.core = core
        far_mate = (mate + n_ctx // 2) % n_ctx
        self.mine = [j * n_ctx + far, j * n_ctx + c, i * n_ctx + far, i * n_ctx + c]
        self.theirs = [j * n_ctx + far_mate, j * n_ctx + mate, i * n_ctx + far_mate, i * n_ctx + mate]
        self.mate = (o, i, mate)
        self.combined = (o, j * (1 - core) + i * core, c * (1 - core) + far * core)
        self.direct = (o, j * core + i * (1 - core), c * core + far * (1 - core))
        self.s_direct = self.mine[2] * (1 - core) + self.mine[1] * core
        self.s_combined = self.mine[1] * (1 - core) + self.mine[2] * core
        self.copies = []

    def go(self, kind, part, src, dst, device):
        copy = send(src.at[part], dst.at[part], self.sems[0].at[kind, part], self.sems[1].at[kind, part], device)
        self.copies.append(copy)
        return copy

    def each(self, part, body):
        tiles = self.ready.shape[-1] // self.tile

        @pl.loop(0, tiles)
        def _(t):
            at = pl.multiple_of(t * self.tile, self.tile)
            body(part * tiles + t, pl.ds(at, self.tile), pl.ds(part * tiles * self.tile + at, self.tile))

    def fill(self, n, part):
        def body(t, lanes, _):
            self.ready[n, part, :, lanes] = self.partial(self.theirs[n], t).astype(BF)

        self.each(part, body)

    def give(self, n, part):
        self.mates[n, part] = self.go(n, part, self.ready.at[n], self.from_mate.at[n], self.mate)

    def pair(self, slot, n, part, place):
        def body(t, lanes, _):
            pair = self.partial(slot, t) + self.from_mate[n, part, :, lanes].astype(F32)
            self.going[place, part, :, lanes] = pair.astype(BF)

        self.each(part, body)

    def to_mate(self):
        self.mates, self.straights, self.diagonals, self.joins = {}, [], [], []
        order = [(0, 0), (0, 1), (1, 0), (2, 0), (1, 1), (2, 1), (3, 0), (3, 1)]
        self.fill(*order[0])
        for k, at in enumerate(order[1:]):
            self.fill(*at)
            self.give(*order[k])
            if k == 2:
                self.mates[0, 0].wait_recv()
                self.pair(self.mine[0], 0, 0, 0)
            if k == 3:
                self.diagonals.append(self.go(4, 0, self.going.at[0], self.got.at[0], self.direct))
                self.mates[0, 1].wait_recv()
                self.pair(self.mine[0], 0, 1, 0)
            if k == 4:
                self.diagonals.append(self.go(4, 1, self.going.at[0], self.got.at[0], self.direct))
        self.last = order[-1]

    def pairs(self):
        for part in range(PARTS):
            self.mates[1, part].wait_recv()
            self.mates[2, part].wait_recv()
            self.pair(self.s_direct, 2 - self.core, part, 1)
            if part == 0:
                self.give(*self.last)
            else:
                self.straights.append(self.go(5, part - 1, self.going.at[1], self.got.at[1], self.direct))

    def join(self):
        for part in range(PARTS):
            self.diagonals[part].wait_recv()
            if part == 0:
                self.straights.append(self.go(5, PARTS - 1, self.going.at[1], self.got.at[1], self.direct))

            def combined(t, lanes, _):
                pair = self.partial(self.s_combined, t) + self.from_mate[1 + self.core, part, :, lanes].astype(F32)
                self.going[2, part, :, lanes] = (pair + self.got[0, part, :, lanes].astype(F32)).astype(BF)

            self.each(part, combined)
            if part:
                self.joins.append(self.go(6, part - 1, self.going.at[2], self.got.at[2], self.combined))
        self.own(0)
        self.joins.append(self.go(6, PARTS - 1, self.going.at[2], self.got.at[2], self.combined))

    def own(self, part):
        self.mates[3, part].wait_recv()

        def body(t, lanes, out):
            self.total[:, out] = self.partial(self.mine[3], t) + self.from_mate[3, part, :, lanes].astype(F32)

        self.each(part, body)

    def end(self):
        total = self.total
        for part in range(1, PARTS):
            self.own(part)
        for part in range(PARTS):
            self.straights[part].wait_recv()
            self.joins[part].wait_recv()

            def rest(t, lanes, out):
                other = self.got[1, part, :, lanes].astype(F32) + self.got[2, part, :, lanes].astype(F32)
                total[:, out] = total[:, out] + other

            self.each(part, rest)
        for copy in self.copies:
            copy.wait_send()


PARTS = 2


def scatter_scratch(rows, width):
    return [
        pltpu.VMEM((4, PARTS, rows, width // PARTS), BF),
        pltpu.VMEM((4, PARTS, rows, width // PARTS), BF),
        pltpu.VMEM((3, PARTS, rows, width // PARTS), BF),
        pltpu.VMEM((3, PARTS, rows, width // PARTS), BF),
        pltpu.SemaphoreType.DMA((7, PARTS)),
        pltpu.SemaphoreType.DMA((7, PARTS)),
        pltpu.VMEM((rows, width), F32),
    ]


def row_chunks(rows, step, body):
    @pl.loop(0, rows // step)
    def _(r):
        body(pl.ds(pl.multiple_of(r * step, step), step))


class Load:
    def __init__(self, parts, sem):
        self.copies = [pltpu.make_async_copy(src, dst, sem.at[n]) for n, (src, dst) in enumerate(parts)]

    def begin(self):
        for copy in self.copies:
            copy.start()
        return self

    def wait(self):
        for copy in self.copies:
            copy.wait()


IN_VMEM = pl.BlockSpec(memory_space=pltpu.VMEM)
ANYWHERE = pl.BlockSpec(memory_space=pl.ANY)


def remote_call(kernel, number, ins, outs, scratch, any_outs=(), any_ins=()):
    return pl.pallas_call(
        kernel,
        out_shape=outs,
        in_specs=[ANYWHERE if n in any_ins else IN_VMEM for n in range(len(ins))],
        out_specs=[ANYWHERE if n in any_outs else IN_VMEM for n in range(len(outs))],
        scratch_shapes=scratch,
        compiler_params=pltpu.CompilerParams(collective_id=number, has_side_effects=True, vmem_limit_bytes=60 << 20),
    )(*ins)


def shape(dims, dtype):
    return jax.ShapeDtypeStruct(tuple(dims), dtype)


class Swap:
    def __init__(self, n_ctx, pairs, send_sem, recv_sem, local_sem):
        self.pairs, self.sems = pairs, (send_sem, recv_sem, local_sem)
        self.o, i, c, _, _ = places(n_ctx)
        self.n, self.n_ctx = 2 * n_ctx, n_ctx
        self.me = i * n_ctx + c
        self.others = [(self.me + k) % self.n for k in range(1, self.n)]
        self.devices = [(self.o, d // n_ctx, d % n_ctx) for d in self.others]

    def begin(self):
        self.copies, self.own = [], []
        for a, (src, dst) in enumerate(self.pairs):
            for k, (d, device) in enumerate(zip(self.others, self.devices)):
                self.copies.append(
                    send(src.at[d], dst.at[self.me], self.sems[0].at[a, k], self.sems[1].at[a, k], device)
                )
            own = pltpu.make_async_copy(src.at[self.me], dst.at[self.me], self.sems[2].at[a])
            own.start()
            self.own.append(own)

    def end(self):
        for copy in self.copies:
            copy.wait_recv()
            copy.wait_send()
        for copy in self.own:
            copy.wait()


def swap_sems(n_arrays, n_ctx):
    return [
        pltpu.SemaphoreType.DMA((n_arrays, 2 * n_ctx - 1)),
        pltpu.SemaphoreType.DMA((n_arrays, 2 * n_ctx - 1)),
        pltpu.SemaphoreType.DMA((n_arrays,)),
    ]


def outer_peers(n_outer):
    o, i, c = lax.axis_index("o"), lax.axis_index("i"), lax.axis_index("ctx")
    return [(lax.rem(o + k, n_outer), i, c) for k in range(1, n_outer)]


def rotary_constants():
    frequency = THETA ** -(np.arange(HEAD_SIZE // 2) * (2.0 / HEAD_SIZE))
    rates = np.zeros((8, LANES), np.float32)
    for half, sign in ((0, -1.0), (LANES // 2, 1.0)):
        rates[0, half : half + HEAD_SIZE // 2] = frequency
        rates[1, half : half + HEAD_SIZE // 2] = sign
    angles = np.arange(BLK)[:, None] * rates[0].astype(np.float64)
    return rates, np.stack([np.cos(angles), np.sin(angles)]).astype(np.float32)


def prologue(tokens, out_parts, down_parts, gains, meta, n_seqs, n_outer, n_ctx, number):
    rows, width = tokens.shape
    n = 2 * n_ctx
    blocks = n_ctx * rows // BLK

    def kernel(
        x_ref,
        out_src,
        down_src,
        gains_ref,
        meta_ref,
        rates_ref,
        angles_ref,
        x_all,
        out_dst,
        down_dst,
        gains_out,
        cos_ref,
        sin_ref,
        rows_ref,
        columns_ref,
        *sems,
    ):
        o = lax.axis_index("o")
        metas_ref, send_sem, recv_sem, local_sem = sems[:4]
        out_swap = Swap(n_ctx, [(out_src, out_dst)], *sems[4:7])
        down_swap = Swap(n_ctx, [(down_src, down_dst)], *sems[7:10])
        gather = Gather(n_ctx, x_ref, x_all, *sems[10:])
        peers = outer_peers(n_outer)
        me = out_swap.me
        greet(out_swap.devices + peers)
        gather.begin()
        own = [
            pltpu.make_async_copy(meta_ref, metas_ref.at[me], local_sem.at[0]),
            pltpu.make_async_copy(gains_ref, gains_out.at[o, me], local_sem.at[1]),
        ]
        meta_copies, gain_copies, z_copies = [], [], []
        for copy in own:
            copy.start()
        for k, device in enumerate(out_swap.devices):
            meta_copies.append(send(meta_ref, metas_ref.at[me], send_sem.at[0, k], recv_sem.at[0, k], device))
            gain_copies.append(send(gains_ref, gains_out.at[o, me], send_sem.at[1, k], recv_sem.at[1, k], device))
        out_swap.begin()
        for copy in own:
            copy.wait()
        for copy in meta_copies:
            copy.wait_recv()
        lane = lax.broadcasted_iota(jnp.int32, (BLK, LANES), 1)
        row = lax.broadcasted_iota(jnp.int32, (BLK, LANES), 0)
        rows_ref[...] = jnp.zeros_like(rows_ref)
        pieces = 2 * blocks * n_seqs
        piece = lax.broadcasted_iota(jnp.int32, (pieces, LANES), 0)
        bases = jnp.zeros((pieces, LANES), jnp.int32)
        places_of = []
        for g in range(2):
            starts, end = [], jnp.zeros((1, 1), jnp.int32)
            for q in range(n_seqs):
                starts.append(end)
                end = end + metas_ref[g * n_ctx, 0:1, q : q + 1]
            for b in range(blocks):
                first = metas_ref[g * n_ctx, 0:1, n_seqs + b : n_seqs + b + 1] * BLK
                for q in range(n_seqs):
                    index = (g * blocks + b) * n_seqs + q
                    bases = jnp.where(piece == index, first - starts[q], bases)
                places_of.append((first, starts))
        angle = bases.astype(F32) * rates_ref[0:1]
        base_cos, base_sin = jnp.cos(angle), jnp.sin(angle)
        for n_block, (first, starts) in enumerate(places_of):
            at = slice(n_block * BLK, (n_block + 1) * BLK)
            stream, lanes_stream = first + row, first + lane[0:1]
            start, lanes_start = jnp.zeros_like(stream), jnp.zeros_like(lanes_stream)
            cos, sin = angles_ref[0], angles_ref[1]
            for q in range(n_seqs):
                index = n_block * n_seqs + q
                cos_0, sin_0 = base_cos[index : index + 1], base_sin[index : index + 1]
                cos_q = cos_0 * angles_ref[0] - sin_0 * angles_ref[1]
                sin_q = sin_0 * angles_ref[0] + cos_0 * angles_ref[1]
                inside = stream >= starts[q]
                start = jnp.where(inside, starts[q], start)
                lanes_start = jnp.where(lanes_stream >= starts[q], starts[q], lanes_start)
                cos, sin = jnp.where(inside, cos_q, cos), jnp.where(inside, sin_q, sin)
            cos_ref[at] = cos
            sin_ref[at] = sin * rates_ref[1:2]
            columns_ref[at] = jnp.where(lane == 0, stream, start)
            rows_ref[0:1, at] = lanes_stream
            rows_ref[1:2, at] = lanes_start
        for copy in gain_copies:
            copy.wait_recv()
        for k, device in enumerate(peers):
            z_copies.append(send(gains_out.at[o], gains_out.at[o], send_sem.at[2, k], recv_sem.at[2, k], device))
        gather.middle()
        down_swap.begin()
        gather.end()
        out_swap.end()
        down_swap.end()
        for copy in z_copies:
            copy.wait_recv()
        for copy in meta_copies + gain_copies + z_copies:
            copy.wait_send()

    outs = [
        shape((n, rows, width), BF),
        shape(out_parts.shape, BF),
        shape(down_parts.shape, BF),
        shape((n_outer, n) + gains.shape, F32),
        shape((n * rows, LANES), F32),
        shape((n * rows, LANES), F32),
        shape((8, n * rows), jnp.int32),
        shape((n * rows, LANES), jnp.int32),
    ]
    rates, angles = rotary_constants()
    ins = [tokens, out_parts, down_parts, gains, meta, jnp.asarray(rates), jnp.asarray(angles)]
    most = max(n, n_outer) - 1
    scratch = [
        pltpu.VMEM((n,) + meta.shape, jnp.int32),
        pltpu.SemaphoreType.DMA((3, most)),
        pltpu.SemaphoreType.DMA((3, most)),
        pltpu.SemaphoreType.DMA((2,)),
    ]
    scratch += swap_sems(1, n_ctx) + swap_sems(1, n_ctx) + GATHER_SEMS
    return remote_call(kernel, number, ins, outs, scratch, any_outs=(0,))


def rotate(x, cosine, sine):
    return x * cosine + pltpu.roll(x, LANES // 2, 1) * sine


def qkv_rows(features):
    return features // LANES * HEAD_SIZE // CHUNKS


def padded_loads(w_ref, w_pad):
    half = HEAD_SIZE // 2
    rows = qkv_rows(w_pad.shape[0])
    pairs, at = [], 0
    for row in range(half, w_pad.shape[0], LANES // 2):
        w_pad[row : row + LANES // 2 - half] = jnp.zeros((LANES // 2 - half, w_pad.shape[1]), BF)
    for n in range(w_ref.shape[0]):
        for b in range(rows // half):
            src = w_ref.at[n, pl.ds(b * half, half)]
            pairs.append((src, w_pad.at[pl.ds(at * LANES // 2, half)]))
            at += 1
    return pairs


def attention_forward(x_all, gains, w, cosine, sine, pos_rows, pos_columns, dy, out_part, n_outer, n_ctx, number):
    rows, width = x_all.shape
    group = rows // 2
    heads = QUERY_HEADS // (2 * n_ctx)
    features = (heads + 2) * LANES
    k_at, v_at = heads * LANES, (heads + 1) * LANES
    block = min(QUERY_BLOCK, group)
    n_loads = features // (LANES // 2)

    def kernel(
        x_hbm,
        gain_ref,
        w_hbm,
        cos_ref,
        sin_ref,
        rows_ref,
        columns_ref,
        dy_ref,
        part_ref,
        qkv_ref,
        attn_ref,
        lse_ref,
        dy_all,
        xn_out,
        out_w,
        w_ref,
        xn_ref,
        load_sem,
        xn_sem,
        store_sem,
        z_send,
        z_recv,
        z_local,
        *sems,
    ):
        gather = Gather(n_ctx, dy_ref, dy_all, *sems)
        load = Load(padded_loads(w_hbm, w_ref), load_sem).begin()
        xn_load = Load([(x_hbm, xn_ref)], xn_sem).begin()
        o = lax.axis_index("o")
        peers = outer_peers(n_outer)
        greet([gather.mate, gather.x, gather.y] + peers)
        gather.begin()
        z_copies = [send(part_ref, out_w.at[o], z_send.at[k], z_recv.at[k], device) for k, device in enumerate(peers)]
        own_part = pltpu.make_async_copy(part_ref, out_w.at[o], z_local)
        own_part.start()
        load.wait()
        xn_load.wait()

        def normalise(r):
            x = xn_ref[r].astype(F32)
            xn_ref[r] = (x * inv_rms(x) * gain_ref[0:1]).astype(BF)

        def project(r):
            cos, sin = cos_ref[r], sin_ref[r]
            for h in range(heads + 2):
                lanes = slice(h * LANES, (h + 1) * LANES)
                part = nt(xn_ref[r], w_ref[lanes])
                qkv_ref[r, lanes] = (rotate(part, cos, sin) if h <= heads else part).astype(BF)

        def attend(g):
            keys_at = pl.ds(g * group, group)

            @pl.loop(0, group // block)
            def _(b):
                r = pl.ds(pl.multiple_of(g * group + b * block, block), block)
                key_pos = rows_ref[0:1, keys_at]
                ok = (key_pos >= columns_ref[r, 1:2]) & (key_pos <= columns_ref[r, 0:1])
                for h in range(heads):
                    lanes = slice(h * LANES, (h + 1) * LANES)
                    s = nt(qkv_ref[r, lanes], qkv_ref[keys_at, k_at : k_at + LANES])
                    s = jnp.where(ok, s, MASK_FILL)
                    high = jnp.max(s, -1, keepdims=True)
                    e = jnp.exp((s - high) * SCALE)
                    total = jnp.sum(e, -1, keepdims=True)
                    mixed = nn(e.astype(BF), qkv_ref[keys_at, v_at : v_at + LANES])
                    attn_ref[r, lanes] = (mixed / total).astype(BF)
                    lse = jnp.broadcast_to(high * SCALE + jnp.log(total), (block, LANES))
                    lse_ref[h : h + 1, r] = jnp.transpose(lse)[0:1]

        row_chunks(rows, 64, normalise)
        row_chunks(rows, block, project)
        gather.middle()
        store = Load([(xn_ref, xn_out)], store_sem).begin()
        attend(0)
        attend(1)
        gather.end()
        store.wait()
        own_part.wait()
        for copy in z_copies:
            copy.wait_recv()
            copy.wait_send()

    outs = [
        shape((rows, features), BF),
        shape((rows, heads * LANES), BF),
        shape((8, rows), F32),
        shape((2 * n_ctx,) + dy.shape, BF),
        shape(x_all.shape, BF),
        shape((n_outer,) + out_part.shape, BF),
    ]
    ins = [x_all, gains, w, cosine, sine, pos_rows, pos_columns, dy, out_part]
    scratch = [
        pltpu.VMEM((features, width), BF),
        pltpu.VMEM(x_all.shape, BF),
        pltpu.SemaphoreType.DMA((n_loads,)),
        pltpu.SemaphoreType.DMA((1,)),
        pltpu.SemaphoreType.DMA((1,)),
        pltpu.SemaphoreType.DMA((n_outer - 1,)),
        pltpu.SemaphoreType.DMA((n_outer - 1,)),
        pltpu.SemaphoreType.DMA,
    ]
    scratch += GATHER_SEMS
    got = remote_call(kernel, number, ins, outs, scratch, any_outs=(3, 4), any_ins=(0, 2))
    return got[0], got[1], got[2], got[3].reshape(rows, width), got[4], got[5]


def output_projection(attn, out_w, tokens, gain, down_part, n_outer, n_ctx, number):
    rows, width = tokens.shape
    tile = 256


    def kernel(attn_ref, w_ref, x_ref, gain_ref, part_ref, h_ref, xn_ref, down_w, z_send, z_recv, z_local, *scratch):
        total = scratch[-1]

        def partial(slot, t):
            a = attn_ref[pl.ds(pl.multiple_of(slot * rows, rows), rows)]
            return nt(a, w_ref[pl.ds(pl.multiple_of(t * tile, tile), tile)])

        scatter = Scatter(n_ctx, partial, tile, *scratch)
        o, i, c, mate, far = places(n_ctx)
        peers = outer_peers(n_outer)
        greet([(o, i, mate), (o, 1 - i, c), (o, i, far)] + peers)
        z_copies = [send(part_ref, down_w.at[o], z_send.at[k], z_recv.at[k], device) for k, device in enumerate(peers)]
        own_part = pltpu.make_async_copy(part_ref, down_w.at[o], z_local)
        own_part.start()
        scatter.to_mate()
        scatter.pairs()
        scatter.join()
        scatter.end()

        def finish(r):
            h = x_ref[r].astype(F32) + total[r]
            h_ref[r] = h
            xn_ref[r] = (h * inv_rms(h) * gain_ref[1:2]).astype(BF)

        row_chunks(rows, 32, finish)
        own_part.wait()
        for copy in z_copies:
            copy.wait_recv()
            copy.wait_send()

    outs = [shape((rows, width), F32), shape((rows, width), BF), shape((n_outer,) + down_part.shape, BF)]
    sems = [
        pltpu.SemaphoreType.DMA((n_outer - 1,)),
        pltpu.SemaphoreType.DMA((n_outer - 1,)),
        pltpu.SemaphoreType.DMA,
    ]
    ins = [attn, out_w, tokens, gain, down_part]
    return remote_call(kernel, number, ins, outs, sems + scatter_scratch(rows, width), any_outs=(2,))


def feed_forward(xn, dy, gate_up, down, n_ctx, number):
    rows, width = xn.shape
    n = 2 * n_ctx
    chunks, unit_rows, _ = gate_up.shape
    units = down.shape[1]
    tile = 256

    def kernel(
        x_ref,
        dy_hbm,
        up_hbm,
        down_hbm,
        xn_all,
        hidden_ref,
        dgu_ref,
        dgu_t,
        g_down_ref,
        raw,
        dy_ref,
        up_ref,
        down_ref,
        hidden_t,
        g_acc,
        load_sem,
        store_sem,
        *sems,
    ):
        gather = Gather(n_ctx, x_ref, raw, *sems)
        pairs = [(up_hbm, up_ref), (down_hbm, down_ref), (dy_hbm, dy_ref)]
        load = Load(pairs, load_sem).begin()
        greet_neighbours(n_ctx)
        gather.begin()
        half = chunks // 2
        core = gather.me % 2

        def chip(slot):
            both = pl.ds(pl.multiple_of((slot - core) * rows, 2 * rows), 2 * rows)
            x = raw[pl.ds(slot - core, 2)].reshape(2 * rows, width)
            for m in range(half):
                lanes = slice(m * unit_rows, (m + 1) * unit_rows)
                second = slice(units + m * unit_rows, units + (m + 1) * unit_rows)
                gate = nt(x, up_ref[m])
                up = nt(x, up_ref[half + m])
                dhid = nn(dy_ref[both], down_ref[:, lanes])
                sg = 1.0 / (1.0 + jnp.exp(-gate))
                act = gate * sg
                hidden = act * up
                dgate = dhid * up * sg * (1.0 + gate * (1.0 - sg))
                dup = dhid * act
                hidden_ref[both, lanes] = hidden.astype(BF)
                dgu_ref[both, lanes] = dgate.astype(BF)
                dgu_ref[both, second] = dup.astype(BF)
                hidden_t[lanes] = jnp.transpose(hidden).astype(BF)
                dgu_t[lanes, both] = jnp.transpose(dgate).astype(BF)
                dgu_t[second, both] = jnp.transpose(dup).astype(BF)

            @pl.loop(0, width // tile)
            def _(t):
                lanes = pl.ds(pl.multiple_of(t * tile, tile), tile)
                g = nn(hidden_t[...], dy_ref[both, lanes])
                g_acc[:, lanes] = g if slot is gather.me else g_acc[:, lanes] + g

        stores = []

        def store(slot):
            copy = pltpu.make_async_copy(raw.at[slot], xn_all.at[slot], store_sem.at[len(stores)])
            copy.start()
            stores.append(copy)

        load.wait()
        gather.arrived(0)
        gather.own.wait()
        store(gather.me)
        store(gather.mates_slots[0])
        chip(gather.me)
        gather.middle()
        gather.arrived(3)
        store(gather.s_x)
        store(gather.mates_slots[1])
        chip(gather.s_x)
        gather.arrived(4)
        store(gather.s_y)
        store(gather.mates_slots[2])
        chip(gather.s_y)
        gather.corner()
        gather.arrived(6)
        store(gather.s_d)
        store(gather.mates_slots[3])
        chip(gather.s_d)

        @pl.loop(0, width // tile)
        def _(t):
            lanes = pl.ds(pl.multiple_of(t * tile, tile), tile)
            g_down_ref[lanes] = jnp.transpose(g_acc[:, lanes]).astype(BF)

        for copy in gather.copies.values():
            copy.wait_send()
        for copy in stores:
            copy.wait()

    outs = [
        shape((n, rows, width), BF),
        shape((n * rows, units), BF),
        shape((n * rows, 2 * units), BF),
        shape((2 * units, n * rows), BF),
        shape((width, units), BF),
    ]
    scratch = [
        pltpu.VMEM((n, rows, width), BF),
        pltpu.VMEM(dy.shape, BF),
        pltpu.VMEM(gate_up.shape, BF),
        pltpu.VMEM(down.shape, BF),
        pltpu.VMEM((units, 2 * rows), BF),
        pltpu.VMEM((units, width), F32),
        pltpu.SemaphoreType.DMA((3,)),
        pltpu.SemaphoreType.DMA((n,)),
    ]
    ins = [xn, dy, gate_up, down]
    return remote_call(kernel, number, ins, outs, scratch + GATHER_SEMS, any_outs=(0,), any_ins=(1, 2, 3))


def feed_forward_input(dgu, gate_up, h1, cotangent, gain, xn_all, dgu_t, n_ctx, number):
    rows, width = h1.shape
    chunks, unit_rows, _ = gate_up.shape
    units = chunks * unit_rows // 2
    tile, part = 256, 256

    def kernel(
        dgu_ref,
        w_hbm,
        h_ref,
        dy_ref,
        gain_ref,
        xn_hbm,
        dgu_t_hbm,
        dh_ref,
        dhb_all,
        dgain_ref,
        g_up_ref,
        w_ref,
        xn_ref,
        dgu_t_ref,
        dhb_ref,
        w_sem,
        load_sem,
        *scratch,
    ):
        gather_sems, scratch = scratch[:3], scratch[3:]
        total = scratch[-1]
        gather = Gather(n_ctx, dhb_ref, dhb_all, *gather_sems)
        w_load = Load([(w_hbm, w_ref)], w_sem).begin()
        load = Load([(dgu_t_hbm, dgu_t_ref), (xn_hbm, xn_ref)], load_sem).begin()

        def partial(slot, t):
            r = pl.ds(pl.multiple_of(slot * rows, rows), rows)
            lanes = pl.ds(pl.multiple_of(t * tile, tile), tile)
            acc = nn(dgu_ref[r, :unit_rows], w_ref[0, :, lanes])
            for n in range(1, chunks):
                acc = acc + nn(dgu_ref[r, n * unit_rows : (n + 1) * unit_rows], w_ref[n, :, lanes])
            return acc

        def up_gradient(first, last):
            @pl.loop(first, last)
            def _(k):
                r = pl.ds(pl.multiple_of(k * part, part), part)

                @pl.loop(0, width // tile)
                def _(t):
                    lanes = pl.ds(pl.multiple_of(t * tile, tile), tile)
                    g_up_ref[r, lanes] = nn(dgu_t_ref[r], xn_ref[:, lanes]).astype(BF)

        scatter = Scatter(n_ctx, partial, tile, *scratch)
        greet_neighbours(n_ctx)
        w_load.wait()
        scatter.to_mate()
        scatter.pairs()
        load.wait()
        up_gradient(0, units // part)
        scatter.join()
        scatter.end()
        dgain_ref[...] = jnp.zeros_like(dgain_ref)

        def finish(r):
            h, d = h_ref[r], total[r]
            scale = inv_rms(h)
            dgain_ref[0:1] += jnp.sum(d * h * scale, 0, keepdims=True)
            dh = dy_ref[r].astype(F32) + norm_back(d, gain_ref[1:2], h, scale)
            dh_ref[r] = dh
            dhb_ref[r] = dh.astype(BF)

        row_chunks(rows, 32, finish)
        up_gradient(units // part, units // part + 1)
        gather.begin()
        up_gradient(units // part + 1, 2 * units // part)
        gather.middle()
        gather.end()

    outs = [
        shape((rows, width), F32),
        shape((2 * n_ctx, rows, width), BF),
        shape((8, width), F32),
        shape((2 * units, width), BF),
    ]
    scratch = [
        pltpu.VMEM((chunks, unit_rows, width), BF),
        pltpu.VMEM(xn_all.shape, BF),
        pltpu.VMEM(dgu_t.shape, BF),
        pltpu.VMEM((rows, width), BF),
        pltpu.SemaphoreType.DMA((1,)),
        pltpu.SemaphoreType.DMA((2,)),
    ]
    return remote_call(
        kernel,
        number,
        [dgu, gate_up, h1, cotangent, gain, xn_all, dgu_t],
        outs,
        scratch + GATHER_SEMS + scatter_scratch(rows, width),
        any_outs=(1,),
        any_ins=(1, 5, 6),
    )


def attention_backward(
    dh_all, xn, qkv, attn, lse, cosine, sine, pos_rows, pos_columns, hidden, out_w, down_w, h1, swapped, n_outer, n_ctx, number
):
    rows = dh_all.shape[0]
    own_rows, width = h1.shape
    group = rows // 2
    heads = attn.shape[1] // LANES
    k_at, v_at = heads * LANES, (heads + 1) * LANES
    block = min(QUERY_BLOCK, group)
    features = attn.shape[1]
    tile = 256
    place_rows = width // n_outer // (2 * n_ctx)

    def kernel(
        dh_hbm,
        xn_hbm,
        qkv_hbm,
        attn_hbm,
        lse_ref,
        cos_hbm,
        sin_hbm,
        rows_ref,
        columns_hbm,
        hidden_ref,
        out_w_hbm,
        w_hbm,
        h_ref,
        swap_src,
        dproj_ref,
        result_ref,
        swap_dst,
        g_dst,
        g_qkv_ref,
        xn_ref,
        qkv_ref,
        attn_ref,
        cos_ref,
        sin_ref,
        columns_ref,
        g_ref,
        g_arrived,
        g_sum,
        g_send,
        g_recv,
        dk_ref,
        dv_ref,
        w_ref,
        out_w_ref,
        dh_ref,
        load_sem,
        dh_sem,
        *scratch,
    ):
        swap_sem, g_swap_sem, scratch = scratch[:3], scratch[3:6], scratch[6:]
        total = scratch[-1]
        o = lax.axis_index("o")
        peers = outer_peers(n_outer)
        load = Load([(w_hbm, w_ref)], load_sem).begin()
        pairs = [(out_w_hbm, out_w_ref), (dh_hbm, dh_ref), (attn_hbm, attn_ref), (qkv_hbm, qkv_ref), (cos_hbm, cos_ref), (sin_hbm, sin_ref)]
        dh_load = Load(pairs + [(columns_hbm, columns_ref), (xn_hbm, xn_ref)], dh_sem).begin()
        swap = Swap(n_ctx, [(swap_src, swap_dst)], *swap_sem)
        g_swap = Swap(n_ctx, [(g_sum, g_dst)], *g_swap_sem)

        def partial(slot, t):
            a = hidden_ref[pl.ds(pl.multiple_of(slot * own_rows, own_rows), own_rows)]
            return nt(a, w_ref[pl.ds(pl.multiple_of(t * tile, tile), tile)])

        scatter = Scatter(n_ctx, partial, tile, *scratch)
        greet(swap.devices + peers)

        def back(g, b):
            keys_at = pl.ds(g * group, group)
            r = pl.ds(g * group + b * block, block)
            if b == 0:
                dk_ref[...] = jnp.zeros_like(dk_ref)
                dv_ref[...] = jnp.zeros_like(dv_ref)
            key_pos = columns_ref[keys_at, 0:1]
            ok = (key_pos >= rows_ref[1:2, r]) & (key_pos <= rows_ref[0:1, r])
            da_all = nn(dh_ref[r], out_w_ref[...]).astype(BF)

            for h in range(heads):
                lanes = slice(h * LANES, (h + 1) * LANES)
                da, q = da_all[:, lanes], qkv_ref[r, lanes]
                keys = qkv_ref[keys_at, k_at : k_at + LANES]
                s = nt(keys, q) * SCALE - lse_ref[h : h + 1, r]
                p = jnp.exp(jnp.where(ok, s, MASK_FILL))
                dv_ref[...] += nn(p.astype(BF), da)
                delta = jnp.transpose(da.astype(F32) * attn_ref[r, lanes].astype(F32))
                delta = jnp.sum(delta, 0, keepdims=True)
                dp = nt(qkv_ref[keys_at, v_at : v_at + LANES], da)
                ds = (p * (dp - delta)).astype(BF)
                dk_ref[...] += nn(ds, q)
                dq = tn(ds, keys) * SCALE
                dproj_ref[r, lanes] = rotate(dq, cos_ref[r], -sin_ref[r]).astype(BF)

            if b == group // block - 1:
                dk = rotate(dk_ref[...] * SCALE, cos_ref[keys_at], -sin_ref[keys_at])
                dproj_ref[keys_at, k_at : k_at + LANES] = dk.astype(BF)
                dproj_ref[keys_at, v_at : v_at + LANES] = dv_ref[...].astype(BF)

        def out_gradient():
            @pl.loop(0, width // 384)
            def _(k):
                d = pl.ds(pl.multiple_of(k * 384, 384), 384)
                g_ref[d] = jnp.transpose(tn(attn_ref[...], dh_ref[:, d])).astype(BF)

        def own_place(outer):
            return pl.ds(pl.multiple_of(outer * (width // n_outer), 16), width // n_outer)

        def qkv_gradient():
            half = HEAD_SIZE // 2

            @pl.loop(0, width // 256)
            def _(t):
                lanes = pl.ds(pl.multiple_of(t * 256, 256), 256)
                for h in range(heads + 2):
                    g = tn(dproj_ref[:, h * LANES : (h + 1) * LANES], xn_ref[:, lanes]).astype(BF)
                    for k in range(2):
                        at = h * HEAD_SIZE + k * half
                        g_qkv_ref[at : at + half, lanes] = g[k * LANES // 2 : k * LANES // 2 + half]

        load.wait()
        units = [(g, b) for g in range(2) for b in range(group // block)]
        scatter.to_mate()
        dh_load.wait()
        back(*units[0])
        scatter.pairs()
        swap.begin()
        out_gradient()
        back(*units[1])
        scatter.join()
        g_copies = [
            send(g_ref.at[own_place(device[0])], g_arrived.at[k], g_send.at[k], g_recv.at[k], device)
            for k, device in enumerate(peers)
        ]
        for unit in units[2:]:
            back(*unit)
        for copy in g_copies:
            copy.wait_recv()
        g_total = g_ref[own_place(o)].astype(F32)
        for k in range(n_outer - 1):
            g_total = g_total + g_arrived[k].astype(F32)
        for d in range(2 * n_ctx):
            g_sum[d] = g_total[d * place_rows : (d + 1) * place_rows].astype(BF)
        qkv_gradient()
        g_swap.begin()
        scatter.end()
        swap.end()

        def finish(r):
            result_ref[r] = (h_ref[r] + total[r]).astype(BF)

        row_chunks(own_rows, 32, finish)
        g_swap.end()
        for copy in g_copies:
            copy.wait_send()

    outs = [
        shape(qkv.shape, BF),
        shape((own_rows, width), BF),
        shape(swapped.shape, BF),
        shape((2 * n_ctx, place_rows, features), BF),
        shape((qkv.shape[1] // LANES * HEAD_SIZE, width), BF),
    ]
    ins = [dh_all, xn, qkv, attn, lse, cosine, sine, pos_rows, pos_columns, hidden, out_w, down_w, h1, swapped]
    scratch = [
        pltpu.VMEM(xn.shape, BF),
        pltpu.VMEM(qkv.shape, BF),
        pltpu.VMEM(attn.shape, BF),
        pltpu.VMEM(cosine.shape, F32),
        pltpu.VMEM(sine.shape, F32),
        pltpu.VMEM(pos_columns.shape, jnp.int32),
        pltpu.VMEM((width, features), BF),
        pltpu.VMEM((n_outer - 1, width // n_outer, features), BF),
        pltpu.VMEM((2 * n_ctx, place_rows, features), BF),
        pltpu.SemaphoreType.DMA((n_outer - 1,)),
        pltpu.SemaphoreType.DMA((n_outer - 1,)),
        pltpu.VMEM((group, LANES), F32),
        pltpu.VMEM((group, LANES), F32),
        pltpu.VMEM(down_w.shape, BF),
        pltpu.VMEM(out_w.shape, BF),
        pltpu.VMEM(dh_all.shape, BF),
        pltpu.SemaphoreType.DMA((1,)),
        pltpu.SemaphoreType.DMA((8,)),
    ]
    scratch += swap_sems(1, n_ctx) + swap_sems(1, n_ctx) + scatter_scratch(own_rows, width)
    return remote_call(kernel, number, ins, outs, scratch, any_ins=(0, 1, 2, 3, 5, 6, 8, 10, 11))


def attention_input(dproj, w, tokens, dh1, gain, gain_terms, n_outer, n_ctx, number):
    rows, width = tokens.shape
    tile = 256
    features = dproj.shape[1]
    n = 2 * n_ctx

    def kernel(
        d_ref, w_hbm, x_ref, dh_ref, gain_ref, terms_ref, out_ref, sum_ref, w_ref, load_sem, *scratch
    ):
        swap_sem, scratch = scratch[:3], scratch[3:]
        terms, summed, arrived, send_sem, recv_sem, local_sem = scratch[:6]
        scratch = scratch[6:]
        total = scratch[-1]
        load = Load(padded_loads(w_hbm, w_ref), load_sem).begin()
        o = lax.axis_index("o")

        def partial(slot, t):
            a = d_ref[pl.ds(pl.multiple_of(slot * rows, rows), rows)]
            return nn(a, w_ref[:, pl.ds(pl.multiple_of(t * tile, tile), tile)])

        scatter = Scatter(n_ctx, partial, tile, *scratch)
        swap = Swap(n_ctx, [(terms_ref, terms)], *swap_sem)
        peers = outer_peers(n_outer)
        greet(swap.devices + peers)
        swap.begin()
        load.wait()
        scatter.to_mate()
        scatter.pairs()
        swap.end()
        summed[...] = jnp.sum(terms[...], 0)
        scatter.join()
        copies = []
        for k, device in enumerate(peers):
            copies.append(send(summed.at[device[0]], arrived.at[o], send_sem.at[k], recv_sem.at[k], device))
        own = pltpu.make_async_copy(summed.at[o], arrived.at[o], local_sem)
        own.start()
        scatter.end()

        def finish(r):
            x, d = x_ref[r].astype(F32), total[r]
            out_ref[r] = dh_ref[r] + norm_back(d, gain_ref[0:1], x, inv_rms(x))

        row_chunks(rows, 32, finish)
        for copy in copies:
            copy.wait_recv()
        own.wait()
        sum_ref[...] = jnp.sum(arrived[...], 0)
        for copy in copies:
            copy.wait_send()

    outs = [shape((rows, width), F32), shape((8, LANES), F32)]
    ins = [dproj, w, tokens, dh1, gain, gain_terms]
    n_loads = features // (LANES // 2)
    scratch = [pltpu.VMEM((features, width), BF), pltpu.SemaphoreType.DMA((n_loads,))]
    scratch += swap_sems(1, n_ctx)
    scratch += [
        pltpu.VMEM((n, n_outer, 8, LANES), F32),
        pltpu.VMEM((n_outer, 8, LANES), F32),
        pltpu.VMEM((n_outer, 8, LANES), F32),
        pltpu.SemaphoreType.DMA((n_outer - 1,)),
        pltpu.SemaphoreType.DMA((n_outer - 1,)),
        pltpu.SemaphoreType.DMA,
    ]
    scratch += scatter_scratch(rows, width)
    return remote_call(kernel, number, ins, outs, scratch, any_ins=(1,))


def make_shards(n_outer, n_inner, n_ctx):
    n_plane = n_inner * n_ctx
    moves = feature_moves(n_outer, n_plane)
    back = [(b, a) for a, b in moves]

    def layer(tokens, norm_attn, w_qkv, w_out, norm_mlp, w_gate_up, w_down, cotangent, seq_lengths, block_slot):
        _, width = tokens.shape
        gain_rows = norm_attn.shape[0]
        out_rows = w_out.shape[0]
        unit_rows = w_gate_up.shape[0]
        n_seqs, n_slots = seq_lengths.shape[1], block_slot.shape[1]
        units = FF // n_plane
        qkv_w = z_ag(lax.ppermute(w_qkv, ALL, moves)).reshape(CHUNKS, -1, width)
        gain_part = jnp.pad(jnp.stack([norm_attn, norm_mlp]), ((0, 6), (0, LANES - gain_rows)))
        meta = jnp.concatenate([seq_lengths[0], block_slot[0]])
        meta = jnp.pad(meta[None], ((0, 7), (0, LANES - n_seqs - n_slots)))
        out_parts = pad_heads(w_out, 1).reshape(out_rows, 2, n_plane // 2, -1).transpose(2, 1, 0, 3)
        out_parts = out_parts.reshape(n_plane, out_rows, -1)
        down_parts = w_down.reshape(out_rows, n_outer // 2, n_plane, unit_rows).transpose(2, 0, 1, 3)
        down_parts = down_parts.reshape(n_plane, out_rows, units)
        w_gate_up, out_parts, down_parts = lax.optimization_barrier((w_gate_up, out_parts, down_parts))
        gate_up = z_ag(w_gate_up)
        gate_up = gate_up.reshape(CHUNKS, -1, width)
        x_all, out_parts, down_parts, gains, cosine, sine, pos_rows, pos_columns = prologue(
            tokens, out_parts, down_parts, gain_part, meta, n_seqs, n_outer, n_ctx, 1
        )
        x_all = x_all.reshape(-1, width)
        gains = gains[:, :, :2, :gain_rows].transpose(2, 0, 1, 3).reshape(2, width)
        qkv, attn, lse, dy_all, xn1, out_w = attention_forward(
            x_all, gains, qkv_w, cosine, sine, pos_rows, pos_columns, cotangent, out_parts, n_outer, n_ctx, 2
        )
        out_w = out_w.reshape(width, -1)
        h1, xn2, down_w = output_projection(attn, out_w, tokens, gains, down_parts, n_outer, n_ctx, 3)
        down_w = down_w.reshape(-1, units)
        xn2_all, hidden, dgu, dgu_t, g_down = feed_forward(xn2, dy_all, gate_up, down_w, n_ctx, 4)
        dgu, g_down = lax.optimization_barrier((dgu, g_down))
        g_down = z_rs(g_down)
        dh1, dh1_all, dgain_two, g_gate_up = feed_forward_input(
            dgu, gate_up, h1, cotangent, gains, xn2_all.reshape(-1, width), dgu_t, n_ctx, 5
        )
        g_gate_up = z_rs(g_gate_up)
        dh1_all = dh1_all.reshape(-1, width)
        dh1_all, g_down = lax.optimization_barrier((dh1_all, g_down))
        g_down = g_down.reshape(n_plane, out_rows, units)
        dproj, result, g_down, g_out, g_qkv = attention_backward(
            dh1_all, xn1, qkv, attn, lse, cosine, sine, pos_rows, pos_columns, hidden, out_w, down_w, h1, g_down, n_outer, n_ctx, 7
        )
        terms = jnp.sum(qkv_w.reshape(-1, width).astype(F32) * g_qkv.astype(F32), 0) / gains[0]
        terms = jnp.stack([terms, dgain_two[0]]).reshape(2, n_outer, n_plane, gain_rows).transpose(2, 1, 0, 3)
        terms = jnp.pad(terms, ((0, 0), (0, 0), (0, 6), (0, LANES - gain_rows)))
        dproj, g_qkv, g_gate_up = lax.optimization_barrier((dproj, g_qkv, g_gate_up))
        g_qkv = z_rs(g_qkv)
        grad_input, g = attention_input(dproj, qkv_w, tokens, dh1, gains, terms, n_outer, n_ctx, 8)
        grad_input, g_qkv = lax.optimization_barrier((grad_input, g_qkv))
        grad_qkv = lax.ppermute(g_qkv, ALL, back).astype(F32)
        g_out = g_out.reshape(n_plane // 2, 2, out_rows, -1).transpose(2, 1, 0, 3)
        grad_out = cut_heads(g_out.reshape(out_rows, -1), 1).astype(F32)
        grad_down = g_down.reshape(n_plane, out_rows, n_outer // 2, unit_rows).transpose(1, 2, 0, 3)
        grad_down = grad_down.reshape(out_rows, -1).astype(F32)
        g = g[:, :gain_rows]
        return (result, grad_input, g[0], grad_qkv, grad_out, g[1], g_gate_up.astype(F32), grad_down)

    return layer


def solution(mesh):
    n_inner = 2
    n_ctx = mesh.shape["ctx"]
    n_outer = mesh.shape["dp"] // n_inner
    split = Mesh(mesh.devices.reshape(n_outer, n_inner, n_ctx), ALL)
    rows, vec, grp = P(ALL, None), P(ALL), P(("o", "i"), None)
    return jax.shard_map(
        make_shards(n_outer, n_inner, n_ctx),
        mesh=split,
        in_specs=(rows, vec, rows, rows, vec, rows, rows, rows, grp, grp),
        out_specs=(rows, rows, vec, rows, rows, vec, rows, rows),
        check_vma=False,
    )
```

```python
import math

import jax
import jax.numpy as jnp
import numpy as np
from jax import lax
from jax.experimental import pallas as pl
from jax.experimental.pallas import tpu as pltpu
from jax.sharding import Mesh
from jax.sharding import PartitionSpec as P


QUERY_HEADS = 16
HEAD_SIZE = 96
FF = 4096
BLK = 128
LANES = 128
QUERY_BLOCK = 512
CHUNKS = 4

EPSILON = 1e-05
THETA = 100000.0
MASK_FILL = -1e30
BF = jnp.bfloat16
F32 = jnp.float32
ALL = ("o", "i", "ctx")
MESH = pl.DeviceIdType.MESH
SCALE = 1.0 / math.sqrt(HEAD_SIZE)


def nt(a, b):
    return lax.dot_general(a, b, (((1,), (1,)), ((), ())), preferred_element_type=F32)


def nn(a, b):
    return lax.dot_general(a, b, (((1,), (0,)), ((), ())), preferred_element_type=F32)


def tn(a, b):
    return lax.dot_general(a, b, (((0,), (0,)), ((), ())), preferred_element_type=F32)


def z_ag(x):
    return lax.all_gather(x, "o", axis=0, tiled=True)


def z_rs(x):
    return lax.psum_scatter(x, "o", scatter_dimension=0, tiled=True)


def inv_rms(x):
    return lax.rsqrt(jnp.mean(x * x, -1, keepdims=True) + EPSILON)


def norm_back(grad_normed, gain, source, scale):
    weighted = grad_normed * gain
    return scale * weighted - source * scale**3 * jnp.mean(weighted * source, -1, keepdims=True)


def feature_moves(n_outer, n_plane):
    moves = []
    half, quarter = n_outer // 2, n_outer // 4
    for block in range(n_outer * n_plane):
        if block < 4 * n_outer:
            head, step = block // half, block % half
        elif block < 6 * n_outer:
            head, step = divmod(block - 4 * n_outer, quarter)
            step += half
        else:
            head, step = divmod(block - 6 * n_outer, quarter)
            step += half + quarter
        place = 2 * (head % (n_plane // 2)) + head // (n_plane // 2)
        moves.append((block, step * n_plane + place))
    return moves


def pad_heads(x, axis):
    half = HEAD_SIZE // 2
    shape = x.shape
    x = x.reshape(shape[:axis] + (-1, half) + shape[axis + 1 :])
    pads = [(0, 0)] * x.ndim
    pads[axis + 1] = (0, LANES // 2 - half)
    return jnp.pad(x, pads).reshape(shape[:axis] + (-1,) + shape[axis + 1 :])


def cut_heads(x, axis):
    half = HEAD_SIZE // 2
    shape = x.shape
    x = x.reshape(shape[:axis] + (-1, LANES // 2) + shape[axis + 1 :])
    x = lax.slice_in_dim(x, 0, half, axis=axis + 1)
    return x.reshape(shape[:axis] + (-1,) + shape[axis + 1 :])


def places(n_ctx):
    o, i, c = lax.axis_index("o"), lax.axis_index("i"), lax.axis_index("ctx")
    return o, i, c, c + 1 - 2 * (c % 2), (c + n_ctx // 2) % n_ctx


def greet(devices):
    barrier = pltpu.get_barrier_semaphore()
    for device in devices:
        pl.semaphore_signal(barrier, inc=1, device_id=device, device_id_type=MESH)
    pl.semaphore_wait(barrier, len(devices))


def greet_neighbours(n_ctx):
    o, i, c, mate, far = places(n_ctx)
    greet([(o, i, mate), (o, 1 - i, c), (o, i, far)])


def send(src, dst, send_sem, recv_sem, device):
    copy = pltpu.make_async_remote_copy(
        src_ref=src, dst_ref=dst, send_sem=send_sem, recv_sem=recv_sem, device_id=device, device_id_type=MESH
    )
    copy.start()
    return copy


class Gather:
    def __init__(self, n_ctx, src, out, send_sem, recv_sem, local_sem):
        self.src, self.out, self.sems = src, out, (send_sem, recv_sem, local_sem)
        o, i, c, mate, far = places(n_ctx)
        j, core = 1 - i, c % 2
        self.mate, self.x, self.y = (o, i, mate), (o, j, c), (o, i, far)
        self.me, self.s_x = i * n_ctx + c, j * n_ctx + c
        self.s_y, self.s_d = i * n_ctx + far, j * n_ctx + far
        self.relay = (o, j * core + i * (1 - core), c * core + far * (1 - core))
        self.relayed = self.s_y * core + self.s_x * (1 - core)
        mate_far = (mate + n_ctx // 2) % n_ctx
        self.mates_slots = [i * n_ctx + mate, j * n_ctx + mate, i * n_ctx + mate_far, j * n_ctx + mate_far]
        self.copies = {}

    def go(self, kind, part, src, slot, device):
        rows = src.shape[0] // PARTS
        at = pl.ds(part * rows, rows)
        copy = send(src.at[at], self.out.at[slot, at], self.sems[0].at[kind, part], self.sems[1].at[kind, part], device)
        self.copies[kind, part] = copy

    def begin(self):
        for part in range(PARTS):
            self.go(1, part, self.src, self.me, self.x)
            self.go(2, part, self.src, self.me, self.y)
        for part in range(PARTS):
            self.go(0, part, self.src, self.me, self.mate)
        self.own = pltpu.make_async_copy(self.src, self.out.at[self.me], self.sems[2])
        self.own.start()

    def middle(self):
        for part in range(PARTS):
            self.copies[1, part].wait_recv()
            self.copies[2, part].wait_recv()
            self.go(5, part, self.out.at[self.relayed], self.relayed, self.relay)
            self.go(3, part, self.out.at[self.s_x], self.s_x, self.mate)
            self.go(4, part, self.out.at[self.s_y], self.s_y, self.mate)

    def corner(self):
        for part in range(PARTS):
            self.copies[5, part].wait_recv()
            self.go(6, part, self.out.at[self.s_d], self.s_d, self.mate)

    def arrived(self, kind):
        for part in range(PARTS):
            self.copies[kind, part].wait_recv()

    def sent(self):
        self.own.wait()
        for copy in self.copies.values():
            copy.wait_send()

    def end(self):
        self.corner()
        for kind in (0, 3, 4, 6):
            self.arrived(kind)
        self.sent()


PARTS = 2
GATHER_SEMS = [pltpu.SemaphoreType.DMA((7, PARTS)), pltpu.SemaphoreType.DMA((7, PARTS)), pltpu.SemaphoreType.DMA]


class Scatter:
    def __init__(self, n_ctx, partial, tile, ready, from_mate, going, got, send_sem, recv_sem, total):
        self.partial, self.tile = partial, tile
        self.ready, self.from_mate, self.going, self.got = ready, from_mate, going, got
        self.sems, self.total = (send_sem, recv_sem), total
        o, i, c, mate, far = places(n_ctx)
        j, core = 1 - i, c % 2
        self.core = core
        far_mate = (mate + n_ctx // 2) % n_ctx
        self.mine = [j * n_ctx + far, j * n_ctx + c, i * n_ctx + far, i * n_ctx + c]
        self.theirs = [j * n_ctx + far_mate, j * n_ctx + mate, i * n_ctx + far_mate, i * n_ctx + mate]
        self.mate = (o, i, mate)
        self.combined = (o, j * (1 - core) + i * core, c * (1 - core) + far * core)
        self.direct = (o, j * core + i * (1 - core), c * core + far * (1 - core))
        self.s_direct = self.mine[2] * (1 - core) + self.mine[1] * core
        self.s_combined = self.mine[1] * (1 - core) + self.mine[2] * core
        self.copies = []

    def go(self, kind, part, src, dst, device):
        copy = send(src.at[part], dst.at[part], self.sems[0].at[kind, part], self.sems[1].at[kind, part], device)
        self.copies.append(copy)
        return copy

    def each(self, part, body):
        tiles = self.ready.shape[-1] // self.tile

        @pl.loop(0, tiles)
        def _(t):
            at = pl.multiple_of(t * self.tile, self.tile)
            body(part * tiles + t, pl.ds(at, self.tile), pl.ds(part * tiles * self.tile + at, self.tile))

    def fill(self, n, part):
        def body(t, lanes, _):
            self.ready[n, part, :, lanes] = self.partial(self.theirs[n], t).astype(BF)

        self.each(part, body)

    def give(self, n, part):
        self.mates[n, part] = self.go(n, part, self.ready.at[n], self.from_mate.at[n], self.mate)

    def pair(self, slot, n, part, place):
        def body(t, lanes, _):
            pair = self.partial(slot, t) + self.from_mate[n, part, :, lanes].astype(F32)
            self.going[place, part, :, lanes] = pair.astype(BF)

        self.each(part, body)

    def to_mate(self):
        self.mates, self.straights, self.diagonals, self.joins = {}, [], [], []
        order = [(0, 0), (0, 1), (1, 0), (2, 0), (1, 1), (2, 1), (3, 0), (3, 1)]
        self.fill(*order[0])
        for k, at in enumerate(order[1:]):
            self.fill(*at)
            self.give(*order[k])
            if k == 2:
                self.mates[0, 0].wait_recv()
                self.pair(self.mine[0], 0, 0, 0)
            if k == 3:
                self.diagonals.append(self.go(4, 0, self.going.at[0], self.got.at[0], self.direct))
                self.mates[0, 1].wait_recv()
                self.pair(self.mine[0], 0, 1, 0)
            if k == 4:
                self.diagonals.append(self.go(4, 1, self.going.at[0], self.got.at[0], self.direct))
        self.last = order[-1]

    def pairs(self):
        for part in range(PARTS):
            self.mates[1, part].wait_recv()
            self.mates[2, part].wait_recv()
            self.pair(self.s_direct, 2 - self.core, part, 1)
            if part == 0:
                self.give(*self.last)
            else:
                self.straights.append(self.go(5, part - 1, self.going.at[1], self.got.at[1], self.direct))

    def join(self):
        for part in range(PARTS):
            self.diagonals[part].wait_recv()
            if part == 0:
                self.straights.append(self.go(5, PARTS - 1, self.going.at[1], self.got.at[1], self.direct))

            def combined(t, lanes, _):
                pair = self.partial(self.s_combined, t) + self.from_mate[1 + self.core, part, :, lanes].astype(F32)
                self.going[2, part, :, lanes] = (pair + self.got[0, part, :, lanes].astype(F32)).astype(BF)

            self.each(part, combined)
            if part:
                self.joins.append(self.go(6, part - 1, self.going.at[2], self.got.at[2], self.combined))
        self.own(0)
        self.joins.append(self.go(6, PARTS - 1, self.going.at[2], self.got.at[2], self.combined))

    def own(self, part):
        self.mates[3, part].wait_recv()

        def body(t, lanes, out):
            self.total[:, out] = self.partial(self.mine[3], t) + self.from_mate[3, part, :, lanes].astype(F32)

        self.each(part, body)

    def end(self):
        total = self.total
        for part in range(1, PARTS):
            self.own(part)
        for part in range(PARTS):
            self.straights[part].wait_recv()
            self.joins[part].wait_recv()

            def rest(t, lanes, out):
                other = self.got[1, part, :, lanes].astype(F32) + self.got[2, part, :, lanes].astype(F32)
                total[:, out] = total[:, out] + other

            self.each(part, rest)
        for copy in self.copies:
            copy.wait_send()


def scatter_scratch(rows, width):
    return [
        pltpu.VMEM((4, PARTS, rows, width // PARTS), BF),
        pltpu.VMEM((4, PARTS, rows, width // PARTS), BF),
        pltpu.VMEM((3, PARTS, rows, width // PARTS), BF),
        pltpu.VMEM((3, PARTS, rows, width // PARTS), BF),
        pltpu.SemaphoreType.DMA((7, PARTS)),
        pltpu.SemaphoreType.DMA((7, PARTS)),
        pltpu.VMEM((rows, width), F32),
    ]


def row_chunks(rows, step, body):
    @pl.loop(0, rows // step)
    def _(r):
        body(pl.ds(pl.multiple_of(r * step, step), step))


class Load:
    def __init__(self, parts, sem):
        self.copies = [pltpu.make_async_copy(src, dst, sem.at[n]) for n, (src, dst) in enumerate(parts)]

    def begin(self):
        for copy in self.copies:
            copy.start()
        return self

    def wait(self):
        for copy in self.copies:
            copy.wait()


IN_VMEM = pl.BlockSpec(memory_space=pltpu.VMEM)
ANYWHERE = pl.BlockSpec(memory_space=pl.ANY)


def remote_call(kernel, number, ins, outs, scratch, any_outs=(), any_ins=()):
    return pl.pallas_call(
        kernel,
        out_shape=outs,
        in_specs=[ANYWHERE if n in any_ins else IN_VMEM for n in range(len(ins))],
        out_specs=[ANYWHERE if n in any_outs else IN_VMEM for n in range(len(outs))],
        scratch_shapes=scratch,
        compiler_params=pltpu.CompilerParams(collective_id=number, has_side_effects=True, vmem_limit_bytes=60 << 20),
    )(*ins)


def shape(dims, dtype):
    return jax.ShapeDtypeStruct(tuple(dims), dtype)


class Swap:
    def __init__(self, n_ctx, pairs, send_sem, recv_sem, local_sem):
        self.pairs, self.sems = pairs, (send_sem, recv_sem, local_sem)
        self.o, i, c, _, _ = places(n_ctx)
        self.n, self.n_ctx = 2 * n_ctx, n_ctx
        self.me = i * n_ctx + c
        self.others = [(self.me + k) % self.n for k in range(1, self.n)]
        self.devices = [(self.o, d // n_ctx, d % n_ctx) for d in self.others]

    def begin(self):
        self.copies, self.own = [], []
        for a, (src, dst) in enumerate(self.pairs):
            for k, (d, device) in enumerate(zip(self.others, self.devices)):
                self.copies.append(
                    send(src.at[d], dst.at[self.me], self.sems[0].at[a, k], self.sems[1].at[a, k], device)
                )
            own = pltpu.make_async_copy(src.at[self.me], dst.at[self.me], self.sems[2].at[a])
            own.start()
            self.own.append(own)

    def end(self):
        for copy in self.copies:
            copy.wait_recv()
            copy.wait_send()
        for copy in self.own:
            copy.wait()


def swap_sems(n_arrays, n_ctx):
    return [
        pltpu.SemaphoreType.DMA((n_arrays, 2 * n_ctx - 1)),
        pltpu.SemaphoreType.DMA((n_arrays, 2 * n_ctx - 1)),
        pltpu.SemaphoreType.DMA((n_arrays,)),
    ]


def outer_peers(n_outer):
    o, i, c = lax.axis_index("o"), lax.axis_index("i"), lax.axis_index("ctx")
    return [(lax.rem(o + k, n_outer), i, c) for k in range(1, n_outer)]


def rotary_constants():
    frequency = THETA ** -(np.arange(HEAD_SIZE // 2) * (2.0 / HEAD_SIZE))
    rates = np.zeros((8, LANES), np.float32)
    for half, sign in ((0, -1.0), (LANES // 2, 1.0)):
        rates[0, half : half + HEAD_SIZE // 2] = frequency
        rates[1, half : half + HEAD_SIZE // 2] = sign
    angles = np.arange(BLK)[:, None] * rates[0].astype(np.float64)
    return rates, np.stack([np.cos(angles), np.sin(angles)]).astype(np.float32)


def prologue(tokens, out_parts, down_parts, gains, meta, n_seqs, n_outer, n_ctx, number):
    rows, width = tokens.shape
    n = 2 * n_ctx
    blocks = n_ctx * rows // BLK

    def kernel(
        x_ref,
        out_src,
        down_src,
        gains_ref,
        meta_ref,
        rates_ref,
        angles_ref,
        x_all,
        out_dst,
        down_dst,
        gains_out,
        cos_ref,
        sin_ref,
        rows_ref,
        columns_ref,
        *sems,
    ):
        o = lax.axis_index("o")
        metas_ref, send_sem, recv_sem, local_sem = sems[:4]
        out_swap = Swap(n_ctx, [(out_src, out_dst)], *sems[4:7])
        down_swap = Swap(n_ctx, [(down_src, down_dst)], *sems[7:10])
        gather = Gather(n_ctx, x_ref, x_all, *sems[10:])
        peers = outer_peers(n_outer)
        me = out_swap.me
        greet(out_swap.devices + peers)
        gather.begin()
        own = [
            pltpu.make_async_copy(meta_ref, metas_ref.at[me], local_sem.at[0]),
            pltpu.make_async_copy(gains_ref, gains_out.at[o, me], local_sem.at[1]),
        ]
        meta_copies, gain_copies, z_copies = [], [], []
        for copy in own:
            copy.start()
        for k, device in enumerate(out_swap.devices):
            meta_copies.append(send(meta_ref, metas_ref.at[me], send_sem.at[0, k], recv_sem.at[0, k], device))
            gain_copies.append(send(gains_ref, gains_out.at[o, me], send_sem.at[1, k], recv_sem.at[1, k], device))
        out_swap.begin()
        for copy in own:
            copy.wait()
        for copy in meta_copies:
            copy.wait_recv()
        lane = lax.broadcasted_iota(jnp.int32, (BLK, LANES), 1)
        row = lax.broadcasted_iota(jnp.int32, (BLK, LANES), 0)
        rows_ref[...] = jnp.zeros_like(rows_ref)
        pieces = 2 * blocks * n_seqs
        piece = lax.broadcasted_iota(jnp.int32, (pieces, LANES), 0)
        bases = jnp.zeros((pieces, LANES), jnp.int32)
        places_of = []
        for g in range(2):
            starts, end = [], jnp.zeros((1, 1), jnp.int32)
            for q in range(n_seqs):
                starts.append(end)
                end = end + metas_ref[g * n_ctx, 0:1, q : q + 1]
            for b in range(blocks):
                first = metas_ref[g * n_ctx, 0:1, n_seqs + b : n_seqs + b + 1] * BLK
                for q in range(n_seqs):
                    index = (g * blocks + b) * n_seqs + q
                    bases = jnp.where(piece == index, first - starts[q], bases)
                places_of.append((first, starts))
        angle = bases.astype(F32) * rates_ref[0:1]
        base_cos, base_sin = jnp.cos(angle), jnp.sin(angle)
        for n_block, (first, starts) in enumerate(places_of):
            at = slice(n_block * BLK, (n_block + 1) * BLK)
            stream, lanes_stream = first + row, first + lane[0:1]
            start, lanes_start = jnp.zeros_like(stream), jnp.zeros_like(lanes_stream)
            cos, sin = angles_ref[0], angles_ref[1]
            for q in range(n_seqs):
                index = n_block * n_seqs + q
                cos_0, sin_0 = base_cos[index : index + 1], base_sin[index : index + 1]
                cos_q = cos_0 * angles_ref[0] - sin_0 * angles_ref[1]
                sin_q = sin_0 * angles_ref[0] + cos_0 * angles_ref[1]
                inside = stream >= starts[q]
                start = jnp.where(inside, starts[q], start)
                lanes_start = jnp.where(lanes_stream >= starts[q], starts[q], lanes_start)
                cos, sin = jnp.where(inside, cos_q, cos), jnp.where(inside, sin_q, sin)
            cos_ref[at] = cos
            sin_ref[at] = sin * rates_ref[1:2]
            columns_ref[at] = jnp.where(lane == 0, stream, start)
            rows_ref[0:1, at] = lanes_stream
            rows_ref[1:2, at] = lanes_start
        for copy in gain_copies:
            copy.wait_recv()
        for k, device in enumerate(peers):
            z_copies.append(send(gains_out.at[o], gains_out.at[o], send_sem.at[2, k], recv_sem.at[2, k], device))
        gather.middle()
        down_swap.begin()
        gather.end()
        out_swap.end()
        down_swap.end()
        for copy in z_copies:
            copy.wait_recv()
        for copy in meta_copies + gain_copies + z_copies:
            copy.wait_send()

    outs = [
        shape((n, rows, width), BF),
        shape(out_parts.shape, BF),
        shape(down_parts.shape, BF),
        shape((n_outer, n) + gains.shape, F32),
        shape((n * rows, LANES), F32),
        shape((n * rows, LANES), F32),
        shape((8, n * rows), jnp.int32),
        shape((n * rows, LANES), jnp.int32),
    ]
    rates, angles = rotary_constants()
    ins = [tokens, out_parts, down_parts, gains, meta, jnp.asarray(rates), jnp.asarray(angles)]
    most = max(n, n_outer) - 1
    scratch = [
        pltpu.VMEM((n,) + meta.shape, jnp.int32),
        pltpu.SemaphoreType.DMA((3, most)),
        pltpu.SemaphoreType.DMA((3, most)),
        pltpu.SemaphoreType.DMA((2,)),
    ]
    scratch += swap_sems(1, n_ctx) + swap_sems(1, n_ctx) + GATHER_SEMS
    return remote_call(kernel, number, ins, outs, scratch, any_outs=(0,))


def plane_gather(x, n_ctx, number):
    def kernel(src, out, *sems):
        gather = Gather(n_ctx, src, out, *sems)
        greet_neighbours(n_ctx)
        gather.begin()
        gather.middle()
        gather.end()

    outs = [shape((2 * n_ctx,) + x.shape, x.dtype)]
    got = remote_call(kernel, number, [x], outs, GATHER_SEMS, any_outs=(0,))
    return got[0].reshape(-1, x.shape[-1])


def rotate(x, cosine, sine):
    return x * cosine + pltpu.roll(x, LANES // 2, 1) * sine


def qkv_rows(features):
    return features // LANES * HEAD_SIZE // CHUNKS


def padded_loads(w_ref, w_pad):
    half = HEAD_SIZE // 2
    rows = qkv_rows(w_pad.shape[0])
    pairs, at = [], 0
    for row in range(half, w_pad.shape[0], LANES // 2):
        w_pad[row : row + LANES // 2 - half] = jnp.zeros((LANES // 2 - half, w_pad.shape[1]), BF)
    for n in range(w_ref.shape[0]):
        for b in range(rows // half):
            src = w_ref.at[n, pl.ds(b * half, half)]
            pairs.append((src, w_pad.at[pl.ds(at * LANES // 2, half)]))
            at += 1
    return pairs


def attention_forward(x_all, gains, w, cosine, sine, pos_rows, pos_columns, dy, out_part, n_outer, n_ctx, number):
    rows, width = x_all.shape
    group = rows // 2
    heads = QUERY_HEADS // (2 * n_ctx)
    features = (heads + 2) * LANES
    k_at, v_at = heads * LANES, (heads + 1) * LANES
    block = min(QUERY_BLOCK, group)
    n_loads = features // (LANES // 2)

    def kernel(
        x_hbm,
        gain_ref,
        w_hbm,
        cos_ref,
        sin_ref,
        rows_ref,
        columns_ref,
        dy_ref,
        part_ref,
        qkv_ref,
        attn_ref,
        lse_ref,
        dy_all,
        xn_out,
        out_w,
        w_ref,
        xn_ref,
        load_sem,
        xn_sem,
        store_sem,
        z_send,
        z_recv,
        z_local,
        *sems,
    ):
        gather = Gather(n_ctx, dy_ref, dy_all, *sems)
        load = Load(padded_loads(w_hbm, w_ref), load_sem).begin()
        xn_load = Load([(x_hbm, xn_ref)], xn_sem).begin()
        o = lax.axis_index("o")
        peers = outer_peers(n_outer)
        greet([gather.mate, gather.x, gather.y] + peers)
        gather.begin()
        z_copies = [send(part_ref, out_w.at[o], z_send.at[k], z_recv.at[k], device) for k, device in enumerate(peers)]
        own_part = pltpu.make_async_copy(part_ref, out_w.at[o], z_local)
        own_part.start()
        load.wait()
        xn_load.wait()

        def normalise(r):
            x = xn_ref[r].astype(F32)
            xn_ref[r] = (x * inv_rms(x) * gain_ref[0:1]).astype(BF)

        def project(r):
            cos, sin = cos_ref[r], sin_ref[r]
            for h in range(heads + 2):
                lanes = slice(h * LANES, (h + 1) * LANES)
                part = nt(xn_ref[r], w_ref[lanes])
                qkv_ref[r, lanes] = (rotate(part, cos, sin) if h <= heads else part).astype(BF)

        def attend(g):
            keys_at = pl.ds(g * group, group)

            @pl.loop(0, group // block)
            def _(b):
                r = pl.ds(pl.multiple_of(g * group + b * block, block), block)
                key_pos = rows_ref[0:1, keys_at]
                ok = (key_pos >= columns_ref[r, 1:2]) & (key_pos <= columns_ref[r, 0:1])
                for h in range(heads):
                    lanes = slice(h * LANES, (h + 1) * LANES)
                    s = nt(qkv_ref[r, lanes], qkv_ref[keys_at, k_at : k_at + LANES])
                    s = jnp.where(ok, s, MASK_FILL)
                    high = jnp.max(s, -1, keepdims=True)
                    e = jnp.exp((s - high) * SCALE)
                    total = jnp.sum(e, -1, keepdims=True)
                    mixed = nn(e.astype(BF), qkv_ref[keys_at, v_at : v_at + LANES])
                    attn_ref[r, lanes] = (mixed / total).astype(BF)
                    lse = jnp.broadcast_to(high * SCALE + jnp.log(total), (block, LANES))
                    lse_ref[h : h + 1, r] = jnp.transpose(lse)[0:1]

        row_chunks(rows, 64, normalise)
        row_chunks(rows, block, project)
        gather.middle()
        store = Load([(xn_ref, xn_out)], store_sem).begin()
        attend(0)
        attend(1)
        gather.end()
        store.wait()
        own_part.wait()
        for copy in z_copies:
            copy.wait_recv()
            copy.wait_send()

    outs = [
        shape((rows, features), BF),
        shape((rows, heads * LANES), BF),
        shape((8, rows), F32),
        shape((2 * n_ctx,) + dy.shape, BF),
        shape(x_all.shape, BF),
        shape((n_outer,) + out_part.shape, BF),
    ]
    ins = [x_all, gains, w, cosine, sine, pos_rows, pos_columns, dy, out_part]
    scratch = [
        pltpu.VMEM((features, width), BF),
        pltpu.VMEM(x_all.shape, BF),
        pltpu.SemaphoreType.DMA((n_loads,)),
        pltpu.SemaphoreType.DMA((1,)),
        pltpu.SemaphoreType.DMA((1,)),
        pltpu.SemaphoreType.DMA((n_outer - 1,)),
        pltpu.SemaphoreType.DMA((n_outer - 1,)),
        pltpu.SemaphoreType.DMA,
    ]
    scratch += GATHER_SEMS
    got = remote_call(kernel, number, ins, outs, scratch, any_outs=(3, 4), any_ins=(0, 2))
    return got[0], got[1], got[2], got[3].reshape(rows, width), got[4], got[5]


def output_projection(attn, out_w, tokens, gain, down_part, n_outer, n_ctx, number):
    rows, width = tokens.shape
    tile = 256


    def kernel(attn_ref, w_ref, x_ref, gain_ref, part_ref, h_ref, xn_ref, down_w, z_send, z_recv, z_local, *scratch):
        total = scratch[-1]

        def partial(slot, t):
            a = attn_ref[pl.ds(pl.multiple_of(slot * rows, rows), rows)]
            return nt(a, w_ref[pl.ds(pl.multiple_of(t * tile, tile), tile)])

        scatter = Scatter(n_ctx, partial, tile, *scratch)
        o, i, c, mate, far = places(n_ctx)
        peers = outer_peers(n_outer)
        greet([(o, i, mate), (o, 1 - i, c), (o, i, far)] + peers)
        z_copies = [send(part_ref, down_w.at[o], z_send.at[k], z_recv.at[k], device) for k, device in enumerate(peers)]
        own_part = pltpu.make_async_copy(part_ref, down_w.at[o], z_local)
        own_part.start()
        scatter.to_mate()
        scatter.pairs()
        scatter.join()
        scatter.end()

        def finish(r):
            h = x_ref[r].astype(F32) + total[r]
            h_ref[r] = h
            xn_ref[r] = (h * inv_rms(h) * gain_ref[1:2]).astype(BF)

        row_chunks(rows, 32, finish)
        own_part.wait()
        for copy in z_copies:
            copy.wait_recv()
            copy.wait_send()

    outs = [shape((rows, width), F32), shape((rows, width), BF), shape((n_outer,) + down_part.shape, BF)]
    sems = [
        pltpu.SemaphoreType.DMA((n_outer - 1,)),
        pltpu.SemaphoreType.DMA((n_outer - 1,)),
        pltpu.SemaphoreType.DMA,
    ]
    ins = [attn, out_w, tokens, gain, down_part]
    return remote_call(kernel, number, ins, outs, sems + scatter_scratch(rows, width), any_outs=(2,))


def feed_forward(xn, dy, gate_up, down, n_ctx, number):
    rows, width = xn.shape
    n = 2 * n_ctx
    chunks, unit_rows, _ = gate_up.shape
    units = down.shape[1]
    tile = 256

    def kernel(
        x_ref,
        dy_hbm,
        up_hbm,
        down_hbm,
        xn_all,
        hidden_ref,
        dgu_ref,
        dgu_t,
        g_down_ref,
        raw,
        dy_ref,
        up_ref,
        down_ref,
        hidden_t,
        g_acc,
        load_sem,
        store_sem,
        *sems,
    ):
        gather = Gather(n_ctx, x_ref, raw, *sems)
        pairs = [(up_hbm, up_ref), (down_hbm, down_ref), (dy_hbm, dy_ref)]
        load = Load(pairs, load_sem).begin()
        greet_neighbours(n_ctx)
        gather.begin()
        half = chunks // 2
        core = gather.me % 2

        def chip(slot):
            both = pl.ds(pl.multiple_of((slot - core) * rows, 2 * rows), 2 * rows)
            x = raw[pl.ds(slot - core, 2)].reshape(2 * rows, width)
            for m in range(half):
                lanes = slice(m * unit_rows, (m + 1) * unit_rows)
                second = slice(units + m * unit_rows, units + (m + 1) * unit_rows)
                gate = nt(x, up_ref[m])
                up = nt(x, up_ref[half + m])
                dhid = nn(dy_ref[both], down_ref[:, lanes])
                sg = 1.0 / (1.0 + jnp.exp(-gate))
                act = gate * sg
                hidden = act * up
                dgate = dhid * up * sg * (1.0 + gate * (1.0 - sg))
                dup = dhid * act
                hidden_ref[both, lanes] = hidden.astype(BF)
                dgu_ref[both, lanes] = dgate.astype(BF)
                dgu_ref[both, second] = dup.astype(BF)
                hidden_t[lanes] = jnp.transpose(hidden).astype(BF)
                dgu_t[lanes, both] = jnp.transpose(dgate).astype(BF)
                dgu_t[second, both] = jnp.transpose(dup).astype(BF)

            @pl.loop(0, width // tile)
            def _(t):
                lanes = pl.ds(pl.multiple_of(t * tile, tile), tile)
                g = nn(hidden_t[...], dy_ref[both, lanes])
                g_acc[:, lanes] = g if slot is gather.me else g_acc[:, lanes] + g

        stores = []

        def store(slot):
            copy = pltpu.make_async_copy(raw.at[slot], xn_all.at[slot], store_sem.at[len(stores)])
            copy.start()
            stores.append(copy)

        load.wait()
        gather.arrived(0)
        gather.own.wait()
        store(gather.me)
        store(gather.mates_slots[0])
        chip(gather.me)
        gather.middle()
        gather.arrived(3)
        store(gather.s_x)
        store(gather.mates_slots[1])
        chip(gather.s_x)
        gather.arrived(4)
        store(gather.s_y)
        store(gather.mates_slots[2])
        chip(gather.s_y)
        gather.corner()
        gather.arrived(6)
        store(gather.s_d)
        store(gather.mates_slots[3])
        chip(gather.s_d)

        @pl.loop(0, width // tile)
        def _(t):
            lanes = pl.ds(pl.multiple_of(t * tile, tile), tile)
            g_down_ref[lanes] = jnp.transpose(g_acc[:, lanes]).astype(BF)

        for copy in gather.copies.values():
            copy.wait_send()
        for copy in stores:
            copy.wait()

    outs = [
        shape((n, rows, width), BF),
        shape((n * rows, units), BF),
        shape((n * rows, 2 * units), BF),
        shape((2 * units, n * rows), BF),
        shape((width, units), BF),
    ]
    scratch = [
        pltpu.VMEM((n, rows, width), BF),
        pltpu.VMEM(dy.shape, BF),
        pltpu.VMEM(gate_up.shape, BF),
        pltpu.VMEM(down.shape, BF),
        pltpu.VMEM((units, 2 * rows), BF),
        pltpu.VMEM((units, width), F32),
        pltpu.SemaphoreType.DMA((3,)),
        pltpu.SemaphoreType.DMA((n,)),
    ]
    ins = [xn, dy, gate_up, down]
    return remote_call(kernel, number, ins, outs, scratch + GATHER_SEMS, any_outs=(0,), any_ins=(1, 2, 3))


def feed_forward_input(dgu, gate_up, h1, cotangent, gain, xn_all, dgu_t, n_ctx, number):
    rows, width = h1.shape
    chunks, unit_rows, _ = gate_up.shape
    units = chunks * unit_rows // 2
    tile, part = 256, 256

    def kernel(
        dgu_ref,
        w_hbm,
        h_ref,
        dy_ref,
        gain_ref,
        xn_hbm,
        dgu_t_hbm,
        dh_ref,
        dhb_ref,
        dgain_ref,
        g_up_ref,
        w_ref,
        xn_ref,
        dgu_t_ref,
        w_sem,
        load_sem,
        *scratch,
    ):
        total = scratch[-1]
        w_load = Load([(w_hbm, w_ref)], w_sem).begin()
        load = Load([(dgu_t_hbm, dgu_t_ref), (xn_hbm, xn_ref)], load_sem).begin()

        def partial(slot, t):
            r = pl.ds(pl.multiple_of(slot * rows, rows), rows)
            lanes = pl.ds(pl.multiple_of(t * tile, tile), tile)
            acc = nn(dgu_ref[r, :unit_rows], w_ref[0, :, lanes])
            for n in range(1, chunks):
                acc = acc + nn(dgu_ref[r, n * unit_rows : (n + 1) * unit_rows], w_ref[n, :, lanes])
            return acc

        def up_gradient(first, last):
            @pl.loop(first, last)
            def _(k):
                r = pl.ds(pl.multiple_of(k * part, part), part)

                @pl.loop(0, width // tile)
                def _(t):
                    lanes = pl.ds(pl.multiple_of(t * tile, tile), tile)
                    g_up_ref[r, lanes] = nn(dgu_t_ref[r], xn_ref[:, lanes]).astype(BF)

        scatter = Scatter(n_ctx, partial, tile, *scratch)
        greet_neighbours(n_ctx)
        w_load.wait()
        scatter.to_mate()
        scatter.pairs()
        load.wait()
        up_gradient(0, units // part)
        scatter.join()
        up_gradient(units // part, 2 * units // part)
        scatter.end()
        dgain_ref[...] = jnp.zeros_like(dgain_ref)

        def finish(r):
            h, d = h_ref[r], total[r]
            scale = inv_rms(h)
            dgain_ref[0:1] += jnp.sum(d * h * scale, 0, keepdims=True)
            dh = dy_ref[r].astype(F32) + norm_back(d, gain_ref[1:2], h, scale)
            dh_ref[r] = dh
            dhb_ref[r] = dh.astype(BF)

        row_chunks(rows, 32, finish)

    outs = [
        shape((rows, width), F32),
        shape((rows, width), BF),
        shape((8, width), F32),
        shape((2 * units, width), BF),
    ]
    scratch = [
        pltpu.VMEM((chunks, unit_rows, width), BF),
        pltpu.VMEM(xn_all.shape, BF),
        pltpu.VMEM(dgu_t.shape, BF),
        pltpu.SemaphoreType.DMA((1,)),
        pltpu.SemaphoreType.DMA((2,)),
    ]
    return remote_call(
        kernel,
        number,
        [dgu, gate_up, h1, cotangent, gain, xn_all, dgu_t],
        outs,
        scratch + scatter_scratch(rows, width),
        any_ins=(1, 5, 6),
    )


def attention_backward(
    dh_all, xn, qkv, attn, lse, cosine, sine, pos_rows, pos_columns, hidden, out_w, down_w, h1, swapped, n_outer, n_ctx, number
):
    rows = dh_all.shape[0]
    own_rows, width = h1.shape
    group = rows // 2
    heads = attn.shape[1] // LANES
    k_at, v_at = heads * LANES, (heads + 1) * LANES
    block = min(QUERY_BLOCK, group)
    features = attn.shape[1]
    tile = 256
    place_rows = width // n_outer // (2 * n_ctx)

    def kernel(
        dh_hbm,
        xn_hbm,
        qkv_hbm,
        attn_hbm,
        lse_ref,
        cos_hbm,
        sin_hbm,
        rows_ref,
        columns_hbm,
        hidden_ref,
        out_w_hbm,
        w_hbm,
        h_ref,
        swap_src,
        dproj_ref,
        result_ref,
        swap_dst,
        g_dst,
        g_qkv_ref,
        xn_ref,
        qkv_ref,
        attn_ref,
        cos_ref,
        sin_ref,
        columns_ref,
        g_ref,
        g_arrived,
        g_sum,
        g_send,
        g_recv,
        dk_ref,
        dv_ref,
        w_ref,
        out_w_ref,
        dh_ref,
        load_sem,
        dh_sem,
        *scratch,
    ):
        swap_sem, g_swap_sem, scratch = scratch[:3], scratch[3:6], scratch[6:]
        total = scratch[-1]
        o = lax.axis_index("o")
        peers = outer_peers(n_outer)
        load = Load([(w_hbm, w_ref)], load_sem).begin()
        pairs = [(out_w_hbm, out_w_ref), (dh_hbm, dh_ref), (attn_hbm, attn_ref), (qkv_hbm, qkv_ref), (cos_hbm, cos_ref), (sin_hbm, sin_ref)]
        dh_load = Load(pairs + [(columns_hbm, columns_ref), (xn_hbm, xn_ref)], dh_sem).begin()
        swap = Swap(n_ctx, [(swap_src, swap_dst)], *swap_sem)
        g_swap = Swap(n_ctx, [(g_sum, g_dst)], *g_swap_sem)

        def partial(slot, t):
            a = hidden_ref[pl.ds(pl.multiple_of(slot * own_rows, own_rows), own_rows)]
            return nt(a, w_ref[pl.ds(pl.multiple_of(t * tile, tile), tile)])

        scatter = Scatter(n_ctx, partial, tile, *scratch)
        greet(swap.devices + peers)

        def back(g, b):
            keys_at = pl.ds(g * group, group)
            r = pl.ds(g * group + b * block, block)
            if b == 0:
                dk_ref[...] = jnp.zeros_like(dk_ref)
                dv_ref[...] = jnp.zeros_like(dv_ref)
            key_pos = columns_ref[keys_at, 0:1]
            ok = (key_pos >= rows_ref[1:2, r]) & (key_pos <= rows_ref[0:1, r])
            da_all = nn(dh_ref[r], out_w_ref[...]).astype(BF)

            for h in range(heads):
                lanes = slice(h * LANES, (h + 1) * LANES)
                da, q = da_all[:, lanes], qkv_ref[r, lanes]
                keys = qkv_ref[keys_at, k_at : k_at + LANES]
                s = nt(keys, q) * SCALE - lse_ref[h : h + 1, r]
                p = jnp.exp(jnp.where(ok, s, MASK_FILL))
                dv_ref[...] += nn(p.astype(BF), da)
                delta = jnp.transpose(da.astype(F32) * attn_ref[r, lanes].astype(F32))
                delta = jnp.sum(delta, 0, keepdims=True)
                dp = nt(qkv_ref[keys_at, v_at : v_at + LANES], da)
                ds = (p * (dp - delta)).astype(BF)
                dk_ref[...] += nn(ds, q)
                dq = tn(ds, keys) * SCALE
                dproj_ref[r, lanes] = rotate(dq, cos_ref[r], -sin_ref[r]).astype(BF)

            if b == group // block - 1:
                dk = rotate(dk_ref[...] * SCALE, cos_ref[keys_at], -sin_ref[keys_at])
                dproj_ref[keys_at, k_at : k_at + LANES] = dk.astype(BF)
                dproj_ref[keys_at, v_at : v_at + LANES] = dv_ref[...].astype(BF)

        def out_gradient():
            @pl.loop(0, width // 384)
            def _(k):
                d = pl.ds(pl.multiple_of(k * 384, 384), 384)
                g_ref[d] = jnp.transpose(tn(attn_ref[...], dh_ref[:, d])).astype(BF)

        def own_place(outer):
            return pl.ds(pl.multiple_of(outer * (width // n_outer), 16), width // n_outer)

        def qkv_gradient(first, last):
            half = HEAD_SIZE // 2

            @pl.loop(first, last)
            def _(t):
                lanes = pl.ds(pl.multiple_of(t * 256, 256), 256)
                for h in range(heads + 2):
                    g = tn(dproj_ref[:, h * LANES : (h + 1) * LANES], xn_ref[:, lanes]).astype(BF)
                    for k in range(2):
                        at = h * HEAD_SIZE + k * half
                        g_qkv_ref[at : at + half, lanes] = g[k * LANES // 2 : k * LANES // 2 + half]

        load.wait()
        units = [(g, b) for g in range(2) for b in range(group // block)]
        scatter.to_mate()
        dh_load.wait()
        back(*units[0])
        scatter.pairs()
        swap.begin()
        out_gradient()
        back(*units[1])
        scatter.join()
        g_copies = [
            send(g_ref.at[own_place(device[0])], g_arrived.at[k], g_send.at[k], g_recv.at[k], device)
            for k, device in enumerate(peers)
        ]
        for unit in units[2:]:
            back(*unit)
        for copy in g_copies:
            copy.wait_recv()
        g_total = g_ref[own_place(o)].astype(F32)
        for k in range(n_outer - 1):
            g_total = g_total + g_arrived[k].astype(F32)
        for d in range(2 * n_ctx):
            g_sum[d] = g_total[d * place_rows : (d + 1) * place_rows].astype(BF)
        qkv_gradient(0, 2)
        g_swap.begin()
        qkv_gradient(2, width // 256)
        scatter.end()
        swap.end()

        def finish(r):
            result_ref[r] = (h_ref[r] + total[r]).astype(BF)

        row_chunks(own_rows, 32, finish)
        g_swap.end()
        for copy in g_copies:
            copy.wait_send()

    outs = [
        shape(qkv.shape, BF),
        shape((own_rows, width), BF),
        shape(swapped.shape, BF),
        shape((2 * n_ctx, place_rows, features), BF),
        shape((qkv.shape[1] // LANES * HEAD_SIZE, width), BF),
    ]
    ins = [dh_all, xn, qkv, attn, lse, cosine, sine, pos_rows, pos_columns, hidden, out_w, down_w, h1, swapped]
    scratch = [
        pltpu.VMEM(xn.shape, BF),
        pltpu.VMEM(qkv.shape, BF),
        pltpu.VMEM(attn.shape, BF),
        pltpu.VMEM(cosine.shape, F32),
        pltpu.VMEM(sine.shape, F32),
        pltpu.VMEM(pos_columns.shape, jnp.int32),
        pltpu.VMEM((width, features), BF),
        pltpu.VMEM((n_outer - 1, width // n_outer, features), BF),
        pltpu.VMEM((2 * n_ctx, place_rows, features), BF),
        pltpu.SemaphoreType.DMA((n_outer - 1,)),
        pltpu.SemaphoreType.DMA((n_outer - 1,)),
        pltpu.VMEM((group, LANES), F32),
        pltpu.VMEM((group, LANES), F32),
        pltpu.VMEM(down_w.shape, BF),
        pltpu.VMEM(out_w.shape, BF),
        pltpu.VMEM(dh_all.shape, BF),
        pltpu.SemaphoreType.DMA((1,)),
        pltpu.SemaphoreType.DMA((8,)),
    ]
    scratch += swap_sems(1, n_ctx) + swap_sems(1, n_ctx) + scatter_scratch(own_rows, width)
    return remote_call(kernel, number, ins, outs, scratch, any_ins=(0, 1, 2, 3, 5, 6, 8, 10, 11))


def attention_input(dproj, w, tokens, dh1, gain, g_qkv, dgain_two, n_outer, n_ctx, number):
    rows, width = tokens.shape
    tile = 256
    features = dproj.shape[1]
    n = 2 * n_ctx
    half = HEAD_SIZE // 2

    def kernel(
        d_ref, w_hbm, x_ref, dh_ref, gain_ref, g_ref, dgain_ref, out_ref, sum_ref, w_ref, load_sem, *scratch
    ):
        own_terms, terms, summed, arrived, plane_send, plane_recv, send_sem, recv_sem = scratch[:8]
        scratch = scratch[8:]
        total = scratch[-1]
        load = Load(padded_loads(w_hbm, w_ref), load_sem).begin()
        o = lax.axis_index("o")

        def partial(slot, t):
            a = d_ref[pl.ds(pl.multiple_of(slot * rows, rows), rows)]
            return nn(a, w_ref[:, pl.ds(pl.multiple_of(t * tile, tile), tile)])

        scatter = Scatter(n_ctx, partial, tile, *scratch)
        i, c = lax.axis_index("i"), lax.axis_index("ctx")
        me = i * n_ctx + c
        plane = [lax.rem(me + k, n) for k in range(1, n)]
        plane = [(o, d // n_ctx, d % n_ctx) for d in plane]
        peers = outer_peers(n_outer)
        greet(plane + peers)
        load.wait()

        @pl.loop(0, width // tile)
        def _(t):
            lanes = pl.ds(pl.multiple_of(t * tile, tile), tile)
            acc = jnp.zeros((half, tile), F32)
            for k in range(features * 2 // LANES):
                weight = w_ref[k * LANES // 2 : k * LANES // 2 + half, lanes].astype(F32)
                acc = acc + weight * g_ref[k * half : (k + 1) * half, lanes].astype(F32)
            own_terms[0:1, lanes] = jnp.sum(acc, 0, keepdims=True) / gain_ref[0:1, lanes]
            own_terms[1:2, lanes] = dgain_ref[0:1, lanes]

        scatter.to_mate()
        plane_copies = [
            send(own_terms, terms.at[k], plane_send.at[k], plane_recv.at[k], device) for k, device in enumerate(plane)
        ]
        scatter.pairs()
        for copy in plane_copies:
            copy.wait_recv()
        part = own_terms[...]
        for k in range(n - 1):
            part = part + terms[k]
        summed[...] = part
        scatter.join()
        copies = []
        for k, device in enumerate(peers):
            copies.append(send(summed, arrived.at[k], send_sem.at[k], recv_sem.at[k], device))
        scatter.end()

        def finish(r):
            x, d = x_ref[r].astype(F32), total[r]
            out_ref[r] = dh_ref[r] + norm_back(d, gain_ref[0:1], x, inv_rms(x))

        row_chunks(rows, 32, finish)
        for copy in copies:
            copy.wait_recv()
        part = summed[...]
        for k in range(n_outer - 1):
            part = part + arrived[k]
        sum_ref[...] = part
        for copy in copies + plane_copies:
            copy.wait_send()

    outs = [shape((rows, width), F32), shape((2, width), F32)]
    ins = [dproj, w, tokens, dh1, gain, g_qkv, dgain_two]
    n_loads = features // (LANES // 2)
    scratch = [pltpu.VMEM((features, width), BF), pltpu.SemaphoreType.DMA((n_loads,))]
    scratch += [
        pltpu.VMEM((2, width), F32),
        pltpu.VMEM((n - 1, 2, width), F32),
        pltpu.VMEM((2, width), F32),
        pltpu.VMEM((n_outer - 1, 2, width), F32),
        pltpu.SemaphoreType.DMA((n - 1,)),
        pltpu.SemaphoreType.DMA((n - 1,)),
        pltpu.SemaphoreType.DMA((n_outer - 1,)),
        pltpu.SemaphoreType.DMA((n_outer - 1,)),
    ]
    scratch += scatter_scratch(rows, width)
    return remote_call(kernel, number, ins, outs, scratch, any_ins=(1,))


def make_shards(n_outer, n_inner, n_ctx):
    n_plane = n_inner * n_ctx
    moves = feature_moves(n_outer, n_plane)
    back = [(b, a) for a, b in moves]

    def layer(tokens, norm_attn, w_qkv, w_out, norm_mlp, w_gate_up, w_down, cotangent, seq_lengths, block_slot):
        _, width = tokens.shape
        gain_rows = norm_attn.shape[0]
        out_rows = w_out.shape[0]
        unit_rows = w_gate_up.shape[0]
        n_seqs, n_slots = seq_lengths.shape[1], block_slot.shape[1]
        units = FF // n_plane
        qkv_w = z_ag(lax.ppermute(w_qkv, ALL, moves)).reshape(CHUNKS, -1, width)
        gain_part = jnp.pad(jnp.stack([norm_attn, norm_mlp]), ((0, 6), (0, LANES - gain_rows)))
        meta = jnp.concatenate([seq_lengths[0], block_slot[0]])
        meta = jnp.pad(meta[None], ((0, 7), (0, LANES - n_seqs - n_slots)))
        out_parts = pad_heads(w_out, 1).reshape(out_rows, 2, n_plane // 2, -1).transpose(2, 1, 0, 3)
        out_parts = out_parts.reshape(n_plane, out_rows, -1)
        down_parts = w_down.reshape(out_rows, n_outer // 2, n_plane, unit_rows).transpose(2, 0, 1, 3)
        down_parts = down_parts.reshape(n_plane, out_rows, units)
        w_gate_up, out_parts, down_parts = lax.optimization_barrier((w_gate_up, out_parts, down_parts))
        gate_up = z_ag(w_gate_up)
        gate_up = gate_up.reshape(CHUNKS, -1, width)
        x_all, out_parts, down_parts, gains, cosine, sine, pos_rows, pos_columns = prologue(
            tokens, out_parts, down_parts, gain_part, meta, n_seqs, n_outer, n_ctx, 1
        )
        x_all = x_all.reshape(-1, width)
        gains = gains[:, :, :2, :gain_rows].transpose(2, 0, 1, 3).reshape(2, width)
        qkv, attn, lse, dy_all, xn1, out_w = attention_forward(
            x_all, gains, qkv_w, cosine, sine, pos_rows, pos_columns, cotangent, out_parts, n_outer, n_ctx, 2
        )
        out_w = out_w.reshape(width, -1)
        h1, xn2, down_w = output_projection(attn, out_w, tokens, gains, down_parts, n_outer, n_ctx, 3)
        down_w = down_w.reshape(-1, units)
        xn2_all, hidden, dgu, dgu_t, g_down = feed_forward(xn2, dy_all, gate_up, down_w, n_ctx, 4)
        dgu, g_down = lax.optimization_barrier((dgu, g_down))
        g_down = z_rs(g_down)
        dh1, dh1_bf, dgain_two, g_gate_up = feed_forward_input(
            dgu, gate_up, h1, cotangent, gains, xn2_all.reshape(-1, width), dgu_t, n_ctx, 5
        )
        g_gate_up = z_rs(g_gate_up)
        dh1_all = plane_gather(dh1_bf, n_ctx, 6)
        dh1_all, g_down = lax.optimization_barrier((dh1_all, g_down))
        g_down = g_down.reshape(n_plane, out_rows, units)
        dproj, result, g_down, g_out, g_qkv = attention_backward(
            dh1_all, xn1, qkv, attn, lse, cosine, sine, pos_rows, pos_columns, hidden, out_w, down_w, h1, g_down, n_outer, n_ctx, 7
        )
        dproj, g_qkv, g_gate_up = lax.optimization_barrier((dproj, g_qkv, g_gate_up))
        g_qkv_plane, g_qkv = g_qkv, z_rs(g_qkv)
        grad_input, g = attention_input(dproj, qkv_w, tokens, dh1, gains, g_qkv_plane, dgain_two, n_outer, n_ctx, 8)
        grad_input, g_qkv = lax.optimization_barrier((grad_input, g_qkv))
        grad_qkv = lax.ppermute(g_qkv, ALL, back).astype(F32)
        g_out = g_out.reshape(n_plane // 2, 2, out_rows, -1).transpose(2, 1, 0, 3)
        grad_out = cut_heads(g_out.reshape(out_rows, -1), 1).astype(F32)
        grad_down = g_down.reshape(n_plane, out_rows, n_outer // 2, unit_rows).transpose(1, 2, 0, 3)
        grad_down = grad_down.reshape(out_rows, -1).astype(F32)
        index = (lax.axis_index("o") * n_inner + lax.axis_index("i")) * n_ctx + lax.axis_index("ctx")
        g = lax.dynamic_slice_in_dim(g, index * gain_rows, gain_rows, 1)
        return (result, grad_input, g[0], grad_qkv, grad_out, g[1], g_gate_up.astype(F32), grad_down)

    return layer


def solution(mesh):
    n_inner = 2
    n_ctx = mesh.shape["ctx"]
    n_outer = mesh.shape["dp"] // n_inner
    split = Mesh(mesh.devices.reshape(n_outer, n_inner, n_ctx), ALL)
    rows, vec, grp = P(ALL, None), P(ALL), P(("o", "i"), None)
    return jax.shard_map(
        make_shards(n_outer, n_inner, n_ctx),
        mesh=split,
        in_specs=(rows, vec, rows, rows, vec, rows, rows, rows, grp, grp),
        out_specs=(rows, rows, vec, rows, rows, vec, rows, rows),
        check_vma=False,
    )
```

```python
import math

import jax
import jax.numpy as jnp
import numpy as np
from jax import lax
from jax.experimental import pallas as pl
from jax.experimental.pallas import tpu as pltpu
from jax.sharding import Mesh
from jax.sharding import PartitionSpec as P


QUERY_HEADS = 16
HEAD_SIZE = 96
FF = 4096
BLK = 128
LANES = 128
QUERY_BLOCK = 512
CHUNKS = 4

EPSILON = 1e-05
THETA = 100000.0
MASK_FILL = -1e30
BF = jnp.bfloat16
F32 = jnp.float32
ALL = ("o", "i", "ctx")
MESH = pl.DeviceIdType.MESH
SCALE = 1.0 / math.sqrt(HEAD_SIZE)


def nt(a, b):
    return lax.dot_general(a, b, (((1,), (1,)), ((), ())), preferred_element_type=F32)


def nn(a, b):
    return lax.dot_general(a, b, (((1,), (0,)), ((), ())), preferred_element_type=F32)


def tn(a, b):
    return lax.dot_general(a, b, (((0,), (0,)), ((), ())), preferred_element_type=F32)


def z_ag(x):
    return lax.all_gather(x, "o", axis=0, tiled=True)


def z_rs(x):
    return lax.psum_scatter(x, "o", scatter_dimension=0, tiled=True)


def inv_rms(x):
    return lax.rsqrt(jnp.mean(x * x, -1, keepdims=True) + EPSILON)


def norm_back(grad_normed, gain, source, scale):
    weighted = grad_normed * gain
    return scale * weighted - source * scale**3 * jnp.mean(weighted * source, -1, keepdims=True)


def feature_moves(n_outer, n_plane):
    moves = []
    half, quarter = n_outer // 2, n_outer // 4
    for block in range(n_outer * n_plane):
        if block < 4 * n_outer:
            head, step = block // half, block % half
        elif block < 6 * n_outer:
            head, step = divmod(block - 4 * n_outer, quarter)
            step += half
        else:
            head, step = divmod(block - 6 * n_outer, quarter)
            step += half + quarter
        place = 2 * (head % (n_plane // 2)) + head // (n_plane // 2)
        moves.append((block, step * n_plane + place))
    return moves


def pad_heads(x, axis):
    half = HEAD_SIZE // 2
    shape = x.shape
    x = x.reshape(shape[:axis] + (-1, half) + shape[axis + 1 :])
    pads = [(0, 0)] * x.ndim
    pads[axis + 1] = (0, LANES // 2 - half)
    return jnp.pad(x, pads).reshape(shape[:axis] + (-1,) + shape[axis + 1 :])


def cut_heads(x, axis):
    half = HEAD_SIZE // 2
    shape = x.shape
    x = x.reshape(shape[:axis] + (-1, LANES // 2) + shape[axis + 1 :])
    x = lax.slice_in_dim(x, 0, half, axis=axis + 1)
    return x.reshape(shape[:axis] + (-1,) + shape[axis + 1 :])


def places(n_ctx):
    o, i, c = lax.axis_index("o"), lax.axis_index("i"), lax.axis_index("ctx")
    return o, i, c, c + 1 - 2 * (c % 2), (c + n_ctx // 2) % n_ctx


def greet(devices):
    barrier = pltpu.get_barrier_semaphore()
    for device in devices:
        pl.semaphore_signal(barrier, inc=1, device_id=device, device_id_type=MESH)
    pl.semaphore_wait(barrier, len(devices))


def greet_neighbours(n_ctx):
    o, i, c, mate, far = places(n_ctx)
    greet([(o, i, mate), (o, 1 - i, c), (o, i, far)])


def send(src, dst, send_sem, recv_sem, device):
    copy = pltpu.make_async_remote_copy(
        src_ref=src, dst_ref=dst, send_sem=send_sem, recv_sem=recv_sem, device_id=device, device_id_type=MESH
    )
    copy.start()
    return copy


class Gather:
    def __init__(self, n_ctx, src, out, send_sem, recv_sem, local_sem):
        self.src, self.out, self.sems = src, out, (send_sem, recv_sem, local_sem)
        o, i, c, mate, far = places(n_ctx)
        j, core = 1 - i, c % 2
        self.mate, self.x, self.y = (o, i, mate), (o, j, c), (o, i, far)
        self.me, self.s_x = i * n_ctx + c, j * n_ctx + c
        self.s_y, self.s_d = i * n_ctx + far, j * n_ctx + far
        self.relay = (o, j * core + i * (1 - core), c * core + far * (1 - core))
        self.relayed = self.s_y * core + self.s_x * (1 - core)
        mate_far = (mate + n_ctx // 2) % n_ctx
        self.mates_slots = [i * n_ctx + mate, j * n_ctx + mate, i * n_ctx + mate_far, j * n_ctx + mate_far]
        self.copies = {}

    def go(self, kind, part, src, slot, device):
        rows = src.shape[0] // PARTS
        at = pl.ds(part * rows, rows)
        copy = send(src.at[at], self.out.at[slot, at], self.sems[0].at[kind, part], self.sems[1].at[kind, part], device)
        self.copies[kind, part] = copy

    def begin(self):
        for part in range(PARTS):
            self.go(1, part, self.src, self.me, self.x)
            self.go(2, part, self.src, self.me, self.y)
        for part in range(PARTS):
            self.go(0, part, self.src, self.me, self.mate)
        self.own = pltpu.make_async_copy(self.src, self.out.at[self.me], self.sems[2])
        self.own.start()

    def middle(self):
        for part in range(PARTS):
            self.copies[1, part].wait_recv()
            self.copies[2, part].wait_recv()
            self.go(5, part, self.out.at[self.relayed], self.relayed, self.relay)
            self.go(3, part, self.out.at[self.s_x], self.s_x, self.mate)
            self.go(4, part, self.out.at[self.s_y], self.s_y, self.mate)

    def corner(self):
        for part in range(PARTS):
            self.copies[5, part].wait_recv()
            self.go(6, part, self.out.at[self.s_d], self.s_d, self.mate)

    def arrived(self, kind):
        for part in range(PARTS):
            self.copies[kind, part].wait_recv()

    def sent(self):
        self.own.wait()
        for copy in self.copies.values():
            copy.wait_send()

    def end(self):
        self.corner()
        for kind in (0, 3, 4, 6):
            self.arrived(kind)
        self.sent()


PARTS = 2
GATHER_SEMS = [pltpu.SemaphoreType.DMA((7, PARTS)), pltpu.SemaphoreType.DMA((7, PARTS)), pltpu.SemaphoreType.DMA]


class Scatter:
    def __init__(self, n_ctx, partial, tile, ready, from_mate, going, got, send_sem, recv_sem, total):
        self.partial, self.tile = partial, tile
        self.ready, self.from_mate, self.going, self.got = ready, from_mate, going, got
        self.sems, self.total = (send_sem, recv_sem), total
        o, i, c, mate, far = places(n_ctx)
        j, core = 1 - i, c % 2
        self.core = core
        far_mate = (mate + n_ctx // 2) % n_ctx
        self.mine = [j * n_ctx + far, j * n_ctx + c, i * n_ctx + far, i * n_ctx + c]
        self.theirs = [j * n_ctx + far_mate, j * n_ctx + mate, i * n_ctx + far_mate, i * n_ctx + mate]
        self.mate = (o, i, mate)
        self.combined = (o, j * (1 - core) + i * core, c * (1 - core) + far * core)
        self.direct = (o, j * core + i * (1 - core), c * core + far * (1 - core))
        self.s_direct = self.mine[2] * (1 - core) + self.mine[1] * core
        self.s_combined = self.mine[1] * (1 - core) + self.mine[2] * core
        self.copies = []

    def go(self, kind, part, src, dst, device):
        copy = send(src.at[part], dst.at[part], self.sems[0].at[kind, part], self.sems[1].at[kind, part], device)
        self.copies.append(copy)
        return copy

    def each(self, part, body):
        tiles = self.ready.shape[-1] // self.tile

        @pl.loop(0, tiles)
        def _(t):
            at = pl.multiple_of(t * self.tile, self.tile)
            body(part * tiles + t, pl.ds(at, self.tile), pl.ds(part * tiles * self.tile + at, self.tile))

    def fill(self, n, part):
        def body(t, lanes, _):
            self.ready[n, part, :, lanes] = self.partial(self.theirs[n], t).astype(BF)

        self.each(part, body)

    def give(self, n, part):
        self.mates[n, part] = self.go(n, part, self.ready.at[n], self.from_mate.at[n], self.mate)

    def pair(self, slot, n, part, place):
        def body(t, lanes, _):
            pair = self.partial(slot, t) + self.from_mate[n, part, :, lanes].astype(F32)
            self.going[place, part, :, lanes] = pair.astype(BF)

        self.each(part, body)

    def to_mate(self):
        self.mates, self.straights, self.diagonals, self.joins = {}, [], [], []
        order = [(0, 0), (0, 1), (1, 0), (2, 0), (1, 1), (2, 1), (3, 0), (3, 1)]
        self.fill(*order[0])
        for k, at in enumerate(order[1:]):
            self.fill(*at)
            self.give(*order[k])
            if k == 2:
                self.mates[0, 0].wait_recv()
                self.pair(self.mine[0], 0, 0, 0)
            if k == 3:
                self.diagonals.append(self.go(4, 0, self.going.at[0], self.got.at[0], self.direct))
                self.mates[0, 1].wait_recv()
                self.pair(self.mine[0], 0, 1, 0)
            if k == 4:
                self.diagonals.append(self.go(4, 1, self.going.at[0], self.got.at[0], self.direct))
        self.last = order[-1]

    def pairs(self):
        for part in range(PARTS):
            self.mates[1, part].wait_recv()
            self.mates[2, part].wait_recv()
            self.pair(self.s_direct, 2 - self.core, part, 1)
            if part == 0:
                self.give(*self.last)
            else:
                self.straights.append(self.go(5, part - 1, self.going.at[1], self.got.at[1], self.direct))

    def join(self):
        for part in range(PARTS):
            self.diagonals[part].wait_recv()
            if part == 0:
                self.straights.append(self.go(5, PARTS - 1, self.going.at[1], self.got.at[1], self.direct))

            def combined(t, lanes, _):
                pair = self.partial(self.s_combined, t) + self.from_mate[1 + self.core, part, :, lanes].astype(F32)
                self.going[2, part, :, lanes] = (pair + self.got[0, part, :, lanes].astype(F32)).astype(BF)

            self.each(part, combined)
            if part:
                self.joins.append(self.go(6, part - 1, self.going.at[2], self.got.at[2], self.combined))
        self.own(0)
        self.joins.append(self.go(6, PARTS - 1, self.going.at[2], self.got.at[2], self.combined))

    def own(self, part):
        self.mates[3, part].wait_recv()

        def body(t, lanes, out):
            self.total[:, out] = self.partial(self.mine[3], t) + self.from_mate[3, part, :, lanes].astype(F32)

        self.each(part, body)

    def end(self):
        total = self.total
        for part in range(1, PARTS):
            self.own(part)
        for part in range(PARTS):
            self.straights[part].wait_recv()
            self.joins[part].wait_recv()

            def rest(t, lanes, out):
                other = self.got[1, part, :, lanes].astype(F32) + self.got[2, part, :, lanes].astype(F32)
                total[:, out] = total[:, out] + other

            self.each(part, rest)
        for copy in self.copies:
            copy.wait_send()


def scatter_scratch(rows, width):
    return [
        pltpu.VMEM((4, PARTS, rows, width // PARTS), BF),
        pltpu.VMEM((4, PARTS, rows, width // PARTS), BF),
        pltpu.VMEM((3, PARTS, rows, width // PARTS), BF),
        pltpu.VMEM((3, PARTS, rows, width // PARTS), BF),
        pltpu.SemaphoreType.DMA((7, PARTS)),
        pltpu.SemaphoreType.DMA((7, PARTS)),
        pltpu.VMEM((rows, width), F32),
    ]


def row_chunks(rows, step, body):
    @pl.loop(0, rows // step)
    def _(r):
        body(pl.ds(pl.multiple_of(r * step, step), step))


class Load:
    def __init__(self, parts, sem):
        self.copies = [pltpu.make_async_copy(src, dst, sem.at[n]) for n, (src, dst) in enumerate(parts)]

    def begin(self):
        for copy in self.copies:
            copy.start()
        return self

    def wait(self):
        for copy in self.copies:
            copy.wait()


IN_VMEM = pl.BlockSpec(memory_space=pltpu.VMEM)
ANYWHERE = pl.BlockSpec(memory_space=pl.ANY)


def remote_call(kernel, number, ins, outs, scratch, any_outs=(), any_ins=()):
    return pl.pallas_call(
        kernel,
        out_shape=outs,
        in_specs=[ANYWHERE if n in any_ins else IN_VMEM for n in range(len(ins))],
        out_specs=[ANYWHERE if n in any_outs else IN_VMEM for n in range(len(outs))],
        scratch_shapes=scratch,
        compiler_params=pltpu.CompilerParams(collective_id=number, has_side_effects=True, vmem_limit_bytes=60 << 20),
    )(*ins)


def shape(dims, dtype):
    return jax.ShapeDtypeStruct(tuple(dims), dtype)


class Swap:
    def __init__(self, n_ctx, pairs, send_sem, recv_sem, local_sem):
        self.pairs, self.sems = pairs, (send_sem, recv_sem, local_sem)
        self.o, i, c, _, _ = places(n_ctx)
        self.n, self.n_ctx = 2 * n_ctx, n_ctx
        self.me = i * n_ctx + c
        self.others = [(self.me + k) % self.n for k in range(1, self.n)]
        self.devices = [(self.o, d // n_ctx, d % n_ctx) for d in self.others]

    def begin(self):
        self.copies, self.own = [], []
        for a, (src, dst) in enumerate(self.pairs):
            for k, (d, device) in enumerate(zip(self.others, self.devices)):
                self.copies.append(
                    send(src.at[d], dst.at[self.me], self.sems[0].at[a, k], self.sems[1].at[a, k], device)
                )
            own = pltpu.make_async_copy(src.at[self.me], dst.at[self.me], self.sems[2].at[a])
            own.start()
            self.own.append(own)

    def end(self):
        for copy in self.copies:
            copy.wait_recv()
            copy.wait_send()
        for copy in self.own:
            copy.wait()


def swap_sems(n_arrays, n_ctx):
    return [
        pltpu.SemaphoreType.DMA((n_arrays, 2 * n_ctx - 1)),
        pltpu.SemaphoreType.DMA((n_arrays, 2 * n_ctx - 1)),
        pltpu.SemaphoreType.DMA((n_arrays,)),
    ]


def outer_peers(n_outer):
    o, i, c = lax.axis_index("o"), lax.axis_index("i"), lax.axis_index("ctx")
    return [(lax.rem(o + k, n_outer), i, c) for k in range(1, n_outer)]


def rotary_constants():
    frequency = THETA ** -(np.arange(HEAD_SIZE // 2) * (2.0 / HEAD_SIZE))
    rates = np.zeros((8, LANES), np.float32)
    for half, sign in ((0, -1.0), (LANES // 2, 1.0)):
        rates[0, half : half + HEAD_SIZE // 2] = frequency
        rates[1, half : half + HEAD_SIZE // 2] = sign
    angles = np.arange(BLK)[:, None] * rates[0].astype(np.float64)
    return rates, np.stack([np.cos(angles), np.sin(angles)]).astype(np.float32)


def prologue(tokens, out_parts, down_parts, gains, meta, n_seqs, n_outer, n_ctx, number):
    rows, width = tokens.shape
    n = 2 * n_ctx
    blocks = n_ctx * rows // BLK

    def kernel(
        x_ref,
        out_src,
        down_src,
        gains_ref,
        meta_ref,
        rates_ref,
        angles_ref,
        x_all,
        out_dst,
        down_dst,
        gains_out,
        cos_ref,
        sin_ref,
        rows_ref,
        columns_ref,
        *sems,
    ):
        o = lax.axis_index("o")
        metas_ref, send_sem, recv_sem, local_sem = sems[:4]
        out_swap = Swap(n_ctx, [(out_src, out_dst)], *sems[4:7])
        down_swap = Swap(n_ctx, [(down_src, down_dst)], *sems[7:10])
        gather = Gather(n_ctx, x_ref, x_all, *sems[10:])
        peers = outer_peers(n_outer)
        me = out_swap.me
        greet(out_swap.devices + peers)
        gather.begin()
        own = [
            pltpu.make_async_copy(meta_ref, metas_ref.at[me], local_sem.at[0]),
            pltpu.make_async_copy(gains_ref, gains_out.at[o, me], local_sem.at[1]),
        ]
        meta_copies, gain_copies, z_copies = [], [], []
        for copy in own:
            copy.start()
        for k, device in enumerate(out_swap.devices):
            meta_copies.append(send(meta_ref, metas_ref.at[me], send_sem.at[0, k], recv_sem.at[0, k], device))
            gain_copies.append(send(gains_ref, gains_out.at[o, me], send_sem.at[1, k], recv_sem.at[1, k], device))
        out_swap.begin()
        for copy in own:
            copy.wait()
        for copy in meta_copies:
            copy.wait_recv()
        lane = lax.broadcasted_iota(jnp.int32, (BLK, LANES), 1)
        row = lax.broadcasted_iota(jnp.int32, (BLK, LANES), 0)
        rows_ref[...] = jnp.zeros_like(rows_ref)
        pieces = 2 * blocks * n_seqs
        piece = lax.broadcasted_iota(jnp.int32, (pieces, LANES), 0)
        bases = jnp.zeros((pieces, LANES), jnp.int32)
        places_of = []
        for g in range(2):
            starts, end = [], jnp.zeros((1, 1), jnp.int32)
            for q in range(n_seqs):
                starts.append(end)
                end = end + metas_ref[g * n_ctx, 0:1, q : q + 1]
            for b in range(blocks):
                first = metas_ref[g * n_ctx, 0:1, n_seqs + b : n_seqs + b + 1] * BLK
                for q in range(n_seqs):
                    index = (g * blocks + b) * n_seqs + q
                    bases = jnp.where(piece == index, first - starts[q], bases)
                places_of.append((first, starts))
        angle = bases.astype(F32) * rates_ref[0:1]
        base_cos, base_sin = jnp.cos(angle), jnp.sin(angle)
        for n_block, (first, starts) in enumerate(places_of):
            at = slice(n_block * BLK, (n_block + 1) * BLK)
            stream, lanes_stream = first + row, first + lane[0:1]
            start, lanes_start = jnp.zeros_like(stream), jnp.zeros_like(lanes_stream)
            cos, sin = angles_ref[0], angles_ref[1]
            for q in range(n_seqs):
                index = n_block * n_seqs + q
                cos_0, sin_0 = base_cos[index : index + 1], base_sin[index : index + 1]
                cos_q = cos_0 * angles_ref[0] - sin_0 * angles_ref[1]
                sin_q = sin_0 * angles_ref[0] + cos_0 * angles_ref[1]
                inside = stream >= starts[q]
                start = jnp.where(inside, starts[q], start)
                lanes_start = jnp.where(lanes_stream >= starts[q], starts[q], lanes_start)
                cos, sin = jnp.where(inside, cos_q, cos), jnp.where(inside, sin_q, sin)
            cos_ref[at] = cos
            sin_ref[at] = sin * rates_ref[1:2]
            columns_ref[at] = jnp.where(lane == 0, stream, start)
            rows_ref[0:1, at] = lanes_stream
            rows_ref[1:2, at] = lanes_start
        for copy in gain_copies:
            copy.wait_recv()
        for k, device in enumerate(peers):
            z_copies.append(send(gains_out.at[o], gains_out.at[o], send_sem.at[2, k], recv_sem.at[2, k], device))
        gather.middle()
        down_swap.begin()
        gather.end()
        out_swap.end()
        down_swap.end()
        for copy in z_copies:
            copy.wait_recv()
        for copy in meta_copies + gain_copies + z_copies:
            copy.wait_send()

    outs = [
        shape((n, rows, width), BF),
        shape(out_parts.shape, BF),
        shape(down_parts.shape, BF),
        shape((n_outer, n) + gains.shape, F32),
        shape((n * rows, LANES), F32),
        shape((n * rows, LANES), F32),
        shape((8, n * rows), jnp.int32),
        shape((n * rows, LANES), jnp.int32),
    ]
    rates, angles = rotary_constants()
    ins = [tokens, out_parts, down_parts, gains, meta, jnp.asarray(rates), jnp.asarray(angles)]
    most = max(n, n_outer) - 1
    scratch = [
        pltpu.VMEM((n,) + meta.shape, jnp.int32),
        pltpu.SemaphoreType.DMA((3, most)),
        pltpu.SemaphoreType.DMA((3, most)),
        pltpu.SemaphoreType.DMA((2,)),
    ]
    scratch += swap_sems(1, n_ctx) + swap_sems(1, n_ctx) + GATHER_SEMS
    return remote_call(kernel, number, ins, outs, scratch, any_outs=(0,))


def plane_gather(x, n_ctx, number):
    def kernel(src, out, *sems):
        gather = Gather(n_ctx, src, out, *sems)
        greet_neighbours(n_ctx)
        gather.begin()
        gather.middle()
        gather.end()

    outs = [shape((2 * n_ctx,) + x.shape, x.dtype)]
    got = remote_call(kernel, number, [x], outs, GATHER_SEMS, any_outs=(0,))
    return got[0].reshape(-1, x.shape[-1])


def rotate(x, cosine, sine):
    return x * cosine + pltpu.roll(x, LANES // 2, 1) * sine


def qkv_rows(features):
    return features // LANES * HEAD_SIZE // CHUNKS


def padded_loads(w_ref, w_pad):
    half = HEAD_SIZE // 2
    rows = qkv_rows(w_pad.shape[0])
    pairs, at = [], 0
    for row in range(half, w_pad.shape[0], LANES // 2):
        w_pad[row : row + LANES // 2 - half] = jnp.zeros((LANES // 2 - half, w_pad.shape[1]), BF)
    for n in range(w_ref.shape[0]):
        for b in range(rows // half):
            src = w_ref.at[n, pl.ds(b * half, half)]
            pairs.append((src, w_pad.at[pl.ds(at * LANES // 2, half)]))
            at += 1
    return pairs


def attention_forward(x_all, gains, w, cosine, sine, pos_rows, pos_columns, dy, out_part, n_outer, n_ctx, number):
    rows, width = x_all.shape
    group = rows // 2
    heads = QUERY_HEADS // (2 * n_ctx)
    features = (heads + 2) * LANES
    k_at, v_at = heads * LANES, (heads + 1) * LANES
    block = min(QUERY_BLOCK, group)
    n_loads = features // (LANES // 2)

    def kernel(
        x_hbm,
        gain_ref,
        w_hbm,
        cos_ref,
        sin_ref,
        rows_ref,
        columns_ref,
        dy_ref,
        part_ref,
        qkv_ref,
        attn_ref,
        lse_ref,
        dy_all,
        xn_out,
        out_w,
        w_ref,
        xn_ref,
        load_sem,
        xn_sem,
        store_sem,
        z_send,
        z_recv,
        z_local,
        *sems,
    ):
        gather = Gather(n_ctx, dy_ref, dy_all, *sems)
        load = Load(padded_loads(w_hbm, w_ref), load_sem).begin()
        xn_load = Load([(x_hbm, xn_ref)], xn_sem).begin()
        o = lax.axis_index("o")
        peers = outer_peers(n_outer)
        greet([gather.mate, gather.x, gather.y] + peers)
        gather.begin()
        z_copies = [send(part_ref, out_w.at[o], z_send.at[k], z_recv.at[k], device) for k, device in enumerate(peers)]
        own_part = pltpu.make_async_copy(part_ref, out_w.at[o], z_local)
        own_part.start()
        load.wait()
        xn_load.wait()

        def normalise(r):
            x = xn_ref[r].astype(F32)
            xn_ref[r] = (x * inv_rms(x) * gain_ref[0:1]).astype(BF)

        def project(r):
            cos, sin = cos_ref[r], sin_ref[r]
            for h in range(heads + 2):
                lanes = slice(h * LANES, (h + 1) * LANES)
                part = nt(xn_ref[r], w_ref[lanes])
                qkv_ref[r, lanes] = (rotate(part, cos, sin) if h <= heads else part).astype(BF)

        def attend(g):
            keys_at = pl.ds(g * group, group)

            @pl.loop(0, group // block)
            def _(b):
                r = pl.ds(pl.multiple_of(g * group + b * block, block), block)
                key_pos = rows_ref[0:1, keys_at]
                ok = (key_pos >= columns_ref[r, 1:2]) & (key_pos <= columns_ref[r, 0:1])
                for h in range(heads):
                    lanes = slice(h * LANES, (h + 1) * LANES)
                    s = nt(qkv_ref[r, lanes], qkv_ref[keys_at, k_at : k_at + LANES])
                    s = jnp.where(ok, s, MASK_FILL)
                    high = jnp.max(s, -1, keepdims=True)
                    e = jnp.exp((s - high) * SCALE)
                    total = jnp.sum(e, -1, keepdims=True)
                    mixed = nn(e.astype(BF), qkv_ref[keys_at, v_at : v_at + LANES])
                    attn_ref[r, lanes] = (mixed / total).astype(BF)
                    lse = jnp.broadcast_to(high * SCALE + jnp.log(total), (block, LANES))
                    lse_ref[h : h + 1, r] = jnp.transpose(lse)[0:1]

        row_chunks(rows, 64, normalise)
        row_chunks(rows, block, project)
        gather.middle()
        store = Load([(xn_ref, xn_out)], store_sem).begin()
        attend(0)
        attend(1)
        gather.end()
        store.wait()
        own_part.wait()
        for copy in z_copies:
            copy.wait_recv()
            copy.wait_send()

    outs = [
        shape((rows, features), BF),
        shape((rows, heads * LANES), BF),
        shape((8, rows), F32),
        shape((2 * n_ctx,) + dy.shape, BF),
        shape(x_all.shape, BF),
        shape((n_outer,) + out_part.shape, BF),
    ]
    ins = [x_all, gains, w, cosine, sine, pos_rows, pos_columns, dy, out_part]
    scratch = [
        pltpu.VMEM((features, width), BF),
        pltpu.VMEM(x_all.shape, BF),
        pltpu.SemaphoreType.DMA((n_loads,)),
        pltpu.SemaphoreType.DMA((1,)),
        pltpu.SemaphoreType.DMA((1,)),
        pltpu.SemaphoreType.DMA((n_outer - 1,)),
        pltpu.SemaphoreType.DMA((n_outer - 1,)),
        pltpu.SemaphoreType.DMA,
    ]
    scratch += GATHER_SEMS
    got = remote_call(kernel, number, ins, outs, scratch, any_outs=(3, 4), any_ins=(0, 2))
    return got[0], got[1], got[2], got[3].reshape(rows, width), got[4], got[5]


def output_projection(attn, out_w, tokens, gain, n_ctx, number):
    rows, width = tokens.shape
    tile = 256


    def kernel(attn_ref, w_ref, x_ref, gain_ref, h_ref, xn_ref, *scratch):
        total = scratch[-1]

        def partial(slot, t):
            a = attn_ref[pl.ds(pl.multiple_of(slot * rows, rows), rows)]
            return nt(a, w_ref[pl.ds(pl.multiple_of(t * tile, tile), tile)])

        scatter = Scatter(n_ctx, partial, tile, *scratch)
        greet_neighbours(n_ctx)
        scatter.to_mate()
        scatter.pairs()
        scatter.join()
        scatter.end()

        def finish(r):
            h = x_ref[r].astype(F32) + total[r]
            h_ref[r] = h
            xn_ref[r] = (h * inv_rms(h) * gain_ref[1:2]).astype(BF)

        row_chunks(rows, 32, finish)

    outs = [shape((rows, width), F32), shape((rows, width), BF)]
    return remote_call(kernel, number, [attn, out_w, tokens, gain], outs, scatter_scratch(rows, width))


def feed_forward(xn, dy, gate_up, down, n_ctx, number):
    rows, width = xn.shape
    n = 2 * n_ctx
    chunks, unit_rows, _ = gate_up.shape
    units = down.shape[1]
    tile = 256

    def kernel(
        x_ref,
        dy_hbm,
        up_hbm,
        down_hbm,
        xn_all,
        hidden_ref,
        dgu_ref,
        dgu_t,
        g_down_ref,
        raw,
        dy_ref,
        up_ref,
        down_ref,
        hidden_t,
        g_acc,
        load_sem,
        store_sem,
        *sems,
    ):
        gather = Gather(n_ctx, x_ref, raw, *sems)
        pairs = [(up_hbm, up_ref), (down_hbm, down_ref), (dy_hbm, dy_ref)]
        load = Load(pairs, load_sem).begin()
        greet_neighbours(n_ctx)
        gather.begin()
        half = chunks // 2
        core = gather.me % 2

        def chip(slot):
            both = pl.ds(pl.multiple_of((slot - core) * rows, 2 * rows), 2 * rows)
            x = raw[pl.ds(slot - core, 2)].reshape(2 * rows, width)
            for m in range(half):
                lanes = slice(m * unit_rows, (m + 1) * unit_rows)
                second = slice(units + m * unit_rows, units + (m + 1) * unit_rows)
                gate = nt(x, up_ref[m])
                up = nt(x, up_ref[half + m])
                dhid = nn(dy_ref[both], down_ref[:, lanes])
                sg = 1.0 / (1.0 + jnp.exp(-gate))
                act = gate * sg
                hidden = act * up
                dgate = dhid * up * sg * (1.0 + gate * (1.0 - sg))
                dup = dhid * act
                hidden_ref[both, lanes] = hidden.astype(BF)
                dgu_ref[both, lanes] = dgate.astype(BF)
                dgu_ref[both, second] = dup.astype(BF)
                hidden_t[lanes] = jnp.transpose(hidden).astype(BF)
                dgu_t[lanes, both] = jnp.transpose(dgate).astype(BF)
                dgu_t[second, both] = jnp.transpose(dup).astype(BF)

            @pl.loop(0, width // tile)
            def _(t):
                lanes = pl.ds(pl.multiple_of(t * tile, tile), tile)
                g = nn(hidden_t[...], dy_ref[both, lanes])
                g_acc[:, lanes] = g if slot is gather.me else g_acc[:, lanes] + g

        stores = []

        def store(slot):
            copy = pltpu.make_async_copy(raw.at[slot], xn_all.at[slot], store_sem.at[len(stores)])
            copy.start()
            stores.append(copy)

        load.wait()
        gather.arrived(0)
        gather.own.wait()
        store(gather.me)
        store(gather.mates_slots[0])
        chip(gather.me)
        gather.middle()
        gather.arrived(3)
        store(gather.s_x)
        store(gather.mates_slots[1])
        chip(gather.s_x)
        gather.arrived(4)
        store(gather.s_y)
        store(gather.mates_slots[2])
        chip(gather.s_y)
        gather.corner()
        gather.arrived(6)
        store(gather.s_d)
        store(gather.mates_slots[3])
        chip(gather.s_d)

        @pl.loop(0, width // tile)
        def _(t):
            lanes = pl.ds(pl.multiple_of(t * tile, tile), tile)
            g_down_ref[lanes] = jnp.transpose(g_acc[:, lanes]).astype(BF)

        for copy in gather.copies.values():
            copy.wait_send()
        for copy in stores:
            copy.wait()

    outs = [
        shape((n, rows, width), BF),
        shape((n * rows, units), BF),
        shape((n * rows, 2 * units), BF),
        shape((2 * units, n * rows), BF),
        shape((width, units), BF),
    ]
    scratch = [
        pltpu.VMEM((n, rows, width), BF),
        pltpu.VMEM(dy.shape, BF),
        pltpu.VMEM(gate_up.shape, BF),
        pltpu.VMEM(down.shape, BF),
        pltpu.VMEM((units, 2 * rows), BF),
        pltpu.VMEM((units, width), F32),
        pltpu.SemaphoreType.DMA((3,)),
        pltpu.SemaphoreType.DMA((n,)),
    ]
    ins = [xn, dy, gate_up, down]
    return remote_call(kernel, number, ins, outs, scratch + GATHER_SEMS, any_outs=(0,), any_ins=(1, 2, 3))


def feed_forward_input(dgu, gate_up, h1, cotangent, gain, xn_all, dgu_t, n_ctx, number):
    rows, width = h1.shape
    chunks, unit_rows, _ = gate_up.shape
    units = chunks * unit_rows // 2
    tile, part = 256, 256

    def kernel(
        dgu_ref,
        w_hbm,
        h_ref,
        dy_ref,
        gain_ref,
        xn_hbm,
        dgu_t_hbm,
        dh_ref,
        dhb_ref,
        dgain_ref,
        g_up_ref,
        w_ref,
        xn_ref,
        dgu_t_ref,
        w_sem,
        load_sem,
        *scratch,
    ):
        total = scratch[-1]
        w_load = Load([(w_hbm, w_ref)], w_sem).begin()
        load = Load([(dgu_t_hbm, dgu_t_ref), (xn_hbm, xn_ref)], load_sem).begin()

        def partial(slot, t):
            r = pl.ds(pl.multiple_of(slot * rows, rows), rows)
            lanes = pl.ds(pl.multiple_of(t * tile, tile), tile)
            acc = nn(dgu_ref[r, :unit_rows], w_ref[0, :, lanes])
            for n in range(1, chunks):
                acc = acc + nn(dgu_ref[r, n * unit_rows : (n + 1) * unit_rows], w_ref[n, :, lanes])
            return acc

        def up_gradient(first, last):
            @pl.loop(first, last)
            def _(k):
                r = pl.ds(pl.multiple_of(k * part, part), part)

                @pl.loop(0, width // tile)
                def _(t):
                    lanes = pl.ds(pl.multiple_of(t * tile, tile), tile)
                    g_up_ref[r, lanes] = nn(dgu_t_ref[r], xn_ref[:, lanes]).astype(BF)

        scatter = Scatter(n_ctx, partial, tile, *scratch)
        greet_neighbours(n_ctx)
        w_load.wait()
        scatter.to_mate()
        scatter.pairs()
        load.wait()
        up_gradient(0, units // part)
        scatter.join()
        up_gradient(units // part, 2 * units // part)
        scatter.end()
        dgain_ref[...] = jnp.zeros_like(dgain_ref)

        def finish(r):
            h, d = h_ref[r], total[r]
            scale = inv_rms(h)
            dgain_ref[0:1] += jnp.sum(d * h * scale, 0, keepdims=True)
            dh = dy_ref[r].astype(F32) + norm_back(d, gain_ref[1:2], h, scale)
            dh_ref[r] = dh
            dhb_ref[r] = dh.astype(BF)

        row_chunks(rows, 32, finish)

    outs = [
        shape((rows, width), F32),
        shape((rows, width), BF),
        shape((8, width), F32),
        shape((2 * units, width), BF),
    ]
    scratch = [
        pltpu.VMEM((chunks, unit_rows, width), BF),
        pltpu.VMEM(xn_all.shape, BF),
        pltpu.VMEM(dgu_t.shape, BF),
        pltpu.SemaphoreType.DMA((1,)),
        pltpu.SemaphoreType.DMA((2,)),
    ]
    return remote_call(
        kernel,
        number,
        [dgu, gate_up, h1, cotangent, gain, xn_all, dgu_t],
        outs,
        scratch + scatter_scratch(rows, width),
        any_ins=(1, 5, 6),
    )


def attention_backward(
    dh_all, xn, qkv, attn, lse, cosine, sine, pos_rows, pos_columns, hidden, out_w, down_w, h1, swapped, n_outer, n_ctx, number
):
    rows = dh_all.shape[0]
    own_rows, width = h1.shape
    group = rows // 2
    heads = attn.shape[1] // LANES
    k_at, v_at = heads * LANES, (heads + 1) * LANES
    block = min(QUERY_BLOCK, group)
    features = attn.shape[1]
    tile = 256
    place_rows = width // n_outer // (2 * n_ctx)

    def kernel(
        dh_hbm,
        xn_hbm,
        qkv_hbm,
        attn_hbm,
        lse_ref,
        cos_hbm,
        sin_hbm,
        rows_ref,
        columns_hbm,
        hidden_ref,
        out_w_hbm,
        w_hbm,
        h_ref,
        swap_src,
        dproj_ref,
        result_ref,
        swap_dst,
        g_dst,
        g_qkv_ref,
        xn_ref,
        qkv_ref,
        attn_ref,
        cos_ref,
        sin_ref,
        columns_ref,
        g_ref,
        g_arrived,
        g_sum,
        g_send,
        g_recv,
        dk_ref,
        dv_ref,
        w_ref,
        out_w_ref,
        dh_ref,
        load_sem,
        dh_sem,
        *scratch,
    ):
        swap_sem, g_swap_sem, scratch = scratch[:3], scratch[3:6], scratch[6:]
        total = scratch[-1]
        o = lax.axis_index("o")
        peers = outer_peers(n_outer)
        load = Load([(w_hbm, w_ref)], load_sem).begin()
        pairs = [(out_w_hbm, out_w_ref), (dh_hbm, dh_ref), (attn_hbm, attn_ref), (qkv_hbm, qkv_ref), (cos_hbm, cos_ref), (sin_hbm, sin_ref)]
        dh_load = Load(pairs + [(columns_hbm, columns_ref), (xn_hbm, xn_ref)], dh_sem).begin()
        swap = Swap(n_ctx, [(swap_src, swap_dst)], *swap_sem)
        g_swap = Swap(n_ctx, [(g_sum, g_dst)], *g_swap_sem)

        def partial(slot, t):
            a = hidden_ref[pl.ds(pl.multiple_of(slot * own_rows, own_rows), own_rows)]
            return nt(a, w_ref[pl.ds(pl.multiple_of(t * tile, tile), tile)])

        scatter = Scatter(n_ctx, partial, tile, *scratch)
        greet(swap.devices + peers)

        def back(g, b):
            keys_at = pl.ds(g * group, group)
            r = pl.ds(g * group + b * block, block)
            if b == 0:
                dk_ref[...] = jnp.zeros_like(dk_ref)
                dv_ref[...] = jnp.zeros_like(dv_ref)
            key_pos = columns_ref[keys_at, 0:1]
            ok = (key_pos >= rows_ref[1:2, r]) & (key_pos <= rows_ref[0:1, r])
            da_all = nn(dh_ref[r], out_w_ref[...]).astype(BF)

            for h in range(heads):
                lanes = slice(h * LANES, (h + 1) * LANES)
                da, q = da_all[:, lanes], qkv_ref[r, lanes]
                keys = qkv_ref[keys_at, k_at : k_at + LANES]
                s = nt(keys, q) * SCALE - lse_ref[h : h + 1, r]
                p = jnp.exp(jnp.where(ok, s, MASK_FILL))
                dv_ref[...] += nn(p.astype(BF), da)
                delta = jnp.transpose(da.astype(F32) * attn_ref[r, lanes].astype(F32))
                delta = jnp.sum(delta, 0, keepdims=True)
                dp = nt(qkv_ref[keys_at, v_at : v_at + LANES], da)
                ds = (p * (dp - delta)).astype(BF)
                dk_ref[...] += nn(ds, q)
                dq = tn(ds, keys) * SCALE
                dproj_ref[r, lanes] = rotate(dq, cos_ref[r], -sin_ref[r]).astype(BF)

            if b == group // block - 1:
                dk = rotate(dk_ref[...] * SCALE, cos_ref[keys_at], -sin_ref[keys_at])
                dproj_ref[keys_at, k_at : k_at + LANES] = dk.astype(BF)
                dproj_ref[keys_at, v_at : v_at + LANES] = dv_ref[...].astype(BF)

        def out_gradient():
            @pl.loop(0, width // 384)
            def _(k):
                d = pl.ds(pl.multiple_of(k * 384, 384), 384)
                g_ref[d] = jnp.transpose(tn(attn_ref[...], dh_ref[:, d])).astype(BF)

        def own_place(outer):
            return pl.ds(pl.multiple_of(outer * (width // n_outer), 16), width // n_outer)

        def qkv_gradient():
            half = HEAD_SIZE // 2

            @pl.loop(0, width // 256)
            def _(t):
                lanes = pl.ds(pl.multiple_of(t * 256, 256), 256)
                for h in range(heads + 2):
                    g = tn(dproj_ref[:, h * LANES : (h + 1) * LANES], xn_ref[:, lanes]).astype(BF)
                    for k in range(2):
                        at = h * HEAD_SIZE + k * half
                        g_qkv_ref[at : at + half, lanes] = g[k * LANES // 2 : k * LANES // 2 + half]

        load.wait()
        units = [(g, b) for g in range(2) for b in range(group // block)]
        scatter.to_mate()
        dh_load.wait()
        back(*units[0])
        scatter.pairs()
        swap.begin()
        out_gradient()
        back(*units[1])
        scatter.join()
        g_copies = [
            send(g_ref.at[own_place(device[0])], g_arrived.at[k], g_send.at[k], g_recv.at[k], device)
            for k, device in enumerate(peers)
        ]
        for unit in units[2:]:
            back(*unit)
        for copy in g_copies:
            copy.wait_recv()
        g_total = g_ref[own_place(o)].astype(F32)
        for k in range(n_outer - 1):
            g_total = g_total + g_arrived[k].astype(F32)
        for d in range(2 * n_ctx):
            g_sum[d] = g_total[d * place_rows : (d + 1) * place_rows].astype(BF)
        qkv_gradient()
        g_swap.begin()
        scatter.end()
        swap.end()

        def finish(r):
            result_ref[r] = (h_ref[r] + total[r]).astype(BF)

        row_chunks(own_rows, 32, finish)
        g_swap.end()
        for copy in g_copies:
            copy.wait_send()

    outs = [
        shape(qkv.shape, BF),
        shape((own_rows, width), BF),
        shape(swapped.shape, BF),
        shape((2 * n_ctx, place_rows, features), BF),
        shape((qkv.shape[1] // LANES * HEAD_SIZE, width), BF),
    ]
    ins = [dh_all, xn, qkv, attn, lse, cosine, sine, pos_rows, pos_columns, hidden, out_w, down_w, h1, swapped]
    scratch = [
        pltpu.VMEM(xn.shape, BF),
        pltpu.VMEM(qkv.shape, BF),
        pltpu.VMEM(attn.shape, BF),
        pltpu.VMEM(cosine.shape, F32),
        pltpu.VMEM(sine.shape, F32),
        pltpu.VMEM(pos_columns.shape, jnp.int32),
        pltpu.VMEM((width, features), BF),
        pltpu.VMEM((n_outer - 1, width // n_outer, features), BF),
        pltpu.VMEM((2 * n_ctx, place_rows, features), BF),
        pltpu.SemaphoreType.DMA((n_outer - 1,)),
        pltpu.SemaphoreType.DMA((n_outer - 1,)),
        pltpu.VMEM((group, LANES), F32),
        pltpu.VMEM((group, LANES), F32),
        pltpu.VMEM(down_w.shape, BF),
        pltpu.VMEM(out_w.shape, BF),
        pltpu.VMEM(dh_all.shape, BF),
        pltpu.SemaphoreType.DMA((1,)),
        pltpu.SemaphoreType.DMA((8,)),
    ]
    scratch += swap_sems(1, n_ctx) + swap_sems(1, n_ctx) + scatter_scratch(own_rows, width)
    return remote_call(kernel, number, ins, outs, scratch, any_ins=(0, 1, 2, 3, 5, 6, 8, 10, 11))


def attention_input(dproj, w, tokens, dh1, gain, gain_terms, n_outer, n_ctx, number):
    rows, width = tokens.shape
    tile = 256
    features = dproj.shape[1]
    n = 2 * n_ctx

    def kernel(
        d_ref, w_hbm, x_ref, dh_ref, gain_ref, terms_ref, out_ref, sum_ref, w_ref, load_sem, *scratch
    ):
        swap_sem, scratch = scratch[:3], scratch[3:]
        terms, summed, arrived, send_sem, recv_sem, local_sem = scratch[:6]
        scratch = scratch[6:]
        total = scratch[-1]
        load = Load(padded_loads(w_hbm, w_ref), load_sem).begin()
        o = lax.axis_index("o")

        def partial(slot, t):
            a = d_ref[pl.ds(pl.multiple_of(slot * rows, rows), rows)]
            return nn(a, w_ref[:, pl.ds(pl.multiple_of(t * tile, tile), tile)])

        scatter = Scatter(n_ctx, partial, tile, *scratch)
        swap = Swap(n_ctx, [(terms_ref, terms)], *swap_sem)
        peers = outer_peers(n_outer)
        greet(swap.devices + peers)
        swap.begin()
        load.wait()
        scatter.to_mate()
        scatter.pairs()
        swap.end()
        summed[...] = jnp.sum(terms[...], 0)
        scatter.join()
        copies = []
        for k, device in enumerate(peers):
            copies.append(send(summed.at[device[0]], arrived.at[o], send_sem.at[k], recv_sem.at[k], device))
        own = pltpu.make_async_copy(summed.at[o], arrived.at[o], local_sem)
        own.start()
        scatter.end()

        def finish(r):
            x, d = x_ref[r].astype(F32), total[r]
            out_ref[r] = dh_ref[r] + norm_back(d, gain_ref[0:1], x, inv_rms(x))

        row_chunks(rows, 32, finish)
        for copy in copies:
            copy.wait_recv()
        own.wait()
        sum_ref[...] = jnp.sum(arrived[...], 0)
        for copy in copies:
            copy.wait_send()

    outs = [shape((rows, width), F32), shape((8, LANES), F32)]
    ins = [dproj, w, tokens, dh1, gain, gain_terms]
    n_loads = features // (LANES // 2)
    scratch = [pltpu.VMEM((features, width), BF), pltpu.SemaphoreType.DMA((n_loads,))]
    scratch += swap_sems(1, n_ctx)
    scratch += [
        pltpu.VMEM((n, n_outer, 8, LANES), F32),
        pltpu.VMEM((n_outer, 8, LANES), F32),
        pltpu.VMEM((n_outer, 8, LANES), F32),
        pltpu.SemaphoreType.DMA((n_outer - 1,)),
        pltpu.SemaphoreType.DMA((n_outer - 1,)),
        pltpu.SemaphoreType.DMA,
    ]
    scratch += scatter_scratch(rows, width)
    return remote_call(kernel, number, ins, outs, scratch, any_ins=(1,))


def make_shards(n_outer, n_inner, n_ctx):
    n_plane = n_inner * n_ctx
    moves = feature_moves(n_outer, n_plane)
    back = [(b, a) for a, b in moves]

    def layer(tokens, norm_attn, w_qkv, w_out, norm_mlp, w_gate_up, w_down, cotangent, seq_lengths, block_slot):
        _, width = tokens.shape
        gain_rows = norm_attn.shape[0]
        out_rows = w_out.shape[0]
        unit_rows = w_gate_up.shape[0]
        n_seqs, n_slots = seq_lengths.shape[1], block_slot.shape[1]
        units = FF // n_plane
        qkv_w = z_ag(lax.ppermute(w_qkv, ALL, moves)).reshape(CHUNKS, -1, width)
        gain_part = jnp.pad(jnp.stack([norm_attn, norm_mlp]), ((0, 6), (0, LANES - gain_rows)))
        meta = jnp.concatenate([seq_lengths[0], block_slot[0]])
        meta = jnp.pad(meta[None], ((0, 7), (0, LANES - n_seqs - n_slots)))
        out_parts = pad_heads(w_out, 1).reshape(out_rows, 2, n_plane // 2, -1).transpose(2, 1, 0, 3)
        out_parts = out_parts.reshape(n_plane, out_rows, -1)
        down_parts = w_down.reshape(out_rows, n_outer // 2, n_plane, unit_rows).transpose(2, 0, 1, 3)
        down_parts = down_parts.reshape(n_plane, out_rows, units)
        w_gate_up, out_parts, down_parts = lax.optimization_barrier((w_gate_up, out_parts, down_parts))
        gate_up = z_ag(w_gate_up)
        gate_up = gate_up.reshape(CHUNKS, -1, width)
        x_all, out_parts, down_w, gains, cosine, sine, pos_rows, pos_columns = prologue(
            tokens, out_parts, down_parts, gain_part, meta, n_seqs, n_outer, n_ctx, 1
        )
        x_all = x_all.reshape(-1, width)
        gains = gains[:, :, :2, :gain_rows].transpose(2, 0, 1, 3).reshape(2, width)
        down_w = z_ag(down_w.reshape(-1, units))
        qkv, attn, lse, dy_all, xn1, out_w = attention_forward(
            x_all, gains, qkv_w, cosine, sine, pos_rows, pos_columns, cotangent, out_parts, n_outer, n_ctx, 2
        )
        out_w = out_w.reshape(width, -1)
        h1, xn2 = output_projection(attn, out_w, tokens, gains, n_ctx, 3)
        xn2_all, hidden, dgu, dgu_t, g_down = feed_forward(xn2, dy_all, gate_up, down_w, n_ctx, 4)
        dgu, g_down = lax.optimization_barrier((dgu, g_down))
        g_down = z_rs(g_down)
        dh1, dh1_bf, dgain_two, g_gate_up = feed_forward_input(
            dgu, gate_up, h1, cotangent, gains, xn2_all.reshape(-1, width), dgu_t, n_ctx, 5
        )
        g_gate_up = z_rs(g_gate_up)
        dh1_all = plane_gather(dh1_bf, n_ctx, 6)
        dh1_all, g_down = lax.optimization_barrier((dh1_all, g_down))
        g_down = g_down.reshape(n_plane, out_rows, units)
        dproj, result, g_down, g_out, g_qkv = attention_backward(
            dh1_all, xn1, qkv, attn, lse, cosine, sine, pos_rows, pos_columns, hidden, out_w, down_w, h1, g_down, n_outer, n_ctx, 7
        )
        terms = jnp.sum(qkv_w.reshape(-1, width).astype(F32) * g_qkv.astype(F32), 0) / gains[0]
        terms = jnp.stack([terms, dgain_two[0]]).reshape(2, n_outer, n_plane, gain_rows).transpose(2, 1, 0, 3)
        terms = jnp.pad(terms, ((0, 0), (0, 0), (0, 6), (0, LANES - gain_rows)))
        dproj, g_qkv, g_gate_up = lax.optimization_barrier((dproj, g_qkv, g_gate_up))
        g_qkv = z_rs(g_qkv)
        grad_input, g = attention_input(dproj, qkv_w, tokens, dh1, gains, terms, n_outer, n_ctx, 8)
        grad_input, g_qkv = lax.optimization_barrier((grad_input, g_qkv))
        grad_qkv = lax.ppermute(g_qkv, ALL, back).astype(F32)
        g_out = g_out.reshape(n_plane // 2, 2, out_rows, -1).transpose(2, 1, 0, 3)
        grad_out = cut_heads(g_out.reshape(out_rows, -1), 1).astype(F32)
        grad_down = g_down.reshape(n_plane, out_rows, n_outer // 2, unit_rows).transpose(1, 2, 0, 3)
        grad_down = grad_down.reshape(out_rows, -1).astype(F32)
        g = g[:, :gain_rows]
        return (result, grad_input, g[0], grad_qkv, grad_out, g[1], g_gate_up.astype(F32), grad_down)

    return layer


def solution(mesh):
    n_inner = 2
    n_ctx = mesh.shape["ctx"]
    n_outer = mesh.shape["dp"] // n_inner
    split = Mesh(mesh.devices.reshape(n_outer, n_inner, n_ctx), ALL)
    rows, vec, grp = P(ALL, None), P(ALL), P(("o", "i"), None)
    return jax.shard_map(
        make_shards(n_outer, n_inner, n_ctx),
        mesh=split,
        in_specs=(rows, vec, rows, rows, vec, rows, rows, rows, grp, grp),
        out_specs=(rows, rows, vec, rows, rows, vec, rows, rows),
        check_vma=False,
    )
```

```python
import math

import jax
import jax.numpy as jnp
import numpy as np
from jax import lax
from jax.experimental import pallas as pl
from jax.experimental.pallas import tpu as pltpu
from jax.sharding import Mesh
from jax.sharding import PartitionSpec as P


QUERY_HEADS = 16
HEAD_SIZE = 96
FF = 4096
BLK = 128
LANES = 128
QUERY_BLOCK = 512
CHUNKS = 4

EPSILON = 1e-05
THETA = 100000.0
MASK_FILL = -1e30
BF = jnp.bfloat16
F32 = jnp.float32
ALL = ("o", "i", "ctx")
MESH = pl.DeviceIdType.MESH
SCALE = 1.0 / math.sqrt(HEAD_SIZE)


def nt(a, b):
    return lax.dot_general(a, b, (((1,), (1,)), ((), ())), preferred_element_type=F32)


def nn(a, b):
    return lax.dot_general(a, b, (((1,), (0,)), ((), ())), preferred_element_type=F32)


def tn(a, b):
    return lax.dot_general(a, b, (((0,), (0,)), ((), ())), preferred_element_type=F32)


def z_ag(x):
    return lax.all_gather(x, "o", axis=0, tiled=True)


def z_rs(x):
    return lax.psum_scatter(x, "o", scatter_dimension=0, tiled=True)


def inv_rms(x):
    return lax.rsqrt(jnp.mean(x * x, -1, keepdims=True) + EPSILON)


def norm_back(grad_normed, gain, source, scale):
    weighted = grad_normed * gain
    return scale * weighted - source * scale**3 * jnp.mean(weighted * source, -1, keepdims=True)


def feature_moves(n_outer, n_plane):
    moves = []
    half, quarter = n_outer // 2, n_outer // 4
    for block in range(n_outer * n_plane):
        if block < 4 * n_outer:
            head, step = block // half, block % half
        elif block < 6 * n_outer:
            head, step = divmod(block - 4 * n_outer, quarter)
            step += half
        else:
            head, step = divmod(block - 6 * n_outer, quarter)
            step += half + quarter
        place = 2 * (head % (n_plane // 2)) + head // (n_plane // 2)
        moves.append((block, step * n_plane + place))
    return moves


def pad_heads(x, axis):
    half = HEAD_SIZE // 2
    shape = x.shape
    x = x.reshape(shape[:axis] + (-1, half) + shape[axis + 1 :])
    pads = [(0, 0)] * x.ndim
    pads[axis + 1] = (0, LANES // 2 - half)
    return jnp.pad(x, pads).reshape(shape[:axis] + (-1,) + shape[axis + 1 :])


def cut_heads(x, axis):
    half = HEAD_SIZE // 2
    shape = x.shape
    x = x.reshape(shape[:axis] + (-1, LANES // 2) + shape[axis + 1 :])
    x = lax.slice_in_dim(x, 0, half, axis=axis + 1)
    return x.reshape(shape[:axis] + (-1,) + shape[axis + 1 :])


def places(n_ctx):
    o, i, c = lax.axis_index("o"), lax.axis_index("i"), lax.axis_index("ctx")
    return o, i, c, c + 1 - 2 * (c % 2), (c + n_ctx // 2) % n_ctx


def greet(devices):
    barrier = pltpu.get_barrier_semaphore()
    for device in devices:
        pl.semaphore_signal(barrier, inc=1, device_id=device, device_id_type=MESH)
    pl.semaphore_wait(barrier, len(devices))


def greet_neighbours(n_ctx):
    o, i, c, mate, far = places(n_ctx)
    greet([(o, i, mate), (o, 1 - i, c), (o, i, far)])


def send(src, dst, send_sem, recv_sem, device):
    copy = pltpu.make_async_remote_copy(
        src_ref=src, dst_ref=dst, send_sem=send_sem, recv_sem=recv_sem, device_id=device, device_id_type=MESH
    )
    copy.start()
    return copy


class Gather:
    def __init__(self, n_ctx, src, out, send_sem, recv_sem, local_sem):
        self.src, self.out, self.sems = src, out, (send_sem, recv_sem, local_sem)
        o, i, c, mate, far = places(n_ctx)
        j, core = 1 - i, c % 2
        self.mate, self.x, self.y = (o, i, mate), (o, j, c), (o, i, far)
        self.me, self.s_x = i * n_ctx + c, j * n_ctx + c
        self.s_y, self.s_d = i * n_ctx + far, j * n_ctx + far
        self.relay = (o, j * core + i * (1 - core), c * core + far * (1 - core))
        self.relayed = self.s_y * core + self.s_x * (1 - core)
        mate_far = (mate + n_ctx // 2) % n_ctx
        self.mates_slots = [i * n_ctx + mate, j * n_ctx + mate, i * n_ctx + mate_far, j * n_ctx + mate_far]
        self.copies = {}

    def go(self, kind, part, src, slot, device):
        rows = src.shape[0] // PARTS
        at = pl.ds(part * rows, rows)
        copy = send(src.at[at], self.out.at[slot, at], self.sems[0].at[kind, part], self.sems[1].at[kind, part], device)
        self.copies[kind, part] = copy

    def begin(self):
        for part in range(PARTS):
            self.go(1, part, self.src, self.me, self.x)
            self.go(2, part, self.src, self.me, self.y)
        for part in range(PARTS):
            self.go(0, part, self.src, self.me, self.mate)
        self.own = pltpu.make_async_copy(self.src, self.out.at[self.me], self.sems[2])
        self.own.start()

    def middle(self):
        for part in range(PARTS):
            self.copies[1, part].wait_recv()
            self.copies[2, part].wait_recv()
            self.go(5, part, self.out.at[self.relayed], self.relayed, self.relay)
            self.go(3, part, self.out.at[self.s_x], self.s_x, self.mate)
            self.go(4, part, self.out.at[self.s_y], self.s_y, self.mate)

    def corner(self):
        for part in range(PARTS):
            self.copies[5, part].wait_recv()
            self.go(6, part, self.out.at[self.s_d], self.s_d, self.mate)

    def arrived(self, kind):
        for part in range(PARTS):
            self.copies[kind, part].wait_recv()

    def sent(self):
        self.own.wait()
        for copy in self.copies.values():
            copy.wait_send()

    def end(self):
        self.corner()
        for kind in (0, 3, 4, 6):
            self.arrived(kind)
        self.sent()


PARTS = 2
GATHER_SEMS = [pltpu.SemaphoreType.DMA((7, PARTS)), pltpu.SemaphoreType.DMA((7, PARTS)), pltpu.SemaphoreType.DMA]


class Scatter:
    def __init__(self, n_ctx, partial, tile, ready, from_mate, going, got, send_sem, recv_sem, total):
        self.partial, self.tile = partial, tile
        self.ready, self.from_mate, self.going, self.got = ready, from_mate, going, got
        self.sems, self.total = (send_sem, recv_sem), total
        o, i, c, mate, far = places(n_ctx)
        j, core = 1 - i, c % 2
        self.core = core
        far_mate = (mate + n_ctx // 2) % n_ctx
        self.mine = [j * n_ctx + far, j * n_ctx + c, i * n_ctx + far, i * n_ctx + c]
        self.theirs = [j * n_ctx + far_mate, j * n_ctx + mate, i * n_ctx + far_mate, i * n_ctx + mate]
        self.mate = (o, i, mate)
        self.combined = (o, j * (1 - core) + i * core, c * (1 - core) + far * core)
        self.direct = (o, j * core + i * (1 - core), c * core + far * (1 - core))
        self.s_direct = self.mine[2] * (1 - core) + self.mine[1] * core
        self.s_combined = self.mine[1] * (1 - core) + self.mine[2] * core
        self.copies = []

    def go(self, kind, part, src, dst, device):
        copy = send(src.at[part], dst.at[part], self.sems[0].at[kind, part], self.sems[1].at[kind, part], device)
        self.copies.append(copy)
        return copy

    def each(self, part, body):
        tiles = self.ready.shape[-1] // self.tile

        @pl.loop(0, tiles)
        def _(t):
            at = pl.multiple_of(t * self.tile, self.tile)
            body(part * tiles + t, pl.ds(at, self.tile), pl.ds(part * tiles * self.tile + at, self.tile))

    def fill(self, n, part):
        def body(t, lanes, _):
            self.ready[n, part, :, lanes] = self.partial(self.theirs[n], t).astype(BF)

        self.each(part, body)

    def give(self, n, part):
        self.mates[n, part] = self.go(n, part, self.ready.at[n], self.from_mate.at[n], self.mate)

    def pair(self, slot, n, part, place):
        def body(t, lanes, _):
            pair = self.partial(slot, t) + self.from_mate[n, part, :, lanes].astype(F32)
            self.going[place, part, :, lanes] = pair.astype(BF)

        self.each(part, body)

    def to_mate(self):
        self.mates, self.straights, self.diagonals, self.joins = {}, [], [], []
        order = [(0, 0), (0, 1), (1, 0), (2, 0), (1, 1), (2, 1), (3, 0), (3, 1)]
        self.fill(*order[0])
        for k, at in enumerate(order[1:]):
            self.fill(*at)
            self.give(*order[k])
            if k == 2:
                self.mates[0, 0].wait_recv()
                self.pair(self.mine[0], 0, 0, 0)
            if k == 3:
                self.diagonals.append(self.go(4, 0, self.going.at[0], self.got.at[0], self.direct))
                self.mates[0, 1].wait_recv()
                self.pair(self.mine[0], 0, 1, 0)
            if k == 4:
                self.diagonals.append(self.go(4, 1, self.going.at[0], self.got.at[0], self.direct))
        self.last = order[-1]

    def pairs(self):
        for part in range(PARTS):
            self.mates[1, part].wait_recv()
            self.mates[2, part].wait_recv()
            self.pair(self.s_direct, 2 - self.core, part, 1)
            if part == 0:
                self.give(*self.last)
            else:
                self.straights.append(self.go(5, part - 1, self.going.at[1], self.got.at[1], self.direct))

    def join(self):
        for part in range(PARTS):
            self.diagonals[part].wait_recv()
            if part == 0:
                self.straights.append(self.go(5, PARTS - 1, self.going.at[1], self.got.at[1], self.direct))

            def combined(t, lanes, _):
                pair = self.partial(self.s_combined, t) + self.from_mate[1 + self.core, part, :, lanes].astype(F32)
                self.going[2, part, :, lanes] = (pair + self.got[0, part, :, lanes].astype(F32)).astype(BF)

            self.each(part, combined)
            if part:
                self.joins.append(self.go(6, part - 1, self.going.at[2], self.got.at[2], self.combined))
        self.own(0)
        self.joins.append(self.go(6, PARTS - 1, self.going.at[2], self.got.at[2], self.combined))

    def own(self, part):
        self.mates[3, part].wait_recv()

        def body(t, lanes, out):
            self.total[:, out] = self.partial(self.mine[3], t) + self.from_mate[3, part, :, lanes].astype(F32)

        self.each(part, body)

    def end(self):
        total = self.total
        for part in range(1, PARTS):
            self.own(part)
        for part in range(PARTS):
            self.straights[part].wait_recv()
            self.joins[part].wait_recv()

            def rest(t, lanes, out):
                other = self.got[1, part, :, lanes].astype(F32) + self.got[2, part, :, lanes].astype(F32)
                total[:, out] = total[:, out] + other

            self.each(part, rest)
        for copy in self.copies:
            copy.wait_send()


def scatter_scratch(rows, width):
    return [
        pltpu.VMEM((4, PARTS, rows, width // PARTS), BF),
        pltpu.VMEM((4, PARTS, rows, width // PARTS), BF),
        pltpu.VMEM((3, PARTS, rows, width // PARTS), BF),
        pltpu.VMEM((3, PARTS, rows, width // PARTS), BF),
        pltpu.SemaphoreType.DMA((7, PARTS)),
        pltpu.SemaphoreType.DMA((7, PARTS)),
        pltpu.VMEM((rows, width), F32),
    ]


def row_chunks(rows, step, body):
    @pl.loop(0, rows // step)
    def _(r):
        body(pl.ds(pl.multiple_of(r * step, step), step))


class Load:
    def __init__(self, parts, sem):
        self.copies = [pltpu.make_async_copy(src, dst, sem.at[n]) for n, (src, dst) in enumerate(parts)]

    def begin(self):
        for copy in self.copies:
            copy.start()
        return self

    def wait(self):
        for copy in self.copies:
            copy.wait()


IN_VMEM = pl.BlockSpec(memory_space=pltpu.VMEM)
ANYWHERE = pl.BlockSpec(memory_space=pl.ANY)


def remote_call(kernel, number, ins, outs, scratch, any_outs=(), any_ins=()):
    return pl.pallas_call(
        kernel,
        out_shape=outs,
        in_specs=[ANYWHERE if n in any_ins else IN_VMEM for n in range(len(ins))],
        out_specs=[ANYWHERE if n in any_outs else IN_VMEM for n in range(len(outs))],
        scratch_shapes=scratch,
        compiler_params=pltpu.CompilerParams(collective_id=number, has_side_effects=True, vmem_limit_bytes=60 << 20),
    )(*ins)


def shape(dims, dtype):
    return jax.ShapeDtypeStruct(tuple(dims), dtype)


class Swap:
    def __init__(self, n_ctx, pairs, send_sem, recv_sem, local_sem):
        self.pairs, self.sems = pairs, (send_sem, recv_sem, local_sem)
        self.o, i, c, _, _ = places(n_ctx)
        self.n, self.n_ctx = 2 * n_ctx, n_ctx
        self.me = i * n_ctx + c
        self.others = [(self.me + k) % self.n for k in range(1, self.n)]
        self.devices = [(self.o, d // n_ctx, d % n_ctx) for d in self.others]

    def begin(self):
        self.copies, self.own = [], []
        for a, (src, dst) in enumerate(self.pairs):
            for k, (d, device) in enumerate(zip(self.others, self.devices)):
                self.copies.append(
                    send(src.at[d], dst.at[self.me], self.sems[0].at[a, k], self.sems[1].at[a, k], device)
                )
            own = pltpu.make_async_copy(src.at[self.me], dst.at[self.me], self.sems[2].at[a])
            own.start()
            self.own.append(own)

    def end(self):
        for copy in self.copies:
            copy.wait_recv()
            copy.wait_send()
        for copy in self.own:
            copy.wait()


def swap_sems(n_arrays, n_ctx):
    return [
        pltpu.SemaphoreType.DMA((n_arrays, 2 * n_ctx - 1)),
        pltpu.SemaphoreType.DMA((n_arrays, 2 * n_ctx - 1)),
        pltpu.SemaphoreType.DMA((n_arrays,)),
    ]


def outer_peers(n_outer):
    o, i, c = lax.axis_index("o"), lax.axis_index("i"), lax.axis_index("ctx")
    return [(lax.rem(o + k, n_outer), i, c) for k in range(1, n_outer)]


def rotary_constants():
    frequency = THETA ** -(np.arange(HEAD_SIZE // 2) * (2.0 / HEAD_SIZE))
    rates = np.zeros((8, LANES), np.float32)
    for half, sign in ((0, -1.0), (LANES // 2, 1.0)):
        rates[0, half : half + HEAD_SIZE // 2] = frequency
        rates[1, half : half + HEAD_SIZE // 2] = sign
    angles = np.arange(BLK)[:, None] * rates[0].astype(np.float64)
    return rates, np.stack([np.cos(angles), np.sin(angles)]).astype(np.float32)


def prologue(tokens, out_parts, down_parts, gains, meta, n_seqs, n_outer, n_ctx, number):
    rows, width = tokens.shape
    n = 2 * n_ctx
    blocks = n_ctx * rows // BLK

    def kernel(
        x_ref,
        out_src,
        down_src,
        gains_ref,
        meta_ref,
        rates_ref,
        angles_ref,
        x_all,
        out_dst,
        down_dst,
        gains_out,
        cos_ref,
        sin_ref,
        rows_ref,
        columns_ref,
        *sems,
    ):
        o = lax.axis_index("o")
        metas_ref, send_sem, recv_sem, local_sem = sems[:4]
        out_swap = Swap(n_ctx, [(out_src, out_dst)], *sems[4:7])
        down_swap = Swap(n_ctx, [(down_src, down_dst)], *sems[7:10])
        gather = Gather(n_ctx, x_ref, x_all, *sems[10:])
        peers = outer_peers(n_outer)
        me = out_swap.me
        greet(out_swap.devices + peers)
        gather.begin()
        own = [
            pltpu.make_async_copy(meta_ref, metas_ref.at[me], local_sem.at[0]),
            pltpu.make_async_copy(gains_ref, gains_out.at[o, me], local_sem.at[1]),
        ]
        meta_copies, gain_copies, z_copies = [], [], []
        for copy in own:
            copy.start()
        for k, device in enumerate(out_swap.devices):
            meta_copies.append(send(meta_ref, metas_ref.at[me], send_sem.at[0, k], recv_sem.at[0, k], device))
            gain_copies.append(send(gains_ref, gains_out.at[o, me], send_sem.at[1, k], recv_sem.at[1, k], device))
        out_swap.begin()
        for copy in own:
            copy.wait()
        for copy in meta_copies:
            copy.wait_recv()
        lane = lax.broadcasted_iota(jnp.int32, (BLK, LANES), 1)
        row = lax.broadcasted_iota(jnp.int32, (BLK, LANES), 0)
        rows_ref[...] = jnp.zeros_like(rows_ref)
        pieces = 2 * blocks * n_seqs
        piece = lax.broadcasted_iota(jnp.int32, (pieces, LANES), 0)
        bases = jnp.zeros((pieces, LANES), jnp.int32)
        places_of = []
        for g in range(2):
            starts, end = [], jnp.zeros((1, 1), jnp.int32)
            for q in range(n_seqs):
                starts.append(end)
                end = end + metas_ref[g * n_ctx, 0:1, q : q + 1]
            for b in range(blocks):
                first = metas_ref[g * n_ctx, 0:1, n_seqs + b : n_seqs + b + 1] * BLK
                for q in range(n_seqs):
                    index = (g * blocks + b) * n_seqs + q
                    bases = jnp.where(piece == index, first - starts[q], bases)
                places_of.append((first, starts))
        angle = bases.astype(F32) * rates_ref[0:1]
        base_cos, base_sin = jnp.cos(angle), jnp.sin(angle)
        for n_block, (first, starts) in enumerate(places_of):
            at = slice(n_block * BLK, (n_block + 1) * BLK)
            stream, lanes_stream = first + row, first + lane[0:1]
            start, lanes_start = jnp.zeros_like(stream), jnp.zeros_like(lanes_stream)
            cos, sin = angles_ref[0], angles_ref[1]
            for q in range(n_seqs):
                index = n_block * n_seqs + q
                cos_0, sin_0 = base_cos[index : index + 1], base_sin[index : index + 1]
                cos_q = cos_0 * angles_ref[0] - sin_0 * angles_ref[1]
                sin_q = sin_0 * angles_ref[0] + cos_0 * angles_ref[1]
                inside = stream >= starts[q]
                start = jnp.where(inside, starts[q], start)
                lanes_start = jnp.where(lanes_stream >= starts[q], starts[q], lanes_start)
                cos, sin = jnp.where(inside, cos_q, cos), jnp.where(inside, sin_q, sin)
            cos_ref[at] = cos
            sin_ref[at] = sin * rates_ref[1:2]
            columns_ref[at] = jnp.where(lane == 0, stream, start)
            rows_ref[0:1, at] = lanes_stream
            rows_ref[1:2, at] = lanes_start
        for copy in gain_copies:
            copy.wait_recv()
        for k, device in enumerate(peers):
            z_copies.append(send(gains_out.at[o], gains_out.at[o], send_sem.at[2, k], recv_sem.at[2, k], device))
        gather.middle()
        down_swap.begin()
        gather.end()
        out_swap.end()
        down_swap.end()
        for copy in z_copies:
            copy.wait_recv()
        for copy in meta_copies + gain_copies + z_copies:
            copy.wait_send()

    outs = [
        shape((n, rows, width), BF),
        shape(out_parts.shape, BF),
        shape(down_parts.shape, BF),
        shape((n_outer, n) + gains.shape, F32),
        shape((n * rows, LANES), F32),
        shape((n * rows, LANES), F32),
        shape((8, n * rows), jnp.int32),
        shape((n * rows, LANES), jnp.int32),
    ]
    rates, angles = rotary_constants()
    ins = [tokens, out_parts, down_parts, gains, meta, jnp.asarray(rates), jnp.asarray(angles)]
    most = max(n, n_outer) - 1
    scratch = [
        pltpu.VMEM((n,) + meta.shape, jnp.int32),
        pltpu.SemaphoreType.DMA((3, most)),
        pltpu.SemaphoreType.DMA((3, most)),
        pltpu.SemaphoreType.DMA((2,)),
    ]
    scratch += swap_sems(1, n_ctx) + swap_sems(1, n_ctx) + GATHER_SEMS
    return remote_call(kernel, number, ins, outs, scratch, any_outs=(0,))


def plane_gather(x, n_ctx, number):
    def kernel(src, out, *sems):
        gather = Gather(n_ctx, src, out, *sems)
        greet_neighbours(n_ctx)
        gather.begin()
        gather.middle()
        gather.end()

    outs = [shape((2 * n_ctx,) + x.shape, x.dtype)]
    got = remote_call(kernel, number, [x], outs, GATHER_SEMS, any_outs=(0,))
    return got[0].reshape(-1, x.shape[-1])


def rotate(x, cosine, sine):
    return x * cosine + pltpu.roll(x, LANES // 2, 1) * sine


def qkv_rows(features):
    return features // LANES * HEAD_SIZE // CHUNKS


def padded_loads(w_ref, w_pad):
    half = HEAD_SIZE // 2
    rows = qkv_rows(w_pad.shape[0])
    pairs, at = [], 0
    for row in range(half, w_pad.shape[0], LANES // 2):
        w_pad[row : row + LANES // 2 - half] = jnp.zeros((LANES // 2 - half, w_pad.shape[1]), BF)
    for n in range(w_ref.shape[0]):
        for b in range(rows // half):
            src = w_ref.at[n, pl.ds(b * half, half)]
            pairs.append((src, w_pad.at[pl.ds(at * LANES // 2, half)]))
            at += 1
    return pairs


def attention_forward(x_all, gains, w, cosine, sine, pos_rows, pos_columns, dy, out_part, n_outer, n_ctx, number):
    rows, width = x_all.shape
    group = rows // 2
    heads = QUERY_HEADS // (2 * n_ctx)
    features = (heads + 2) * LANES
    k_at, v_at = heads * LANES, (heads + 1) * LANES
    block = min(QUERY_BLOCK, group)
    n_loads = features // (LANES // 2)

    def kernel(
        x_hbm,
        gain_ref,
        w_hbm,
        cos_ref,
        sin_ref,
        rows_ref,
        columns_ref,
        dy_ref,
        part_ref,
        qkv_ref,
        attn_ref,
        lse_ref,
        dy_all,
        xn_out,
        out_w,
        w_ref,
        xn_ref,
        load_sem,
        xn_sem,
        store_sem,
        z_send,
        z_recv,
        z_local,
        *sems,
    ):
        gather = Gather(n_ctx, dy_ref, dy_all, *sems)
        load = Load(padded_loads(w_hbm, w_ref), load_sem).begin()
        xn_load = Load([(x_hbm, xn_ref)], xn_sem).begin()
        o = lax.axis_index("o")
        peers = outer_peers(n_outer)
        greet([gather.mate, gather.x, gather.y] + peers)
        gather.begin()
        z_copies = [send(part_ref, out_w.at[o], z_send.at[k], z_recv.at[k], device) for k, device in enumerate(peers)]
        own_part = pltpu.make_async_copy(part_ref, out_w.at[o], z_local)
        own_part.start()
        load.wait()
        xn_load.wait()

        def normalise(r):
            x = xn_ref[r].astype(F32)
            xn_ref[r] = (x * inv_rms(x) * gain_ref[0:1]).astype(BF)

        def project(r):
            cos, sin = cos_ref[r], sin_ref[r]
            for h in range(heads + 2):
                lanes = slice(h * LANES, (h + 1) * LANES)
                part = nt(xn_ref[r], w_ref[lanes])
                qkv_ref[r, lanes] = (rotate(part, cos, sin) if h <= heads else part).astype(BF)

        def attend(g):
            keys_at = pl.ds(g * group, group)

            @pl.loop(0, group // block)
            def _(b):
                r = pl.ds(pl.multiple_of(g * group + b * block, block), block)
                key_pos = rows_ref[0:1, keys_at]
                ok = (key_pos >= columns_ref[r, 1:2]) & (key_pos <= columns_ref[r, 0:1])
                for h in range(heads):
                    lanes = slice(h * LANES, (h + 1) * LANES)
                    s = nt(qkv_ref[r, lanes], qkv_ref[keys_at, k_at : k_at + LANES])
                    s = jnp.where(ok, s, MASK_FILL)
                    high = jnp.max(s, -1, keepdims=True)
                    e = jnp.exp((s - high) * SCALE)
                    total = jnp.sum(e, -1, keepdims=True)
                    mixed = nn(e.astype(BF), qkv_ref[keys_at, v_at : v_at + LANES])
                    attn_ref[r, lanes] = (mixed / total).astype(BF)
                    lse = jnp.broadcast_to(high * SCALE + jnp.log(total), (block, LANES))
                    lse_ref[h : h + 1, r] = jnp.transpose(lse)[0:1]

        row_chunks(rows, 64, normalise)
        row_chunks(rows, block, project)
        gather.middle()
        store = Load([(xn_ref, xn_out)], store_sem).begin()
        attend(0)
        attend(1)
        gather.end()
        store.wait()
        own_part.wait()
        for copy in z_copies:
            copy.wait_recv()
            copy.wait_send()

    outs = [
        shape((rows, features), BF),
        shape((rows, heads * LANES), BF),
        shape((8, rows), F32),
        shape((2 * n_ctx,) + dy.shape, BF),
        shape(x_all.shape, BF),
        shape((n_outer,) + out_part.shape, BF),
    ]
    ins = [x_all, gains, w, cosine, sine, pos_rows, pos_columns, dy, out_part]
    scratch = [
        pltpu.VMEM((features, width), BF),
        pltpu.VMEM(x_all.shape, BF),
        pltpu.SemaphoreType.DMA((n_loads,)),
        pltpu.SemaphoreType.DMA((1,)),
        pltpu.SemaphoreType.DMA((1,)),
        pltpu.SemaphoreType.DMA((n_outer - 1,)),
        pltpu.SemaphoreType.DMA((n_outer - 1,)),
        pltpu.SemaphoreType.DMA,
    ]
    scratch += GATHER_SEMS
    got = remote_call(kernel, number, ins, outs, scratch, any_outs=(3, 4), any_ins=(0, 2))
    return got[0], got[1], got[2], got[3].reshape(rows, width), got[4], got[5]


def output_projection(attn, out_w, tokens, gain, n_ctx, number):
    rows, width = tokens.shape
    tile = 256


    def kernel(attn_ref, w_ref, x_ref, gain_ref, h_ref, xn_ref, *scratch):
        total = scratch[-1]

        def partial(slot, t):
            a = attn_ref[pl.ds(pl.multiple_of(slot * rows, rows), rows)]
            return nt(a, w_ref[pl.ds(pl.multiple_of(t * tile, tile), tile)])

        scatter = Scatter(n_ctx, partial, tile, *scratch)
        greet_neighbours(n_ctx)
        scatter.to_mate()
        scatter.pairs()
        scatter.join()
        scatter.end()

        def finish(r):
            h = x_ref[r].astype(F32) + total[r]
            h_ref[r] = h
            xn_ref[r] = (h * inv_rms(h) * gain_ref[1:2]).astype(BF)

        row_chunks(rows, 32, finish)

    outs = [shape((rows, width), F32), shape((rows, width), BF)]
    return remote_call(kernel, number, [attn, out_w, tokens, gain], outs, scatter_scratch(rows, width))


def feed_forward(xn, dy, gate_up, down, n_ctx, number):
    rows, width = xn.shape
    n = 2 * n_ctx
    chunks, unit_rows, _ = gate_up.shape
    units = down.shape[1]
    tile = 256

    def kernel(
        x_ref,
        dy_hbm,
        up_hbm,
        down_hbm,
        xn_all,
        hidden_out,
        dgu_out,
        dgu_t_out,
        g_down_ref,
        hidden_ref,
        dgu_ref,
        dgu_t,
        out_sem,
        raw,
        dy_ref,
        up_ref,
        down_ref,
        hidden_t,
        g_acc,
        load_sem,
        store_sem,
        *sems,
    ):
        gather = Gather(n_ctx, x_ref, raw, *sems)
        pairs = [(up_hbm, up_ref), (down_hbm, down_ref), (dy_hbm, dy_ref)]
        load = Load(pairs, load_sem).begin()
        greet_neighbours(n_ctx)
        gather.begin()
        half = chunks // 2
        core = gather.me % 2

        def chip(slot):
            both = pl.ds(pl.multiple_of((slot - core) * rows, 2 * rows), 2 * rows)
            x = raw[pl.ds(slot - core, 2)].reshape(2 * rows, width)
            for m in range(half):
                lanes = slice(m * unit_rows, (m + 1) * unit_rows)
                second = slice(units + m * unit_rows, units + (m + 1) * unit_rows)
                gate = nt(x, up_ref[m])
                up = nt(x, up_ref[half + m])
                dhid = nn(dy_ref[both], down_ref[:, lanes])
                sg = 1.0 / (1.0 + jnp.exp(-gate))
                act = gate * sg
                hidden = act * up
                dgate = dhid * up * sg * (1.0 + gate * (1.0 - sg))
                dup = dhid * act
                hidden_ref[both, lanes] = hidden.astype(BF)
                dgu_ref[both, lanes] = dgate.astype(BF)
                dgu_ref[both, second] = dup.astype(BF)
                hidden_t[lanes] = jnp.transpose(hidden).astype(BF)
                dgu_t[lanes, both] = jnp.transpose(dgate).astype(BF)
                dgu_t[second, both] = jnp.transpose(dup).astype(BF)

            @pl.loop(0, width // tile)
            def _(t):
                lanes = pl.ds(pl.multiple_of(t * tile, tile), tile)
                g = nn(hidden_t[...], dy_ref[both, lanes])
                g_acc[:, lanes] = g if slot is gather.me else g_acc[:, lanes] + g

        stores = []

        def store(slot):
            copy = pltpu.make_async_copy(raw.at[slot], xn_all.at[slot], store_sem.at[len(stores)])
            copy.start()
            stores.append(copy)

        flushes = []

        def flush(slot):
            both = pl.ds(pl.multiple_of((slot - core) * rows, 2 * rows), 2 * rows)
            pairs = [(hidden_ref.at[both], hidden_out.at[both]), (dgu_ref.at[both], dgu_out.at[both])]
            pairs.append((dgu_t.at[:, both], dgu_t_out.at[:, both]))
            flushes.append(Load(pairs, out_sem.at[len(flushes)]).begin())

        load.wait()
        gather.arrived(0)
        gather.own.wait()
        store(gather.me)
        store(gather.mates_slots[0])
        chip(gather.me)
        gather.middle()
        gather.arrived(3)
        store(gather.s_x)
        store(gather.mates_slots[1])
        chip(gather.s_x)
        flush(gather.me)
        gather.arrived(4)
        store(gather.s_y)
        store(gather.mates_slots[2])
        chip(gather.s_y)
        flush(gather.s_x)
        gather.corner()
        gather.arrived(6)
        store(gather.s_d)
        store(gather.mates_slots[3])
        chip(gather.s_d)
        flush(gather.s_y)

        @pl.loop(0, width // tile)
        def _(t):
            lanes = pl.ds(pl.multiple_of(t * tile, tile), tile)
            g_down_ref[lanes] = jnp.transpose(g_acc[:, lanes]).astype(BF)

        flush(gather.s_d)
        for copy in gather.copies.values():
            copy.wait_send()
        for copy in stores + flushes:
            copy.wait()

    outs = [
        shape((n, rows, width), BF),
        shape((n * rows, units), BF),
        shape((n * rows, 2 * units), BF),
        shape((2 * units, n * rows), BF),
        shape((width, units), BF),
    ]
    scratch = [
        pltpu.VMEM((n * rows, units), BF),
        pltpu.VMEM((n * rows, 2 * units), BF),
        pltpu.VMEM((2 * units, n * rows), BF),
        pltpu.SemaphoreType.DMA((4, 3)),
        pltpu.VMEM((n, rows, width), BF),
        pltpu.VMEM(dy.shape, BF),
        pltpu.VMEM(gate_up.shape, BF),
        pltpu.VMEM(down.shape, BF),
        pltpu.VMEM((units, 2 * rows), BF),
        pltpu.VMEM((units, width), F32),
        pltpu.SemaphoreType.DMA((3,)),
        pltpu.SemaphoreType.DMA((n,)),
    ]
    ins = [xn, dy, gate_up, down]
    return remote_call(kernel, number, ins, outs, scratch + GATHER_SEMS, any_outs=(0, 1, 2, 3), any_ins=(1, 2, 3))


def feed_forward_input(dgu, gate_up, h1, cotangent, gain, xn_all, dgu_t, n_ctx, number):
    rows, width = h1.shape
    chunks, unit_rows, _ = gate_up.shape
    units = chunks * unit_rows // 2
    tile, part = 256, 256

    def kernel(
        dgu_ref,
        w_hbm,
        h_ref,
        dy_ref,
        gain_ref,
        xn_hbm,
        dgu_t_hbm,
        dh_ref,
        dhb_ref,
        dgain_ref,
        g_up_out,
        g_up_ref,
        g_up_sem,
        w_ref,
        xn_ref,
        dgu_t_ref,
        w_sem,
        load_sem,
        *scratch,
    ):
        total = scratch[-1]
        w_load = Load([(w_hbm, w_ref)], w_sem).begin()
        load = Load([(dgu_t_hbm, dgu_t_ref), (xn_hbm, xn_ref)], load_sem).begin()

        def partial(slot, t):
            r = pl.ds(pl.multiple_of(slot * rows, rows), rows)
            lanes = pl.ds(pl.multiple_of(t * tile, tile), tile)
            acc = nn(dgu_ref[r, :unit_rows], w_ref[0, :, lanes])
            for n in range(1, chunks):
                acc = acc + nn(dgu_ref[r, n * unit_rows : (n + 1) * unit_rows], w_ref[n, :, lanes])
            return acc

        def up_gradient(first, last):
            @pl.loop(first, last)
            def _(k):
                r = pl.ds(pl.multiple_of(k * part, part), part)

                @pl.loop(0, width // tile)
                def _(t):
                    lanes = pl.ds(pl.multiple_of(t * tile, tile), tile)
                    g_up_ref[r, lanes] = nn(dgu_t_ref[r], xn_ref[:, lanes]).astype(BF)

        scatter = Scatter(n_ctx, partial, tile, *scratch)
        greet_neighbours(n_ctx)
        w_load.wait()
        scatter.to_mate()
        scatter.pairs()
        load.wait()
        up_gradient(0, units // part)
        scatter.join()
        flushes = [Load([(g_up_ref.at[pl.ds(0, units)], g_up_out.at[pl.ds(0, units)])], g_up_sem.at[0]).begin()]
        up_gradient(units // part, 2 * units // part)
        scatter.end()
        flushes.append(Load([(g_up_ref.at[pl.ds(units, units)], g_up_out.at[pl.ds(units, units)])], g_up_sem.at[1]).begin())
        dgain_ref[...] = jnp.zeros_like(dgain_ref)

        def finish(r):
            h, d = h_ref[r], total[r]
            scale = inv_rms(h)
            dgain_ref[0:1] += jnp.sum(d * h * scale, 0, keepdims=True)
            dh = dy_ref[r].astype(F32) + norm_back(d, gain_ref[1:2], h, scale)
            dh_ref[r] = dh
            dhb_ref[r] = dh.astype(BF)

        row_chunks(rows, 32, finish)
        for copy in flushes:
            copy.wait()

    outs = [
        shape((rows, width), F32),
        shape((rows, width), BF),
        shape((8, width), F32),
        shape((2 * units, width), BF),
    ]
    scratch = [
        pltpu.VMEM((2 * units, width), BF),
        pltpu.SemaphoreType.DMA((2, 1)),
        pltpu.VMEM((chunks, unit_rows, width), BF),
        pltpu.VMEM(xn_all.shape, BF),
        pltpu.VMEM(dgu_t.shape, BF),
        pltpu.SemaphoreType.DMA((1,)),
        pltpu.SemaphoreType.DMA((2,)),
    ]
    return remote_call(
        kernel,
        number,
        [dgu, gate_up, h1, cotangent, gain, xn_all, dgu_t],
        outs,
        scratch + scatter_scratch(rows, width),
        any_outs=(3,),
        any_ins=(1, 5, 6),
    )


def attention_backward(
    dh_all, xn, qkv, attn, lse, cosine, sine, pos_rows, pos_columns, hidden, out_w, down_w, h1, swapped, n_outer, n_ctx, number
):
    rows = dh_all.shape[0]
    own_rows, width = h1.shape
    group = rows // 2
    heads = attn.shape[1] // LANES
    k_at, v_at = heads * LANES, (heads + 1) * LANES
    block = min(QUERY_BLOCK, group)
    features = attn.shape[1]
    tile = 256
    place_rows = width // n_outer // (2 * n_ctx)

    def kernel(
        dh_hbm,
        xn_hbm,
        qkv_hbm,
        attn_hbm,
        lse_ref,
        cos_hbm,
        sin_hbm,
        rows_ref,
        columns_hbm,
        hidden_ref,
        out_w_hbm,
        w_hbm,
        h_ref,
        swap_src,
        dproj_ref,
        result_ref,
        swap_dst,
        g_dst,
        g_qkv_ref,
        xn_ref,
        qkv_ref,
        attn_ref,
        cos_ref,
        sin_ref,
        columns_ref,
        g_ref,
        g_arrived,
        g_sum,
        g_send,
        g_recv,
        dk_ref,
        dv_ref,
        w_ref,
        out_w_ref,
        dh_ref,
        load_sem,
        dh_sem,
        *scratch,
    ):
        swap_sem, g_swap_sem, scratch = scratch[:3], scratch[3:6], scratch[6:]
        total = scratch[-1]
        o = lax.axis_index("o")
        peers = outer_peers(n_outer)
        load = Load([(w_hbm, w_ref)], load_sem).begin()
        pairs = [(out_w_hbm, out_w_ref), (dh_hbm, dh_ref), (attn_hbm, attn_ref), (qkv_hbm, qkv_ref), (cos_hbm, cos_ref), (sin_hbm, sin_ref)]
        dh_load = Load(pairs + [(columns_hbm, columns_ref), (xn_hbm, xn_ref)], dh_sem).begin()
        swap = Swap(n_ctx, [(swap_src, swap_dst)], *swap_sem)
        g_swap = Swap(n_ctx, [(g_sum, g_dst)], *g_swap_sem)

        def partial(slot, t):
            a = hidden_ref[pl.ds(pl.multiple_of(slot * own_rows, own_rows), own_rows)]
            return nt(a, w_ref[pl.ds(pl.multiple_of(t * tile, tile), tile)])

        scatter = Scatter(n_ctx, partial, tile, *scratch)
        greet(swap.devices + peers)

        def back(g, b):
            keys_at = pl.ds(g * group, group)
            r = pl.ds(g * group + b * block, block)
            if b == 0:
                dk_ref[...] = jnp.zeros_like(dk_ref)
                dv_ref[...] = jnp.zeros_like(dv_ref)
            key_pos = columns_ref[keys_at, 0:1]
            ok = (key_pos >= rows_ref[1:2, r]) & (key_pos <= rows_ref[0:1, r])
            da_all = nn(dh_ref[r], out_w_ref[...]).astype(BF)

            for h in range(heads):
                lanes = slice(h * LANES, (h + 1) * LANES)
                da, q = da_all[:, lanes], qkv_ref[r, lanes]
                keys = qkv_ref[keys_at, k_at : k_at + LANES]
                s = nt(keys, q) * SCALE - lse_ref[h : h + 1, r]
                p = jnp.exp(jnp.where(ok, s, MASK_FILL))
                dv_ref[...] += nn(p.astype(BF), da)
                delta = jnp.transpose(da.astype(F32) * attn_ref[r, lanes].astype(F32))
                delta = jnp.sum(delta, 0, keepdims=True)
                dp = nt(qkv_ref[keys_at, v_at : v_at + LANES], da)
                ds = (p * (dp - delta)).astype(BF)
                dk_ref[...] += nn(ds, q)
                dq = tn(ds, keys) * SCALE
                dproj_ref[r, lanes] = rotate(dq, cos_ref[r], -sin_ref[r]).astype(BF)

            if b == group // block - 1:
                dk = rotate(dk_ref[...] * SCALE, cos_ref[keys_at], -sin_ref[keys_at])
                dproj_ref[keys_at, k_at : k_at + LANES] = dk.astype(BF)
                dproj_ref[keys_at, v_at : v_at + LANES] = dv_ref[...].astype(BF)

        def out_gradient():
            @pl.loop(0, width // 384)
            def _(k):
                d = pl.ds(pl.multiple_of(k * 384, 384), 384)
                g_ref[d] = jnp.transpose(tn(attn_ref[...], dh_ref[:, d])).astype(BF)

        def own_place(outer):
            return pl.ds(pl.multiple_of(outer * (width // n_outer), 16), width // n_outer)

        def qkv_gradient():
            half = HEAD_SIZE // 2

            @pl.loop(0, width // 256)
            def _(t):
                lanes = pl.ds(pl.multiple_of(t * 256, 256), 256)
                for h in range(heads + 2):
                    g = tn(dproj_ref[:, h * LANES : (h + 1) * LANES], xn_ref[:, lanes]).astype(BF)
                    for k in range(2):
                        at = h * HEAD_SIZE + k * half
                        g_qkv_ref[at : at + half, lanes] = g[k * LANES // 2 : k * LANES // 2 + half]

        load.wait()
        units = [(g, b) for g in range(2) for b in range(group // block)]
        scatter.to_mate()
        dh_load.wait()
        back(*units[0])
        scatter.pairs()
        swap.begin()
        out_gradient()
        back(*units[1])
        scatter.join()
        g_copies = [
            send(g_ref.at[own_place(device[0])], g_arrived.at[k], g_send.at[k], g_recv.at[k], device)
            for k, device in enumerate(peers)
        ]
        for unit in units[2:]:
            back(*unit)
        for copy in g_copies:
            copy.wait_recv()
        g_total = g_ref[own_place(o)].astype(F32)
        for k in range(n_outer - 1):
            g_total = g_total + g_arrived[k].astype(F32)
        for d in range(2 * n_ctx):
            g_sum[d] = g_total[d * place_rows : (d + 1) * place_rows].astype(BF)
        qkv_gradient()
        g_swap.begin()
        scatter.end()
        swap.end()

        def finish(r):
            result_ref[r] = (h_ref[r] + total[r]).astype(BF)

        row_chunks(own_rows, 32, finish)
        g_swap.end()
        for copy in g_copies:
            copy.wait_send()

    outs = [
        shape(qkv.shape, BF),
        shape((own_rows, width), BF),
        shape(swapped.shape, BF),
        shape((2 * n_ctx, place_rows, features), BF),
        shape((qkv.shape[1] // LANES * HEAD_SIZE, width), BF),
    ]
    ins = [dh_all, xn, qkv, attn, lse, cosine, sine, pos_rows, pos_columns, hidden, out_w, down_w, h1, swapped]
    scratch = [
        pltpu.VMEM(xn.shape, BF),
        pltpu.VMEM(qkv.shape, BF),
        pltpu.VMEM(attn.shape, BF),
        pltpu.VMEM(cosine.shape, F32),
        pltpu.VMEM(sine.shape, F32),
        pltpu.VMEM(pos_columns.shape, jnp.int32),
        pltpu.VMEM((width, features), BF),
        pltpu.VMEM((n_outer - 1, width // n_outer, features), BF),
        pltpu.VMEM((2 * n_ctx, place_rows, features), BF),
        pltpu.SemaphoreType.DMA((n_outer - 1,)),
        pltpu.SemaphoreType.DMA((n_outer - 1,)),
        pltpu.VMEM((group, LANES), F32),
        pltpu.VMEM((group, LANES), F32),
        pltpu.VMEM(down_w.shape, BF),
        pltpu.VMEM(out_w.shape, BF),
        pltpu.VMEM(dh_all.shape, BF),
        pltpu.SemaphoreType.DMA((1,)),
        pltpu.SemaphoreType.DMA((8,)),
    ]
    scratch += swap_sems(1, n_ctx) + swap_sems(1, n_ctx) + scatter_scratch(own_rows, width)
    return remote_call(kernel, number, ins, outs, scratch, any_ins=(0, 1, 2, 3, 5, 6, 8, 10, 11))


def attention_input(dproj, w, tokens, dh1, gain, gain_terms, n_outer, n_ctx, number):
    rows, width = tokens.shape
    tile = 256
    features = dproj.shape[1]
    n = 2 * n_ctx

    def kernel(
        d_ref, w_hbm, x_ref, dh_ref, gain_ref, terms_ref, out_ref, sum_ref, w_ref, load_sem, *scratch
    ):
        swap_sem, scratch = scratch[:3], scratch[3:]
        terms, summed, arrived, send_sem, recv_sem, local_sem = scratch[:6]
        scratch = scratch[6:]
        total = scratch[-1]
        load = Load(padded_loads(w_hbm, w_ref), load_sem).begin()
        o = lax.axis_index("o")

        def partial(slot, t):
            a = d_ref[pl.ds(pl.multiple_of(slot * rows, rows), rows)]
            return nn(a, w_ref[:, pl.ds(pl.multiple_of(t * tile, tile), tile)])

        scatter = Scatter(n_ctx, partial, tile, *scratch)
        swap = Swap(n_ctx, [(terms_ref, terms)], *swap_sem)
        peers = outer_peers(n_outer)
        greet(swap.devices + peers)
        swap.begin()
        load.wait()
        scatter.to_mate()
        scatter.pairs()
        swap.end()
        summed[...] = jnp.sum(terms[...], 0)
        scatter.join()
        copies = []
        for k, device in enumerate(peers):
            copies.append(send(summed.at[device[0]], arrived.at[o], send_sem.at[k], recv_sem.at[k], device))
        own = pltpu.make_async_copy(summed.at[o], arrived.at[o], local_sem)
        own.start()
        scatter.end()

        def finish(r):
            x, d = x_ref[r].astype(F32), total[r]
            out_ref[r] = dh_ref[r] + norm_back(d, gain_ref[0:1], x, inv_rms(x))

        row_chunks(rows, 32, finish)
        for copy in copies:
            copy.wait_recv()
        own.wait()
        sum_ref[...] = jnp.sum(arrived[...], 0)
        for copy in copies:
            copy.wait_send()

    outs = [shape((rows, width), F32), shape((8, LANES), F32)]
    ins = [dproj, w, tokens, dh1, gain, gain_terms]
    n_loads = features // (LANES // 2)
    scratch = [pltpu.VMEM((features, width), BF), pltpu.SemaphoreType.DMA((n_loads,))]
    scratch += swap_sems(1, n_ctx)
    scratch += [
        pltpu.VMEM((n, n_outer, 8, LANES), F32),
        pltpu.VMEM((n_outer, 8, LANES), F32),
        pltpu.VMEM((n_outer, 8, LANES), F32),
        pltpu.SemaphoreType.DMA((n_outer - 1,)),
        pltpu.SemaphoreType.DMA((n_outer - 1,)),
        pltpu.SemaphoreType.DMA,
    ]
    scratch += scatter_scratch(rows, width)
    return remote_call(kernel, number, ins, outs, scratch, any_ins=(1,))


def make_shards(n_outer, n_inner, n_ctx):
    n_plane = n_inner * n_ctx
    moves = feature_moves(n_outer, n_plane)
    back = [(b, a) for a, b in moves]

    def layer(tokens, norm_attn, w_qkv, w_out, norm_mlp, w_gate_up, w_down, cotangent, seq_lengths, block_slot):
        _, width = tokens.shape
        gain_rows = norm_attn.shape[0]
        out_rows = w_out.shape[0]
        unit_rows = w_gate_up.shape[0]
        n_seqs, n_slots = seq_lengths.shape[1], block_slot.shape[1]
        units = FF // n_plane
        qkv_w = z_ag(lax.ppermute(w_qkv, ALL, moves)).reshape(CHUNKS, -1, width)
        gain_part = jnp.pad(jnp.stack([norm_attn, norm_mlp]), ((0, 6), (0, LANES - gain_rows)))
        meta = jnp.concatenate([seq_lengths[0], block_slot[0]])
        meta = jnp.pad(meta[None], ((0, 7), (0, LANES - n_seqs - n_slots)))
        out_parts = pad_heads(w_out, 1).reshape(out_rows, 2, n_plane // 2, -1).transpose(2, 1, 0, 3)
        out_parts = out_parts.reshape(n_plane, out_rows, -1)
        down_parts = w_down.reshape(out_rows, n_outer // 2, n_plane, unit_rows).transpose(2, 0, 1, 3)
        down_parts = down_parts.reshape(n_plane, out_rows, units)
        w_gate_up, out_parts, down_parts = lax.optimization_barrier((w_gate_up, out_parts, down_parts))
        gate_up = z_ag(w_gate_up)
        gate_up = gate_up.reshape(CHUNKS, -1, width)
        x_all, out_parts, down_w, gains, cosine, sine, pos_rows, pos_columns = prologue(
            tokens, out_parts, down_parts, gain_part, meta, n_seqs, n_outer, n_ctx, 1
        )
        x_all = x_all.reshape(-1, width)
        gains = gains[:, :, :2, :gain_rows].transpose(2, 0, 1, 3).reshape(2, width)
        down_w = z_ag(down_w.reshape(-1, units))
        qkv, attn, lse, dy_all, xn1, out_w = attention_forward(
            x_all, gains, qkv_w, cosine, sine, pos_rows, pos_columns, cotangent, out_parts, n_outer, n_ctx, 2
        )
        out_w = out_w.reshape(width, -1)
        h1, xn2 = output_projection(attn, out_w, tokens, gains, n_ctx, 3)
        xn2_all, hidden, dgu, dgu_t, g_down = feed_forward(xn2, dy_all, gate_up, down_w, n_ctx, 4)
        dgu, g_down = lax.optimization_barrier((dgu, g_down))
        g_down = z_rs(g_down)
        dh1, dh1_bf, dgain_two, g_gate_up = feed_forward_input(
            dgu, gate_up, h1, cotangent, gains, xn2_all.reshape(-1, width), dgu_t, n_ctx, 5
        )
        g_gate_up = z_rs(g_gate_up)
        dh1_all = plane_gather(dh1_bf, n_ctx, 6)
        dh1_all, g_down = lax.optimization_barrier((dh1_all, g_down))
        g_down = g_down.reshape(n_plane, out_rows, units)
        dproj, result, g_down, g_out, g_qkv = attention_backward(
            dh1_all, xn1, qkv, attn, lse, cosine, sine, pos_rows, pos_columns, hidden, out_w, down_w, h1, g_down, n_outer, n_ctx, 7
        )
        terms = jnp.sum(qkv_w.reshape(-1, width).astype(F32) * g_qkv.astype(F32), 0) / gains[0]
        terms = jnp.stack([terms, dgain_two[0]]).reshape(2, n_outer, n_plane, gain_rows).transpose(2, 1, 0, 3)
        terms = jnp.pad(terms, ((0, 0), (0, 0), (0, 6), (0, LANES - gain_rows)))
        dproj, g_qkv, g_gate_up = lax.optimization_barrier((dproj, g_qkv, g_gate_up))
        g_qkv = z_rs(g_qkv)
        grad_input, g = attention_input(dproj, qkv_w, tokens, dh1, gains, terms, n_outer, n_ctx, 8)
        grad_input, g_qkv = lax.optimization_barrier((grad_input, g_qkv))
        grad_qkv = lax.ppermute(g_qkv, ALL, back).astype(F32)
        g_out = g_out.reshape(n_plane // 2, 2, out_rows, -1).transpose(2, 1, 0, 3)
        grad_out = cut_heads(g_out.reshape(out_rows, -1), 1).astype(F32)
        grad_down = g_down.reshape(n_plane, out_rows, n_outer // 2, unit_rows).transpose(1, 2, 0, 3)
        grad_down = grad_down.reshape(out_rows, -1).astype(F32)
        g = g[:, :gain_rows]
        return (result, grad_input, g[0], grad_qkv, grad_out, g[1], g_gate_up.astype(F32), grad_down)

    return layer


def solution(mesh):
    n_inner = 2
    n_ctx = mesh.shape["ctx"]
    n_outer = mesh.shape["dp"] // n_inner
    split = Mesh(mesh.devices.reshape(n_outer, n_inner, n_ctx), ALL)
    rows, vec, grp = P(ALL, None), P(ALL), P(("o", "i"), None)
    return jax.shard_map(
        make_shards(n_outer, n_inner, n_ctx),
        mesh=split,
        in_specs=(rows, vec, rows, rows, vec, rows, rows, rows, grp, grp),
        out_specs=(rows, rows, vec, rows, rows, vec, rows, rows),
        check_vma=False,
    )
```
